32 devices in a mesh: nest: 4 (over x, core), py: 2 (over y), px: 4 (over z).
Axes of the slice: x: 2, y: 2, z: 4, core: 2. Of those that a mesh axis runs over, the one named last changes fastest.
Arguments:
- initial_state: float32 [4, 4, 256, 256], P('nest', None, 'px', 'py'), may hold values from -6 to 6
- drive_modes: float32 [3, 4, 64, 64], replicated, may hold values from -6 to 6
- relax_rates: float32 [4, 4], P('nest'), may hold values from 0.2 to 0.9
- nest_offsets: int32 [4, 2], replicated, may hold values from 0 to 170
Outputs:
- final_state: float32 [4, 4, 256, 256], P('nest', None, 'px', 'py')
- final_modes: float32 [4, 4, 64, 64], P('nest')
The draws below stay inside these ranges and needn't reach their ends.
Inputs may be any that keep to these rules, and one draw needn't show every extreme that they name: `nest_offsets`: row 0 is not read.
All inputs are finite; a program needn't handle non-finite values.
Results may differ from the reference program's by a relative error of at most 0.0001.
Values sent between devices are 32-bit elements; how exact they have to be, the bound alone decides.
No kernel may reach another device: no remote copies, remote signals or barrier semaphores. Data moves between devices by JAX's collectives and lax.ppermute only.
A program may use at most 64 MiB of HBM per device.

```python
import math
import jax
import jax.numpy as jnp
from jax import lax

LEV = 4
M = 64
RATIO = 3
WIN = 3
NX = 256
NY = 256
N_NEST = 4


def touch_ends(array, stream_key, smallest, high):
    place = [jax.random.randint(jax.random.fold_in(stream_key, axis), (), 0, length) for axis, length in enumerate(array.shape)]
    longest = array.shape.index(max(array.shape))
    next_to = place[:longest] + [(place[longest] + 1) % array.shape[longest]] + place[longest + 1:]
    return array.at[tuple(place)].set(smallest).at[tuple(next_to)].set(high)


def block_scale(rng, shape, split, least, largest):
    loudness = 1.0
    for dim, parts in split:
        heights = jax.random.uniform(jax.random.fold_in(jax.random.fold_in(rng, 6), dim), (parts,), jnp.float32, least / len(split), largest / len(split))
        loudness = loudness * jnp.repeat(jnp.exp(heights), shape[dim] // parts).reshape((-1,) + (1,) * (len(shape) - 1 - dim))
    return loudness


def bell_draw(key, shape, scale, most, split=(), kind=jnp.bfloat16):
    entries = scale * jax.random.normal(key, shape, jnp.float32)
    if split:
        entries = entries * block_scale(key, shape, split, -0.22, 0.18)
    return jnp.clip(entries, -most, most).astype(kind)


def setup_inputs(seed: int = 0) -> dict:
    splits = jax.random.split(jax.random.key(seed), 5)
    return {
        "initial_state": bell_draw(splits[0], (N_NEST, LEV, NX, NY), 1.0, 6.0, ((0, 4), (2, 4), (3, 2)), jnp.float32),
        "drive_modes": bell_draw(splits[1], (WIN, LEV, M, M), 1.0, 6.0, (), jnp.float32),
        "relax_rates": jnp.clip(jnp.exp(math.log(0.9) - 1.50407736 * jax.random.uniform(splits[2], (N_NEST, LEV), jnp.float32) ** block_scale(splits[2], (N_NEST, LEV), ((0, 4),), -0.2, 0.2)), 0.2, 0.9),
        "nest_offsets": touch_ends(jax.random.randint(splits[3], (N_NEST, 2), 0, min(NX, NY) - min(NX, NY) // RATIO), jax.random.fold_in(splits[3], 1), 0, (min(NX, NY) - min(NX, NY) // RATIO) - 1).astype(jnp.int32),
    }


highest = lax.Precision.HIGHEST
diffusion_rate = 0.2

def cosine_basis(numerator, cell_count, mode_count, refine):
    wavenum = jnp.arange(mode_count, dtype=jnp.int32)
    product = wavenum[None, :] * numerator[:, None] % (4 * refine * cell_count)
    angles = jnp.pi * product.astype(jnp.float32) / (2.0 * refine * cell_count)
    weight = jnp.where(wavenum == 0, 1.0, 2.0).astype(jnp.float32) / cell_count
    return jnp.sqrt(weight)[None, :] * jnp.cos(angles)

def diffuse(field_now):
    padded = jnp.pad(field_now, ((0, 0), (1, 1), (1, 1)))
    beside_all = padded[:, 2:, 1:-1] + padded[:, :-2, 1:-1] + padded[:, 1:-1, 2:] + padded[:, 1:-1, :-2]
    return field_now + diffusion_rate * (beside_all - 4.0 * field_now)

def reference(initial_state, drive_modes, relax_rates, nest_offsets):
    cells_x = jnp.arange(NX, dtype=jnp.int32)
    cells_y = jnp.arange(NY, dtype=jnp.int32)
    row_basis = cosine_basis(2 * cells_x + 1, NX, M, 1)
    col_basis = cosine_basis(2 * cells_y + 1, NY, M, 1)
    interp_maps = []
    for domain in range(N_NEST):
        shifted_x = cosine_basis(2 * RATIO * nest_offsets[domain, 0] + 2 * cells_x + 1, NX, M, RATIO)
        shifted_y = cosine_basis(2 * RATIO * nest_offsets[domain, 1] + 2 * cells_y + 1, NY, M, RATIO)
        interp_maps.append((jnp.dot(row_basis.T, shifted_x, precision=highest), jnp.dot(col_basis.T, shifted_y, precision=highest)))
    fields = [initial_state[domain] for domain in range(N_NEST)]
    coeffs = [None] * N_NEST
    for window in range(WIN):
        for domain in range(N_NEST):
            stepped = diffuse(fields[domain])
            partial_rows = jnp.einsum('lxy,ym->lxm', stepped, col_basis, precision=highest)
            own = jnp.einsum('xj,lxm->ljm', row_basis, partial_rows, precision=highest)
            if domain == 0:
                target = drive_modes[window]
            else:
                row_map, col_map = interp_maps[domain]
                target = jnp.einsum('jp,lpq,mq->ljm', row_map, coeffs[domain - 1], col_map, precision=highest)
            change = relax_rates[domain][:, None, None] * (target - own)
            coeffs[domain] = own + change
            back_rows = jnp.einsum('ljm,ym->ljy', change, col_basis, precision=highest)
            fields[domain] = stepped + jnp.einsum('xj,ljy->lxy', row_basis, back_rows, precision=highest)
    return (jnp.stack(fields), jnp.stack(coeffs))
```

```python
import functools
import math

import jax
import jax.numpy as jnp
import numpy as np
from jax import lax
from jax.experimental import pallas as pl
from jax.experimental.pallas import tpu as pltpu
from jax.sharding import PartitionSpec as P

RATIO = 3
RATE = 0.2
EDGE = 8
INTERPRET = False

highest = lax.Precision.HIGHEST


def multinomial(n, i, j):
    return math.factorial(n) // (math.factorial(i) * math.factorial(j) * math.factorial(n - i - j))


@functools.lru_cache(maxsize=None)
def tables(cells, modes, order):
    cell = np.arange(cells)
    mode = np.arange(modes)
    weight = np.sqrt(np.where(mode == 0, 1.0, 2.0) / cells)
    product = mode[None] * (2 * cell[:, None] + 1)
    coarse = np.pi * (product % (4 * cells)) / (2 * cells)
    fine = np.pi * (product % (4 * RATIO * cells)) / (2 * RATIO * cells)
    base = weight * np.cos(coarse)
    second = RATE * (np.eye(cells, k=1) + np.eye(cells, k=-1) - 2 * np.eye(cells))
    powers = [base]
    for _ in range(order):
        powers.append(second @ powers[-1])
    factor = RATE * (2 * np.cos(np.pi * mode / cells) - 2)
    places = list(range(order)) + list(range(cells - order, cells))
    edges = np.zeros((cells, EDGE))
    edges[places, range(2 * order)] = 1
    spill = [(powers[i] - base * factor**i).T @ edges for i in range(order + 1)]
    return {
        "base": base,
        "edges": edges,
        "powers": powers,
        "factor": factor,
        "spill": spill,
        "within": [base.T @ power for power in powers],
        "cos_map": base.T @ (weight * np.cos(fine)),
        "sin_map": base.T @ (weight * np.sin(fine)),
    }


def kron(count, block):
    return np.kron(np.eye(count), block)


def f32(value):
    return jnp.asarray(np.asarray(value, np.float32))


def mm(a, b, dims=((1,), (0,))):
    return lax.dot_general(a, b, (dims, ((), ())), precision=highest, preferred_element_type=jnp.float32)


def call(kernel, shapes, *args):
    specs = [pl.BlockSpec(memory_space=pltpu.SMEM) if a.ndim == 2 and a.size <= 16 else pl.BlockSpec(memory_space=pltpu.VMEM) for a in args]
    return pl.pallas_call(
        kernel,
        in_specs=specs,
        out_specs=jax.tree.map(lambda _: pl.BlockSpec(memory_space=pltpu.VMEM), shapes),
        out_shape=shapes,
        interpret=INTERPRET,
    )(*args)


def shape_of(*dims):
    return jax.ShapeDtypeStruct(dims, jnp.float32)


class Plan:
    def __init__(self, initial_state, drive_modes):
        _, self.levels, self.nx, self.ny = initial_state.shape
        self.windows, _, self.modes, _ = drive_modes.shape
        self.px = lax.axis_size("px")
        self.py = lax.axis_size("py")
        self.nest = lax.axis_size("nest")
        self.lanes = self.levels * self.modes
        self.half = self.levels // 2
        self.low = self.modes + EDGE
        self.sums = self.low + self.half * EDGE
        self.x = tables(self.nx * self.px, self.modes, self.windows)
        self.y = tables(self.ny * self.py, self.modes, self.windows)
        assert self.levels % 4 == 0 and self.modes * 2 == self.ny and self.nx == self.modes
        assert 2 * self.windows <= EDGE and self.half * self.windows <= EDGE


def project(plan, state):
    low, half, lanes = plan.low, plan.half, plan.lanes
    bases = np.concatenate([plan.x["base"], plan.x["edges"]], 1)
    left = np.zeros((plan.px, 2 * plan.modes, plan.nx))
    left[:, :low] = bases.T.reshape(low, plan.px, plan.nx).transpose(1, 0, 2)
    right = plan.y["base"].reshape(plan.py, plan.ny, plan.modes)
    right = np.stack([kron(2, block) for block in right])
    edge = plan.y["edges"].T.reshape(EDGE, plan.py, plan.ny).transpose(1, 0, 2)
    pick = np.zeros((EDGE, plan.ny))
    for i in range(plan.windows):
        pick[i, i] = 1
        pick[plan.windows + i, plan.ny - plan.windows + i] = 1

    def kernel(state_ref, left_ref, right_ref, edge_ref, pick_ref, out_ref):
        px, py = lax.axis_index("px"), lax.axis_index("py")
        basis = left_ref[px]
        rights = right_ref[py]
        edges = edge_ref[py]
        rows = [mm(basis, state_ref[0, level]) for level in range(plan.levels)]
        for pair in range(half):
            both = jnp.concatenate([rows[2 * pair][:low], rows[2 * pair + 1][:low]], 1)
            out_ref[:low, pair * plan.ny : (pair + 1) * plan.ny] = mm(both, rights)
            patch = jnp.concatenate([state_ref[0, 2 * pair], state_ref[0, 2 * pair + 1]], 0)
            out_ref[plan.sums :, pair * plan.ny : (pair + 1) * plan.ny] = mm(pick_ref[...], patch, ((1,), (1,)))
        for level in range(plan.levels):
            at = low + EDGE * (level % half)
            lane = level // half * plan.ny
            out_ref[at : at + EDGE, lane : lane + plan.ny] = mm(edges, rows[level], ((1,), (1,)))

    return call(
        kernel, shape_of(plan.sums + EDGE, lanes), state, f32(left), f32(right), f32(edge), f32(pick)
    )


def facing_rows(plan, state_ref, bottom):
    rows = []
    for group in range(2):
        pair = [state_ref[0, 2 * group + i] for i in range(2)]
        top = jnp.concatenate([p[: plan.windows] for p in pair], 1)
        end = jnp.concatenate([p[plan.nx - plan.windows :] for p in pair], 1)
        rows.append(jnp.where(bottom, end, top))
    rows.append(jnp.zeros((EDGE - 2 * plan.windows, plan.lanes), jnp.float32))
    return jnp.concatenate(rows, 0)


def join_first(plan, own, other, state, columns):
    sums = plan.sums

    def kernel(own_ref, other_ref, state_ref, columns_ref, out_ref):
        out_ref[:sums] = own_ref[:sums] + other_ref[:sums]
        out_ref[sums : sums + EDGE] = facing_rows(plan, state_ref, lax.axis_index("px") % 2 == 0)
        out_ref[sums + EDGE :] = columns_ref[sums:]

    return call(kernel, shape_of(sums + 2 * EDGE, plan.lanes), own, other, state, columns)


def join_second(plan, own, other, state):
    sums = plan.sums

    def kernel(own_ref, other_ref, state_ref, out_ref):
        out_ref[:sums] = own_ref[:sums] + other_ref[:sums]
        out_ref[sums : sums + EDGE] = facing_rows(plan, state_ref, lax.axis_index("px") % 2 == 1)
        out_ref[sums + EDGE :] = own_ref[sums + EDGE :]

    return call(kernel, shape_of(sums + 2 * EDGE, plan.lanes), own, other, state)


def join_last(plan, own, other, rates):
    sums, low, modes = plan.sums, plan.low, plan.modes

    def kernel(own_ref, other_ref, rates_ref, out_ref):
        out_ref[...] = own_ref[:sums] + other_ref[:sums]
        level = lax.broadcasted_iota(jnp.int32, (1, plan.lanes), 1) // modes
        row = jnp.zeros((1, plan.lanes), jnp.float32)
        for i in range(plan.levels):
            row = jnp.where(level == i, rates_ref[0, i], row)
        out_ref[low - 1 : low] = row

    return call(kernel, shape_of(sums, plan.lanes), own, other, rates)


def step_patch(plan, state, columns, above, below):
    nx, ny, windows, sums = plan.nx, plan.ny, plan.windows, plan.sums
    place = np.zeros((EDGE, ny))
    for i in range(windows):
        place[i, i] = 1
        place[windows + i, ny - windows + i] = 1
    rows, lanes = nx + 2 * EDGE, 2 * ny

    def kernel(state_ref, columns_ref, above_ref, below_ref, place_ref, out_ref):
        px, py = lax.axis_index("px"), lax.axis_index("py")
        row = lax.broadcasted_iota(jnp.int32, (rows, lanes), 0) - EDGE + px * nx
        lane = lax.broadcasted_iota(jnp.int32, (rows, lanes), 1)
        lane = jnp.where(lane >= ny + ny // 2, lane - lanes, lane) + py * ny
        inside = (row >= 0) & (row < nx * plan.px) & (lane >= 0) & (lane < ny * plan.py)
        where = place_ref[...]
        for level in range(plan.levels):
            pair, part = level // 2, level % 2

            def beside(ref):
                block = ref[sums : sums + EDGE] if ref is columns_ref else ref[sums + EDGE :]
                block = block[:, pair * ny : (pair + 1) * ny]
                return mm(block, where, ((0,), (0,)))[part * nx : (part + 1) * nx]

            def line(ref):
                block = ref[sums : sums + EDGE]
                return block[pair * windows : (pair + 1) * windows, part * ny : (part + 1) * ny]

            up = jnp.concatenate([line(above_ref), beside(above_ref)[nx - windows :]], 1)
            down = jnp.concatenate([line(below_ref), beside(below_ref)[:windows]], 1)
            middle = jnp.concatenate([state_ref[0, level], beside(columns_ref)], 1)
            blank = jnp.zeros((EDGE - windows, lanes), jnp.float32)
            field = jnp.concatenate([blank, up, middle, down, blank], 0)
            field = jnp.where(inside, field, 0.0)
            for _ in range(windows):
                around = (
                    pltpu.roll(field, 1, 0)
                    + pltpu.roll(field, rows - 1, 0)
                    + pltpu.roll(field, 1, 1)
                    + pltpu.roll(field, lanes - 1, 1)
                )
                field = jnp.where(inside, field + RATE * (around - 4.0 * field), 0.0)
            out_ref[level] = field[EDGE : EDGE + nx, :ny]

    return call(kernel, shape_of(plan.levels, nx, ny), state, columns, above, below, f32(place))


def nudge(plan, stepped, gathered, drive, angles):
    modes, low, lanes, levels = plan.modes, plan.low, plan.lanes, plan.levels
    windows, half, nx, ny = plan.windows, plan.half, plan.nx, plan.ny
    x, y = plan.x, plan.y

    inward = np.concatenate([kron(levels, y["spill"][j].T) for j in range(1, windows + 1)], 1)
    across = [np.concatenate([x["spill"][i] for i in range(1, n + 1)], 1) for n in range(1, windows + 1)]
    width = EDGE * windows
    across = np.concatenate([np.pad(a, ((0, 0), (0, width - a.shape[1]))) for a in across], 0)
    scale_x = np.broadcast_to(x["factor"][:, None], (modes, lanes))
    scale_y = np.broadcast_to(np.tile(y["factor"], levels), (EDGE, lanes))
    maps_x = np.concatenate([x["cos_map"], x["sin_map"]], 0)
    maps_y = np.concatenate([kron(levels, y["cos_map"].T), kron(levels, y["sin_map"].T)], 0)
    again = []
    for p in range(1, windows):
        again.append(
            np.concatenate(
                [
                    sum(multinomial(p, i, j) * x["within"][i] for i in range(p - j + 1))
                    for j in range(p + 1)
                ],
                0,
            )
        )
    again = np.concatenate(again, 0)
    sideways = np.concatenate([kron(levels, y["within"][j]) for j in range(1, windows)], 0)
    rows_x = [p.reshape(plan.px, nx, modes) for p in x["powers"]]
    spread_x = np.zeros((plan.px, windows * nx, windows * modes))
    for j in range(windows):
        for w in range(windows):
            p = windows - 1 - w
            for i in range(p - j + 1):
                spread_x[:, j * nx : (j + 1) * nx, w * modes : (w + 1) * modes] += multinomial(p, i, j) * rows_x[i]
    rows_y = [p.reshape(plan.py, ny, modes) for p in y["powers"]]
    spread_y = np.stack(
        [np.concatenate([kron(2, rows_y[j][d].T) for j in range(windows)], 0) for d in range(plan.py)]
    )

    def kernel(
        stepped_ref, gathered_ref, drive_ref, angles_ref, inward_ref, across_ref, scale_x_ref, scale_y_ref,
        maps_x_ref, maps_y_ref, again_ref, sideways_ref, spread_x_ref, spread_y_ref, state_ref, modes_ref,
    ):
        nest = lax.axis_index("nest")
        px, py = lax.axis_index("px"), lax.axis_index("py")
        scale_x, scale_y = scale_x_ref[...], scale_y_ref[:1]

        def own_modes(domain):
            rows = gathered_ref[domain, :low]
            sides = gathered_ref[domain, low:]
            sides = jnp.concatenate([sides[:, i * ny : (i + 1) * ny] for i in range(2)], 0)
            extra = mm(sides, inward_ref[...], ((0,), (0,)))[:low]
            turned = [rows]
            for j in range(1, windows + 1):
                turned.append(rows * scale_y**j + extra[:, (j - 1) * lanes : j * lanes])
            result = []
            for n in range(1, windows + 1):
                parts = [
                    sum(multinomial(n, i, j) * turned[j] for j in range(n - i + 1)) for i in range(n + 1)
                ]
                total = parts[n][:modes]
                for i in range(n - 1, -1, -1):
                    total = total * scale_x + parts[i][:modes]
                ends = jnp.concatenate([part[modes:] for part in parts[1:]], 0)
                result.append(
                    total + mm(across_ref[(n - 1) * modes : n * modes, : n * EDGE], ends)
                )
            return result

        def carried(p, change):
            at = modes * sum(range(2, p + 1))
            left = mm(again_ref[at : at + (p + 1) * modes], change)
            pieces = jnp.concatenate([left[j * modes : (j + 1) * modes] for j in range(1, p + 1)], 1)
            return left[:modes] + mm(pieces, sideways_ref[: p * lanes])

        coeffs = [jnp.zeros((modes, lanes), jnp.float32)] * windows
        final_modes = coeffs[0]
        final_changes = coeffs
        for domain in range(plan.nest):
            gain = gathered_ref[domain, low - 1 : low]
            own = own_modes(domain)
            cos_x = angles_ref[4 * domain : 4 * domain + 1, :modes]
            sin_x = angles_ref[4 * domain + 1 : 4 * domain + 2, :modes]
            cos_y = angles_ref[4 * domain + 2 : 4 * domain + 3]
            sin_y = angles_ref[4 * domain + 3 : 4 * domain + 4]
            row_map = maps_x_ref[:modes] * cos_x - maps_x_ref[modes:] * sin_x
            new, changes = [], []
            for w in range(windows):
                if domain == 0:
                    target = drive_ref[w]
                else:
                    parent = jnp.concatenate([coeffs[w] * cos_y, coeffs[w] * -sin_y], 1)
                    target = mm(row_map, mm(parent, maps_y_ref[...]))
                before = own[w]
                for v in range(w):
                    before = before + carried(w - v, changes[v])
                change = gain * (target - before)
                changes.append(change)
                new.append(before + change)
            coeffs = new
            mine = nest == domain
            final_modes = jnp.where(mine, new[-1], final_modes)
            final_changes = [jnp.where(mine, a, b) for a, b in zip(changes, final_changes)]
        for level in range(levels):
            modes_ref[0, level] = final_modes[:, level * modes : (level + 1) * modes]
        spread = mm(spread_x_ref[px], jnp.concatenate(final_changes, 0))
        for pair in range(half):
            lane = pair * 2 * modes
            pieces = [spread[j * nx : (j + 1) * nx, lane : lane + 2 * modes] for j in range(windows)]
            field = mm(jnp.concatenate(pieces, 1), spread_y_ref[py])
            for part in range(2):
                level = 2 * pair + part
                state_ref[0, level] = stepped_ref[level] + field[:, part * ny : (part + 1) * ny]

    return call(
        kernel,
        (shape_of(1, levels, nx, ny), shape_of(1, levels, modes, modes)),
        stepped, gathered, drive, angles, f32(inward), f32(across), f32(scale_x), f32(scale_y),
        f32(maps_x), f32(maps_y), f32(again), f32(sideways), f32(spread_x), f32(spread_y),
    )


def map_angles(plan, nest_offsets):
    mode = jnp.tile(jnp.arange(plan.modes, dtype=jnp.int32), plan.levels)
    cells = jnp.array([plan.nx * plan.px, plan.ny * plan.py], jnp.int32)
    turn = nest_offsets[:, :, None] * mode % (2 * cells[None, :, None])
    angle = jnp.pi * turn.astype(jnp.float32) / cells[None, :, None].astype(jnp.float32)
    both = jnp.stack([jnp.cos(angle), jnp.sin(angle)], 2)
    return both.reshape(plan.nest * 4, plan.lanes)


def swap(value, axis, partner):
    size = lax.axis_size(axis)
    return lax.ppermute(value, axis, [(i, partner(i)) for i in range(size) if 0 <= partner(i) < size])


def body(initial_state, drive_modes, relax_rates, nest_offsets):
    plan = Plan(initial_state, drive_modes)
    sums = plan.sums
    angles = map_angles(plan, nest_offsets)
    drive = drive_modes.transpose(0, 2, 1, 3).reshape(plan.windows, plan.modes, plan.lanes)
    share = project(plan, initial_state)
    if plan.py == 2 and plan.px == 4:
        columns = swap(share, "py", lambda i: i ^ 1)
        first = join_first(plan, share, columns, initial_state, columns)
        got_first = swap(first, "px", lambda i: i ^ 1)
        second = join_second(plan, first, got_first, initial_state)
        got_second = swap(second, "px", lambda i: i ^ 3)
        last = join_last(plan, second, got_second, relax_rates)
        even = lax.axis_index("px") % 2 == 0
        above = jnp.where(even, got_second, got_first)
        below = jnp.where(even, got_first, got_second)
    else:
        edge = jnp.arange(sums + EDGE)[:, None] < sums + plan.windows
        right = swap(share, "py", lambda i: i - 1)
        left = swap(share, "py", lambda i: i + 1)
        columns = jnp.where(edge, right, left)
        blank = jnp.zeros_like(share)
        first = join_first(plan, share, blank, initial_state, columns)
        second = join_second(plan, first, jnp.zeros_like(first), initial_state)
        even = lax.axis_index("px") % 2 == 0
        above = swap(jnp.where(even, first, second), "px", lambda i: i + 1)
        below = swap(jnp.where(even, second, first), "px", lambda i: i - 1)
        total = lax.psum(share[:sums], ("py", "px"))
        last = join_last(plan, total, jnp.zeros_like(total), relax_rates)
    gathered = lax.all_gather(last, "nest")
    stepped = step_patch(plan, initial_state, columns, above, below)
    return nudge(plan, stepped, gathered, drive, angles)


def solution(mesh):
    return jax.shard_map(
        body,
        mesh=mesh,
        in_specs=(P("nest", None, "px", "py"), P(), P("nest", None), P()),
        out_specs=(P("nest", None, "px", "py"), P("nest", None, None, None)),
        check_vma=False,
    )
```

```python
import functools
import math

import jax
import jax.numpy as jnp
import numpy as np
from jax import lax
from jax.experimental import pallas as pl
from jax.experimental.pallas import tpu as pltpu
from jax.sharding import PartitionSpec as P

RATIO = 3
RATE = 0.2
EDGE = 8
INTERPRET = False

highest = lax.Precision.HIGHEST


def multinomial(n, i, j):
    return math.factorial(n) // (math.factorial(i) * math.factorial(j) * math.factorial(n - i - j))


@functools.lru_cache(maxsize=None)
def tables(cells, modes, order):
    cell = np.arange(cells)
    mode = np.arange(modes)
    weight = np.sqrt(np.where(mode == 0, 1.0, 2.0) / cells)
    product = mode[None] * (2 * cell[:, None] + 1)
    coarse = np.pi * (product % (4 * cells)) / (2 * cells)
    fine = np.pi * (product % (4 * RATIO * cells)) / (2 * RATIO * cells)
    base = weight * np.cos(coarse)
    second = RATE * (np.eye(cells, k=1) + np.eye(cells, k=-1) - 2 * np.eye(cells))
    powers = [base]
    for _ in range(order):
        powers.append(second @ powers[-1])
    factor = RATE * (2 * np.cos(np.pi * mode / cells) - 2)
    places = list(range(order)) + list(range(cells - order, cells))
    edges = np.zeros((cells, EDGE))
    edges[places, range(2 * order)] = 1
    spill = [(powers[i] - base * factor**i).T @ edges for i in range(order + 1)]
    return {
        "base": base,
        "edges": edges,
        "powers": powers,
        "factor": factor,
        "spill": spill,
        "within": [base.T @ power for power in powers],
        "cos_map": base.T @ (weight * np.cos(fine)),
        "sin_map": base.T @ (weight * np.sin(fine)),
    }


def kron(count, block):
    return np.kron(np.eye(count), block)


def f32(value):
    return jnp.asarray(np.asarray(value, np.float32))


def mm(a, b, dims=((1,), (0,))):
    return lax.dot_general(a, b, (dims, ((), ())), precision=highest, preferred_element_type=jnp.float32)


def bf16(value):
    return np.asarray(value, jnp.bfloat16)


def parts_of(value):
    high = bf16(value)
    return high, bf16(value - high.astype(np.float64))


def left_table(value):
    high, low = parts_of(value)
    return jnp.asarray(np.concatenate([high, low, high], -1))


def right_table(value):
    high, low = parts_of(value)
    upper = np.concatenate([high, low], -1)
    lower = np.concatenate([high, np.zeros_like(low)], -1)
    return jnp.asarray(np.concatenate([upper, lower], -2))


def halves(value):
    high = value.astype(jnp.bfloat16)
    return high, (value - high.astype(jnp.float32)).astype(jnp.bfloat16)


def dot(a, b, dims=((1,), (0,))):
    return lax.dot_general(a, b, (dims, ((), ())), preferred_element_type=jnp.float32)


def stacked(value):
    high, low = halves(value)
    return jnp.concatenate([high, high, low], 0)


def times_right(value, table):
    out = dot(jnp.concatenate(halves(value), 1), table)
    width = out.shape[1] // 2
    return out[:, :width] + out[:, width:]


def in_vmem(value):
    return value if INTERPRET else pltpu.with_memory_space_constraint(value, pltpu.VMEM)


def call(kernel, shapes, *args, first=False, final=False):
    scalars = [a.ndim == 2 and a.size <= 16 for a in args]
    specs = [pl.BlockSpec(memory_space=pltpu.SMEM if s else pltpu.VMEM) for s in scalars]
    if not final and not INTERPRET:
        shapes = jax.tree.map(lambda s: pltpu.VMEM(s.shape, s.dtype), shapes)
    return pl.pallas_call(
        kernel,
        in_specs=specs,
        out_specs=jax.tree.map(lambda _: pl.BlockSpec(memory_space=pltpu.VMEM), shapes),
        out_shape=shapes,
        interpret=INTERPRET,
    )(*[a if s or first else in_vmem(a) for a, s in zip(args, scalars)])


def shape_of(*dims):
    return jax.ShapeDtypeStruct(dims, jnp.float32)


class Plan:
    def __init__(self, initial_state, drive_modes):
        _, self.levels, self.nx, self.ny = initial_state.shape
        self.windows, _, self.modes, _ = drive_modes.shape
        self.px = lax.axis_size("px")
        self.py = lax.axis_size("py")
        self.nest = lax.axis_size("nest")
        self.lanes = self.levels * self.modes
        self.half = self.levels // 2
        self.low = self.modes + EDGE
        self.sums = self.low + self.half * EDGE
        self.x = tables(self.nx * self.px, self.modes, self.windows)
        self.y = tables(self.ny * self.py, self.modes, self.windows)
        assert self.levels % 4 == 0 and self.modes * 2 == self.ny and self.nx == self.modes
        assert 2 * self.windows <= EDGE and self.half * self.windows <= EDGE


def project(plan, state):
    low, half, lanes = plan.low, plan.half, plan.lanes
    bases = np.concatenate([plan.x["base"], plan.x["edges"]], 1)
    left = np.zeros((plan.px, 2 * plan.modes, plan.nx))
    left[:, :low] = bases.T.reshape(low, plan.px, plan.nx).transpose(1, 0, 2)
    right = plan.y["base"].reshape(plan.py, plan.ny, plan.modes)
    right = np.stack([kron(2, block) for block in right])
    edge = plan.y["edges"].T.reshape(EDGE, plan.py, plan.ny).transpose(1, 0, 2)
    pick = np.zeros((EDGE, plan.ny))
    for i in range(plan.windows):
        pick[i, i] = 1
        pick[plan.windows + i, plan.ny - plan.windows + i] = 1

    def kernel(state_ref, left_ref, right_ref, edge_ref, pick_ref, out_ref):
        px, py = lax.axis_index("px"), lax.axis_index("py")
        basis = left_ref[px]
        rights = right_ref[py]
        edges = edge_ref[py]
        rows = [mm(basis, state_ref[0, level]) for level in range(plan.levels)]
        for pair in range(half):
            both = jnp.concatenate([rows[2 * pair][:low], rows[2 * pair + 1][:low]], 1)
            out_ref[:low, pair * plan.ny : (pair + 1) * plan.ny] = mm(both, rights)
            patch = jnp.concatenate([state_ref[0, 2 * pair], state_ref[0, 2 * pair + 1]], 0)
            out_ref[plan.sums :, pair * plan.ny : (pair + 1) * plan.ny] = mm(pick_ref[...], patch, ((1,), (1,)))
        for level in range(plan.levels):
            at = low + EDGE * (level % half)
            lane = level // half * plan.ny
            out_ref[at : at + EDGE, lane : lane + plan.ny] = mm(edges, rows[level], ((1,), (1,)))

    return call(
        kernel, shape_of(plan.sums + EDGE, lanes), state, f32(left), f32(right), f32(edge), f32(pick), first=True
    )


def facing_rows(plan, state_ref, bottom):
    rows = []
    for group in range(2):
        pair = [state_ref[0, 2 * group + i] for i in range(2)]
        top = jnp.concatenate([p[: plan.windows] for p in pair], 1)
        end = jnp.concatenate([p[plan.nx - plan.windows :] for p in pair], 1)
        rows.append(jnp.where(bottom, end, top))
    rows.append(jnp.zeros((EDGE - 2 * plan.windows, plan.lanes), jnp.float32))
    return jnp.concatenate(rows, 0)


def join_first(plan, own, other, state, columns):
    sums = plan.sums

    def kernel(own_ref, other_ref, state_ref, columns_ref, out_ref):
        out_ref[:sums] = own_ref[:sums] + other_ref[:sums]
        out_ref[sums : sums + EDGE] = facing_rows(plan, state_ref, lax.axis_index("px") % 2 == 0)
        out_ref[sums + EDGE :] = columns_ref[sums:]

    return call(kernel, shape_of(sums + 2 * EDGE, plan.lanes), own, other, state, columns)


def join_second(plan, own, other, state):
    sums = plan.sums

    def kernel(own_ref, other_ref, state_ref, out_ref):
        out_ref[:sums] = own_ref[:sums] + other_ref[:sums]
        out_ref[sums : sums + EDGE] = facing_rows(plan, state_ref, lax.axis_index("px") % 2 == 1)
        out_ref[sums + EDGE :] = own_ref[sums + EDGE :]

    return call(kernel, shape_of(sums + 2 * EDGE, plan.lanes), own, other, state)


def join_last(plan, own, other, rates):
    sums, low, modes = plan.sums, plan.low, plan.modes

    def kernel(own_ref, other_ref, rates_ref, out_ref):
        out_ref[...] = own_ref[:sums] + other_ref[:sums]
        level = lax.broadcasted_iota(jnp.int32, (1, plan.lanes), 1) // modes
        row = jnp.zeros((1, plan.lanes), jnp.float32)
        for i in range(plan.levels):
            row = jnp.where(level == i, rates_ref[0, i], row)
        out_ref[low - 1 : low] = row

    return call(kernel, shape_of(sums, plan.lanes), own, other, rates)


def step_patch(plan, state, columns, above, below):
    nx, ny, windows, sums = plan.nx, plan.ny, plan.windows, plan.sums
    place = np.zeros((EDGE, ny))
    for i in range(windows):
        place[i, i] = 1
        place[windows + i, ny - windows + i] = 1
    rows, lanes = nx + 2 * EDGE, 2 * ny

    def kernel(state_ref, columns_ref, above_ref, below_ref, place_ref, out_ref):
        px, py = lax.axis_index("px"), lax.axis_index("py")
        row = lax.broadcasted_iota(jnp.int32, (rows, lanes), 0) - EDGE + px * nx
        lane = lax.broadcasted_iota(jnp.int32, (rows, lanes), 1)
        lane = jnp.where(lane >= ny + ny // 2, lane - lanes, lane) + py * ny
        inside = (row >= 0) & (row < nx * plan.px) & (lane >= 0) & (lane < ny * plan.py)
        where = place_ref[...]
        for level in range(plan.levels):
            pair, part = level // 2, level % 2

            def beside(ref):
                block = ref[sums : sums + EDGE] if ref is columns_ref else ref[sums + EDGE :]
                block = block[:, pair * ny : (pair + 1) * ny]
                return mm(block, where, ((0,), (0,)))[part * nx : (part + 1) * nx]

            def line(ref):
                block = ref[sums : sums + EDGE]
                return block[pair * windows : (pair + 1) * windows, part * ny : (part + 1) * ny]

            up = jnp.concatenate([line(above_ref), beside(above_ref)[nx - windows :]], 1)
            down = jnp.concatenate([line(below_ref), beside(below_ref)[:windows]], 1)
            middle = jnp.concatenate([state_ref[0, level], beside(columns_ref)], 1)
            blank = jnp.zeros((EDGE - windows, lanes), jnp.float32)
            field = jnp.concatenate([blank, up, middle, down, blank], 0)
            field = jnp.where(inside, field, 0.0)
            for _ in range(windows):
                around = (
                    pltpu.roll(field, 1, 0)
                    + pltpu.roll(field, rows - 1, 0)
                    + pltpu.roll(field, 1, 1)
                    + pltpu.roll(field, lanes - 1, 1)
                )
                field = jnp.where(inside, field + RATE * (around - 4.0 * field), 0.0)
            out_ref[level] = field[EDGE : EDGE + nx, :ny]

    return call(kernel, shape_of(plan.levels, nx, ny), state, columns, above, below, f32(place))


def nudge(plan, stepped, gathered, drive, angles, turns):
    modes, low, lanes, levels = plan.modes, plan.low, plan.lanes, plan.levels
    windows, half, nx, ny = plan.windows, plan.half, plan.nx, plan.ny
    x, y = plan.x, plan.y
    width = EDGE * (windows + 1)

    inward = np.concatenate([kron(2, y["spill"][j].T) for j in range(1, windows + 1)], 1)
    high, small = parts_of(inward)
    inward = jnp.asarray(np.concatenate([high, small, high], 0))
    across = np.zeros((windows, modes, width))
    for n in range(1, windows + 1):
        for i in range(1, n + 1):
            across[n - 1, :, (i - 1) * EDGE : i * EDGE] = x["spill"][i]
    across = left_table(across)
    scale_x = f32(np.broadcast_to(x["factor"][:, None], (modes, lanes)))
    scale_y = f32(np.broadcast_to(np.tile(y["factor"], levels), (EDGE, lanes)))
    maps_x = f32(np.stack([np.tile(x["cos_map"], (1, 3)), np.tile(x["sin_map"], (1, 3))]))
    maps_y = f32(np.stack([kron(2, y["cos_map"].T), kron(2, y["sin_map"].T)]))
    again = []
    for p in range(1, windows):
        again.append(sum(multinomial(p, i, 0) * x["within"][i] for i in range(p + 1)))
    again = left_table(np.concatenate(again, 0))
    sideways = jnp.stack([right_table(kron(2, y["within"][j])) for j in range(1, windows)])
    rows_x = [p.reshape(plan.px, nx, modes) for p in x["powers"]]
    spread_x = np.zeros((plan.px, windows, windows * nx, modes))
    for j in range(windows):
        for w in range(windows):
            p = windows - 1 - w
            for i in range(p - j + 1):
                spread_x[:, w, j * nx : (j + 1) * nx] += multinomial(p, i, j) * rows_x[i]
    spread_x = lax.dynamic_index_in_dim(left_table(spread_x), lax.axis_index("px"), 0, keepdims=False)
    rows_y = [p.reshape(plan.py, ny, modes) for p in y["powers"]]
    spread_y = np.stack([[kron(2, rows_y[j][d].T) for j in range(windows)] for d in range(plan.py)])
    spread_y = lax.dynamic_index_in_dim(right_table(spread_y), lax.axis_index("py"), 0, keepdims=False)
    assert windows <= 3

    def pairs(value):
        return jnp.concatenate([value[:, i * ny : (i + 1) * ny] for i in range(half)], 0)

    def unpairs(value):
        return jnp.concatenate([value[i * modes : (i + 1) * modes] for i in range(half)], 1)

    def kernel(
        stepped_ref, drive_ref, angles_ref, turns_ref, inward_ref, across_ref, scale_x_ref, scale_y_ref,
        maps_x_ref, maps_y_ref, again_ref, sideways_ref, spread_x_ref, spread_y_ref, *refs,
    ):
        slots, (state_ref, modes_ref) = refs[:-2], refs[-2:]
        root = plan.nest - 1
        nest = lax.axis_index("nest")
        scale_x, scale_y = scale_x_ref[...], scale_y_ref[:1]
        lane = lax.broadcasted_iota(jnp.int32, (modes, 3 * modes), 1)
        middle = (lane >= modes) & (lane < 2 * modes)

        def own_modes(ref):
            rows = ref[:low]
            extra = []
            for i in range(half):
                sides = ref[low:, i * ny : (i + 1) * ny]
                high = sides.astype(jnp.bfloat16).astype(jnp.float32)
                sides = jnp.concatenate([high, high, sides - high], 0).astype(jnp.bfloat16)
                extra.append(dot(sides, inward_ref[...], ((0,), (0,)))[:low])
            turned = [rows]
            scale = scale_y
            for j in range(windows):
                add = jnp.concatenate([e[:, j * ny : (j + 1) * ny] for e in extra], 1)
                turned.append(rows * scale + add)
                scale = scale * scale_y
            result = []
            for n in range(1, windows + 1):
                parts = [
                    sum(multinomial(n, i, j) * turned[j] for j in range(n - i + 1)) for i in range(n + 1)
                ]
                total = parts[n][:modes]
                for i in range(n - 1, -1, -1):
                    total = total * scale_x + parts[i][:modes]
                ends = [part[modes:] for part in parts[1:]]
                ends += [jnp.zeros((EDGE, lanes), jnp.float32)] * (windows + 1 - n)
                ends = jnp.concatenate(ends, 0)
                result.append(total + dot(across_ref[n - 1], stacked(ends)))
            return result

        def carried(change, count):
            left = dot(again_ref[: count * modes], stacked(change))
            left = [left[i * modes : (i + 1) * modes] for i in range(count)]
            if count == 1:
                return [left[0] + unpairs(times_right(pairs(change), sideways_ref[0]))]
            both = jnp.concatenate([pairs(change), pairs(left[0])], 0)
            once = times_right(both, sideways_ref[0])
            twice = times_right(pairs(change), sideways_ref[1])
            rows = half * modes
            return [left[0] + unpairs(once[:rows]), left[1] + unpairs(2.0 * once[rows:] + twice)]

        owns = [own_modes(ref) for ref in slots]
        coeffs = None
        for slot in range(root, -1, -1):
            gain = slots[slot][low - 1 : low]
            own = owns[slot]
            if slot < root:
                at = 4 * slot
                row_map = (
                    maps_x_ref[0] * angles_ref[at : at + 1, : 3 * modes]
                    - maps_x_ref[1] * angles_ref[at + 1 : at + 2, : 3 * modes]
                )
                rounded = row_map.astype(jnp.bfloat16).astype(jnp.float32)
                row_map = jnp.where(middle, row_map - rounded, rounded).astype(jnp.bfloat16)
                col_map = (
                    maps_y_ref[0] * turns_ref[:, 2 * slot : 2 * slot + 1]
                    - maps_y_ref[1] * turns_ref[:, 2 * slot + 1 : 2 * slot + 2]
                )
                high, small = halves(col_map)
                col_map = jnp.concatenate(
                    [jnp.concatenate([high, small], 1), jnp.concatenate([high, jnp.zeros_like(high)], 1)], 0
                )
            new, changes, later = [], [], []
            for w in range(windows):
                target = drive_ref[w]
                if slot < root:
                    inner = dot(row_map, stacked(unpairs(times_right(pairs(coeffs[w]), col_map))))
                    target = jnp.where(nest <= slot, target, inner)
                before = own[w]
                for v in range(w):
                    before = before + later[v][w - v - 1]
                change = gain * (target - before)
                if w < windows - 1:
                    later.append(carried(change, windows - 1 - w))
                changes.append(change)
                new.append(before + change)
            coeffs = new
        for level in range(levels):
            modes_ref[0, level] = coeffs[-1][:, level * modes : (level + 1) * modes]
        spread = sum(dot(spread_x_ref[w], stacked(changes[w])) for w in range(windows))
        field = sum(
            times_right(pairs(spread[j * nx : (j + 1) * nx]), spread_y_ref[j]) for j in range(windows)
        )
        for level in range(levels):
            row, at = level // 2 * nx, level % 2 * ny
            state_ref[0, level] = stepped_ref[level] + field[row : row + nx, at : at + ny]

    return call(
        kernel,
        (shape_of(1, levels, nx, ny), shape_of(1, levels, modes, modes)),
        stepped, drive, angles, turns, inward, across, scale_x, scale_y,
        maps_x, maps_y, again, sideways, spread_x, spread_y, *gathered,
        final=True,
    )


def map_angles(plan, nest_offsets):
    mode = jnp.tile(jnp.arange(plan.modes, dtype=jnp.int32), plan.levels)
    cells = jnp.array([plan.nx * plan.px, plan.ny * plan.py], jnp.int32)
    domain = lax.axis_index("nest") - jnp.arange(plan.nest)
    offsets = nest_offsets[jnp.maximum(domain, 0)]
    turn = offsets[:, :, None] * mode % (2 * cells[None, :, None])
    angle = jnp.pi * turn.astype(jnp.float32) / cells[None, :, None].astype(jnp.float32)
    both = jnp.stack([jnp.cos(angle), jnp.sin(angle)], 2)
    turns = both[:, 1, :, : 2 * plan.modes].reshape(2 * plan.nest, 2 * plan.modes).T
    return both.reshape(plan.nest * 4, plan.lanes), turns


def swap(value, axis, partner):
    size = lax.axis_size(axis)
    return lax.ppermute(value, axis, [(i, partner(i)) for i in range(size) if 0 <= partner(i) < size])


def body(initial_state, drive_modes, relax_rates, nest_offsets):
    plan = Plan(initial_state, drive_modes)
    sums = plan.sums
    angles, turns = map_angles(plan, nest_offsets)
    drive = drive_modes.transpose(0, 2, 1, 3).reshape(plan.windows, plan.modes, plan.lanes)
    share = project(plan, initial_state)
    if plan.py == 2 and plan.px == 4:
        columns = swap(share, "py", lambda i: i ^ 1)
        first = join_first(plan, share, columns, initial_state, columns)
        got_first = swap(first, "px", lambda i: i ^ 1)
        second = join_second(plan, first, got_first, initial_state)
        got_second = swap(second, "px", lambda i: i ^ 3)
        last = join_last(plan, second, got_second, relax_rates)
        even = lax.axis_index("px") % 2 == 0
        above = jnp.where(even, got_second, got_first)
        below = jnp.where(even, got_first, got_second)
    else:
        edge = jnp.arange(sums + EDGE)[:, None] < sums + plan.windows
        right = swap(share, "py", lambda i: i - 1)
        left = swap(share, "py", lambda i: i + 1)
        columns = jnp.where(edge, right, left)
        blank = jnp.zeros_like(share)
        first = join_first(plan, share, blank, initial_state, columns)
        second = join_second(plan, first, jnp.zeros_like(first), initial_state)
        even = lax.axis_index("px") % 2 == 0
        above = swap(jnp.where(even, first, second), "px", lambda i: i + 1)
        below = swap(jnp.where(even, second, first), "px", lambda i: i - 1)
        total = lax.psum(share[:sums], ("py", "px"))
        last = join_last(plan, total, jnp.zeros_like(total), relax_rates)
    gathered = [last] + [swap(last, "nest", lambda i, s=s: i + s) for s in range(1, plan.nest)]
    stepped = step_patch(plan, initial_state, columns, above, below)
    return nudge(plan, stepped, gathered, drive, angles, turns)


def solution(mesh):
    return jax.shard_map(
        body,
        mesh=mesh,
        in_specs=(P("nest", None, "px", "py"), P(), P("nest", None), P()),
        out_specs=(P("nest", None, "px", "py"), P("nest", None, None, None)),
        check_vma=False,
    )
```

```python
import functools
import math

import jax
import jax.numpy as jnp
import numpy as np
from jax import lax
from jax.experimental import pallas as pl
from jax.experimental.pallas import tpu as pltpu
from jax.sharding import PartitionSpec as P

RATIO = 3
RATE = 0.2
EDGE = 8
INTERPRET = False


def multinomial(n, i, j):
    return math.factorial(n) // (math.factorial(i) * math.factorial(j) * math.factorial(n - i - j))


@functools.lru_cache(maxsize=None)
def tables(cells, modes, order):
    cell = np.arange(cells)
    mode = np.arange(modes)
    weight = np.sqrt(np.where(mode == 0, 1.0, 2.0) / cells)
    product = mode[None] * (2 * cell[:, None] + 1)
    coarse = np.pi * (product % (4 * cells)) / (2 * cells)
    fine = np.pi * (product % (4 * RATIO * cells)) / (2 * RATIO * cells)
    base = weight * np.cos(coarse)
    second = RATE * (np.eye(cells, k=1) + np.eye(cells, k=-1) - 2 * np.eye(cells))
    powers = [base]
    for _ in range(order):
        powers.append(second @ powers[-1])
    factor = RATE * (2 * np.cos(np.pi * mode / cells) - 2)
    places = list(range(order)) + list(range(cells - order, cells))
    edges = np.zeros((cells, EDGE))
    edges[places, range(2 * order)] = 1
    spill = [(powers[i] - base * factor**i).T @ edges for i in range(order + 1)]
    return {
        "base": base,
        "edges": edges,
        "powers": powers,
        "factor": factor,
        "spill": spill,
        "within": [base.T @ power for power in powers],
        "cos_map": base.T @ (weight * np.cos(fine)),
        "sin_map": base.T @ (weight * np.sin(fine)),
    }


def kron(count, block):
    return np.kron(np.eye(count), block)


def f32(value):
    return jnp.asarray(np.asarray(value, np.float32))


def bf16(value):
    return np.asarray(value, jnp.bfloat16)


def parts_of(value):
    high = bf16(value)
    return high, bf16(value - high.astype(np.float64))


def left_table(value):
    high, low = parts_of(value)
    return jnp.asarray(np.concatenate([high, low, high], -1))


def right_table(value):
    high, low = parts_of(value)
    upper = np.concatenate([high, low], -1)
    lower = np.concatenate([high, np.zeros_like(low)], -1)
    return jnp.asarray(np.concatenate([upper, lower], -2))


def halves(value):
    high = value.astype(jnp.bfloat16)
    return high, (value - high.astype(jnp.float32)).astype(jnp.bfloat16)


def dot(a, b, dims=((1,), (0,))):
    return lax.dot_general(a, b, (dims, ((), ())), preferred_element_type=jnp.float32)


def stacked(value):
    high, low = halves(value)
    return jnp.concatenate([high, high, low], 0)


def short_stacked(value, rows):
    high = value.astype(jnp.bfloat16).astype(jnp.float32)
    blank = jnp.zeros((rows - 3 * value.shape[0], value.shape[1]), jnp.float32)
    return jnp.concatenate([high, high, value - high, blank], 0).astype(jnp.bfloat16)


def times_right(value, table):
    out = dot(jnp.concatenate(halves(value), 1), table)
    width = out.shape[1] // 2
    return out[:, :width] + out[:, width:]


def in_vmem(value):
    return value if INTERPRET else pltpu.with_memory_space_constraint(value, pltpu.VMEM)


def call(kernel, shapes, *args, first=False, final=False):
    scalars = [a.ndim == 2 and a.size <= 16 for a in args]
    specs = [pl.BlockSpec(memory_space=pltpu.SMEM if s else pltpu.VMEM) for s in scalars]
    if not final and not INTERPRET:
        shapes = jax.tree.map(lambda s: pltpu.VMEM(s.shape, s.dtype), shapes)
    return pl.pallas_call(
        kernel,
        in_specs=specs,
        out_specs=jax.tree.map(lambda _: pl.BlockSpec(memory_space=pltpu.VMEM), shapes),
        out_shape=shapes,
        interpret=INTERPRET,
    )(*[a if s or first else in_vmem(a) for a, s in zip(args, scalars)])


def shape_of(*dims, kind=jnp.float32):
    return jax.ShapeDtypeStruct(dims, kind)


class Plan:
    def __init__(self, initial_state, drive_modes):
        _, self.levels, self.nx, self.ny = initial_state.shape
        self.windows, _, self.modes, _ = drive_modes.shape
        self.px = lax.axis_size("px")
        self.py = lax.axis_size("py")
        self.nest = lax.axis_size("nest")
        self.lanes = self.levels * self.modes
        self.half = self.levels // 2
        self.low = self.modes + EDGE
        self.sums = self.low + EDGE
        self.rows = self.sums + EDGE
        self.x = tables(self.nx * self.px, self.modes, self.windows)
        self.y = tables(self.ny * self.py, self.modes, self.windows)
        assert self.levels % 4 == 0 and self.modes * 2 == self.ny and self.nx == self.modes
        assert self.windows == 3 and self.half == 2 and EDGE * EDGE == self.modes

    def pairs(self, value):
        width = 2 * self.modes
        return jnp.concatenate([value[:, i * width : (i + 1) * width] for i in range(self.half)], 0)

    def unpairs(self, value):
        rows = value.shape[0] // self.half
        return jnp.concatenate([value[i * rows : (i + 1) * rows] for i in range(self.half)], 1)


def project(plan, state, rates):
    low, half, lanes, levels = plan.low, plan.half, plan.lanes, plan.levels
    modes, nx, ny, windows = plan.modes, plan.nx, plan.ny, plan.windows
    bases = np.concatenate([plan.x["base"], plan.x["edges"], np.zeros((nx * plan.px, EDGE))], 1)
    left = left_table(bases.T.reshape(low + EDGE, plan.px, nx).transpose(1, 0, 2))
    base_y = plan.y["base"].reshape(plan.py, ny, modes)
    edge_y = plan.y["edges"].reshape(plan.py, ny, EDGE)
    right, corner, edge = [], [], []
    for at in range(plan.py):
        high, small = parts_of(kron(2, base_y[at]))
        right.append(np.concatenate([high, small], 1))
        corner.append(bf16(kron(2, np.repeat(edge_y[at], EDGE, 1))))
        edge.append(bf16(np.pad(np.tile(edge_y[at].T, (1, 2)), ((0, EDGE), (0, 0)))))
    pick = np.zeros((2 * EDGE, 2 * ny))
    for i in range(windows):
        pick[i, [i, ny + i]] = 1
        pick[windows + i, [ny - windows + i, 2 * ny - windows + i]] = 1

    def kernel(state_ref, left_ref, right_ref, corner_ref, edge_ref, pick_ref, rates_ref, out_ref):
        px, py = lax.axis_index("px"), lax.axis_index("py")
        field = jnp.concatenate([state_ref[0, level] for level in range(levels)], 1)
        rows = dot(left_ref[px], stacked(field))
        width = 2 * ny
        both = jnp.concatenate([rows[:low, i * width : (i + 1) * width] for i in range(half)], 0)
        high, small = halves(both)
        table = right_ref[py]
        found = dot(high, table)
        found = found[:, :ny] + found[:, ny:] + dot(small, table[:, :ny])
        out_ref[:modes] = jnp.concatenate([found[i * low : i * low + modes] for i in range(half)], 1)
        ends = jnp.concatenate([found[i * low + modes : (i + 1) * low] for i in range(half)], 1)
        cells = jnp.concatenate([rows[modes:low, i * width : (i + 1) * width] for i in range(half)], 0)
        cells = dot(jnp.concatenate(halves(cells), 0), corner_ref[py])
        cells = cells[: half * EDGE] + cells[half * EDGE :]
        cells = jnp.concatenate([cells[i * EDGE : (i + 1) * EDGE] for i in range(half)], 1)
        row = lax.broadcasted_iota(jnp.int32, (EDGE, lanes), 0)
        lane = lax.broadcasted_iota(jnp.int32, (EDGE, lanes), 1)
        cells = jnp.sum(jnp.where(lane % EDGE == row, cells, 0.0), 0, keepdims=True)
        gain = jnp.zeros((EDGE, lanes), jnp.float32)
        for i in range(levels):
            gain = jnp.where(lane // modes == i, rates_ref[0, i], gain)
        gain = jnp.where((px == 0) & (py == 0), gain, 0.0)
        ends = jnp.where(row == EDGE - 1, gain, jnp.where(row == EDGE - 2, cells, ends))
        out_ref[modes:low] = ends
        upright = jnp.concatenate([rows[:modes, i * ny : (i + 1) * ny] for i in range(levels)], 0)
        upright = jnp.concatenate(halves(upright), 1)
        out_ref[low : plan.sums] = dot(edge_ref[py], upright, ((1,), (1,)))[:EDGE]
        patch = jnp.concatenate([state_ref[0, level] for level in range(levels)], 0)
        patch = jnp.concatenate(halves(patch), 1)
        out_ref[plan.sums :] = dot(pick_ref[...], patch, ((1,), (1,)))[:EDGE]

    return call(
        kernel,
        shape_of(plan.rows, lanes),
        state, left, jnp.asarray(np.stack(right)), jnp.asarray(np.stack(corner)), jnp.asarray(np.stack(edge)),
        jnp.asarray(bf16(pick)), rates,
        first=True,
    )


def facing(plan, state_ref, columns, bottom):
    rows = []
    for group in range(plan.half):
        pair = [state_ref[0, 2 * group + i] for i in range(2)]
        top = jnp.concatenate([p[: plan.windows] for p in pair], 1)
        end = jnp.concatenate([p[plan.nx - plan.windows :] for p in pair], 1)
        rows.append(jnp.where(bottom, end, top))
    lane = lax.broadcasted_iota(jnp.int32, (EDGE, plan.lanes), 1)
    moved = pltpu.roll(columns, plan.lanes - (plan.nx - plan.windows), 1)
    near = jnp.where(lane % plan.nx < plan.windows, jnp.where(bottom, moved, columns), 0.0)
    packed = near[:1]
    for i in range(1, 2 * plan.windows):
        packed = packed + pltpu.roll(near, EDGE * i, 1)[i : i + 1]
    return jnp.concatenate(rows + [packed, jnp.zeros((1, plan.lanes), jnp.float32)], 0)


def join_first(plan, own, other, state, columns):
    sums = plan.sums

    def kernel(own_ref, other_ref, state_ref, columns_ref, out_ref, next_ref):
        odd = lax.axis_index("px") % 2 == 1
        out_ref[:sums] = own_ref[:sums] + other_ref[:sums]
        out_ref[sums:] = facing(plan, state_ref, columns_ref[sums:], jnp.logical_not(odd))
        next_ref[...] = facing(plan, state_ref, columns_ref[sums:], odd)

    shapes = shape_of(plan.rows, plan.lanes), shape_of(EDGE, plan.lanes)
    return call(kernel, shapes, own, other, state, columns)


def join_second(plan, own, other, halo):
    sums = plan.sums

    def kernel(own_ref, other_ref, halo_ref, out_ref):
        out_ref[:sums] = own_ref[:sums] + other_ref[:sums]
        out_ref[sums:] = halo_ref[...]

    return call(kernel, shape_of(plan.rows, plan.lanes), own, other, halo)


def join_last(plan, own, other):
    sums = plan.sums

    def kernel(own_ref, other_ref, out_ref):
        out_ref[...] = own_ref[:sums] + other_ref[:sums]

    return call(kernel, shape_of(sums, plan.lanes), own, other)


def step_patch(plan, state, columns, got_first, got_second):
    nx, ny, windows, sums, levels = plan.nx, plan.ny, plan.windows, plan.sums, plan.levels
    place = np.zeros((4 * EDGE, ny))
    for i in range(windows):
        for part in range(3):
            place[part * EDGE + i, i] = 1
            place[part * EDGE + windows + i, ny - windows + i] = 1
    rows, lanes = nx + 2 * EDGE, 2 * ny

    def kernel(state_ref, columns_ref, first_ref, second_ref, place_ref, out_ref):
        px, py = lax.axis_index("px"), lax.axis_index("py")
        row = lax.broadcasted_iota(jnp.int32, (rows, lanes), 0) - EDGE + px * nx
        lane = lax.broadcasted_iota(jnp.int32, (rows, lanes), 1)
        lane = jnp.where(lane >= ny + ny // 2, lane - lanes, lane) + py * ny
        inside = (row >= 0) & (row < nx * plan.px) & (lane >= 0) & (lane < ny * plan.py)
        where = place_ref[...]

        def spread(block):
            high = block.astype(jnp.bfloat16).astype(jnp.float32)
            rest = block - high
            middle = rest.astype(jnp.bfloat16).astype(jnp.float32)
            parts = [high, middle, rest - middle, jnp.zeros_like(high)]
            return dot(jnp.concatenate(parts, 0).astype(jnp.bfloat16), where, ((0,), (0,)))

        small_row = lax.broadcasted_iota(jnp.int32, (EDGE, plan.lanes), 0)
        small_lane = lax.broadcasted_iota(jnp.int32, (EDGE, plan.lanes), 1)
        mine = small_lane % nx // EDGE == small_row

        def corners(block):
            line = jnp.broadcast_to(block[2 * windows : 2 * windows + 1], (EDGE, plan.lanes))
            cells = spread(jnp.where(mine, line, 0.0))
            return [
                sum(cells[level * nx + EDGE * i : level * nx + EDGE * (i + 1)] for i in range(2 * windows))
                for level in range(levels)
            ]

        even = px % 2 == 0
        one, two = first_ref[sums:], second_ref[sums:]
        above, below = jnp.where(even, two, one), jnp.where(even, one, two)
        beside = spread(columns_ref[sums:])
        beside_above, beside_below = corners(above), corners(below)
        blank = jnp.zeros((EDGE - windows, lanes), jnp.float32)
        for level in range(levels):
            pair, part = level // 2, level % 2

            def line(block):
                return block[pair * windows : (pair + 1) * windows, part * ny : (part + 1) * ny]

            up = jnp.concatenate([line(above), beside_above[level][:windows]], 1)
            down = jnp.concatenate([line(below), beside_below[level][:windows]], 1)
            middle = jnp.concatenate([state_ref[0, level], beside[level * nx : (level + 1) * nx]], 1)
            field = jnp.concatenate([blank, up, middle, down, blank], 0)
            field = jnp.where(inside, field, 0.0)
            for _ in range(windows):
                around = (
                    pltpu.roll(field, 1, 0)
                    + pltpu.roll(field, rows - 1, 0)
                    + pltpu.roll(field, 1, 1)
                    + pltpu.roll(field, lanes - 1, 1)
                )
                field = jnp.where(inside, field + RATE * (around - 4.0 * field), 0.0)
            out_ref[level] = field[EDGE : EDGE + nx, :ny]

    return call(
        kernel, shape_of(levels, nx, ny), state, columns, got_first, got_second, jnp.asarray(bf16(place))
    )


def prepare(plan, drive, nest_offsets):
    modes, lanes, levels, windows = plan.modes, plan.lanes, plan.levels, plan.windows
    nx, ny, x, y = plan.nx, plan.ny, plan.x, plan.y
    steps = plan.nest - 1
    maps_x = f32(np.stack([np.tile(x[name], (1, 2)) for name in ("cos_map", "sin_map")]))
    maps_y = f32(np.stack([kron(2, y[name].T) for name in ("cos_map", "sin_map")]))
    rows_x = np.stack([np.tile(p, (1, 2)).reshape(plan.px, nx, 2 * modes) for p in x["powers"][:windows]], 1)
    rows_y = np.stack(
        [p.reshape(plan.py, ny, modes).transpose(0, 2, 1) for p in y["powers"][:windows]], 1
    )

    def kernel(
        drive_ref, maps_x_ref, maps_y_ref, rows_x_ref, rows_y_ref, offsets_ref,
        drive_out, row_out, col_out, spread_x_out, spread_y_out,
    ):
        nest, px, py = lax.axis_index("nest"), lax.axis_index("px"), lax.axis_index("py")
        for w in range(windows):
            drive_out[w] = jnp.concatenate([drive_ref[w, level] for level in range(levels)], 1)
        lane = lax.broadcasted_iota(jnp.int32, (modes, 2 * modes), 1)

        def as_left(twice):
            rounded = twice.astype(jnp.bfloat16).astype(jnp.float32)
            pair = jnp.where(lane >= modes, twice - rounded, rounded)
            return jnp.concatenate([pair, rounded], 1)[:, : 3 * modes].astype(jnp.bfloat16)

        def angle(mode, offset, cells):
            turn = (mode * offset).astype(jnp.float32)
            turn = turn - jnp.floor(turn / (2.0 * cells)) * (2.0 * cells)
            return turn * (math.pi / cells)

        mode = lax.broadcasted_iota(jnp.int32, (EDGE, 2 * modes), 1) % modes
        row = lax.broadcasted_iota(jnp.int32, (EDGE, 2 * modes), 0)
        upright = lax.broadcasted_iota(jnp.int32, (2 * modes, 2 * modes), 0) % modes
        place = lax.broadcasted_iota(jnp.int32, (2 * modes, 2 * modes), 1)
        along, down = jnp.zeros_like(mode), jnp.zeros_like(upright)
        for slot in range(steps):
            domain = jnp.maximum(nest - slot, 0)
            along = jnp.where(row == slot, offsets_ref[domain, 0], along)
            down = jnp.where(place == slot, offsets_ref[domain, 1], down)
        along = angle(mode, along, nx * plan.px)
        down = angle(upright, down, ny * plan.py)
        cos_x, sin_x = jnp.cos(along), jnp.sin(along)
        cos_y, sin_y = jnp.cos(down), jnp.sin(down)
        for slot in range(steps):
            at = slice(slot, slot + 1)
            row_out[slot] = as_left(maps_x_ref[0] * cos_x[at] - maps_x_ref[1] * sin_x[at])
            col_map = maps_y_ref[0] * cos_y[:, at] - maps_y_ref[1] * sin_y[:, at]
            high, small = halves(col_map)
            upper = jnp.concatenate([high, small], 1)
            lower = jnp.concatenate([high, jnp.zeros_like(high)], 1)
            col_out[slot] = jnp.concatenate([upper, lower], 0)
        for w in range(windows):
            p = windows - 1 - w
            for j in range(windows):
                if j <= p:
                    combined = sum(multinomial(p, i, j) * rows_x_ref[px, i] for i in range(p - j + 1))
                    spread_x_out[w, j * nx : (j + 1) * nx] = as_left(combined)
                else:
                    spread_x_out[w, j * nx : (j + 1) * nx] = jnp.zeros((nx, 3 * modes), jnp.bfloat16)
        for j in range(windows):
            table = rows_y_ref[py, j]
            blank = jnp.zeros_like(table)
            table = jnp.concatenate(
                [jnp.concatenate([table, blank], 1), jnp.concatenate([blank, table], 1)], 0
            )
            high, small = halves(table)
            spread_y_out[j] = jnp.concatenate([high, high, small], 0)

    shapes = (
        shape_of(windows, modes, lanes),
        shape_of(steps, modes, 3 * modes, kind=jnp.bfloat16),
        shape_of(steps, 4 * modes, 4 * modes, kind=jnp.bfloat16),
        shape_of(windows, windows * nx, 3 * modes, kind=jnp.bfloat16),
        shape_of(windows, 6 * modes, 2 * ny, kind=jnp.bfloat16),
    )
    return call(kernel, shapes, drive, maps_x, maps_y, f32(rows_x), f32(rows_y), nest_offsets, first=True)


def nudge(plan, stepped, gathered, prepared):
    modes, low, lanes, levels = plan.modes, plan.low, plan.lanes, plan.levels
    windows, half, nx, ny = plan.windows, plan.half, plan.nx, plan.ny
    x, y, sums = plan.x, plan.y, plan.sums
    pairs, unpairs = plan.pairs, plan.unpairs

    inward = np.concatenate([np.tile(y["spill"][j].T, (1, 2)) for j in range(1, windows + 1)], 1)
    high, small = parts_of(inward)
    inward = jnp.asarray(np.concatenate([high, small, high, np.zeros_like(high)], 0))
    corner = np.concatenate(
        [kron(2, np.repeat(y["spill"][j].T, EDGE, 0)) for j in range(1, windows + 1)], 1
    )
    high, small = parts_of(corner)
    corner = jnp.asarray(np.concatenate([high, high, small], 0))
    across = np.zeros((windows * modes, windows * EDGE))
    for n in range(1, windows + 1):
        for j in range(n):
            across[(n - 1) * modes : n * modes, j * EDGE : (j + 1) * EDGE] = sum(
                multinomial(n, i, j) * x["spill"][i] for i in range(1, n - j + 1)
            )
    high, small = parts_of(across)
    across = jnp.asarray(np.pad(np.concatenate([high, small, high], 1), ((0, 0), (0, 3 * EDGE))))
    scale_x = f32(np.broadcast_to(1.0 + x["factor"][:, None], (modes, lanes)))
    scale_y = f32(np.broadcast_to(np.tile(y["factor"], levels), (EDGE, lanes)))
    again = []
    for p in range(1, windows):
        again.append(sum(multinomial(p, i, 0) * x["within"][i] for i in range(p + 1)))
    again = left_table(np.concatenate(again, 0))
    sideways = jnp.stack([right_table(kron(2, y["within"][j])) for j in range(1, windows)])
    drive, row_maps, col_maps, spread_x, spread_y = prepared

    def kernel(
        stepped_ref, drive_ref, row_ref, col_ref, spread_x_ref, spread_y_ref, inward_ref, corner_ref,
        across_ref, scale_x_ref, scale_y_ref, again_ref, sideways_ref, *refs,
    ):
        slots, (state_ref, modes_ref) = refs[:-2], refs[-2:]
        root = plan.nest - 1
        nest = lax.axis_index("nest")
        scale_x, scale_y = scale_x_ref[...], scale_y_ref[:1]
        row = lax.broadcasted_iota(jnp.int32, (EDGE, lanes), 0)
        lane = lax.broadcasted_iota(jnp.int32, (EDGE, lanes), 1)
        mine = lane % EDGE == row
        left_lane = lax.broadcasted_iota(jnp.int32, (modes, ny), 1) < modes

        def own_modes(ref):
            rows, ends = ref[:modes], ref[modes:low]
            sides = dot(short_stacked(ref[low:sums], 4 * EDGE), inward_ref[...], ((0,), (0,)))
            cells = jnp.where(mine, jnp.broadcast_to(ends[EDGE - 2 : EDGE - 1], (EDGE, lanes)), 0.0)
            cells = jnp.concatenate([cells[:, i * ny : (i + 1) * ny] for i in range(half)], 0)
            high, small = halves(cells)
            cells = dot(jnp.concatenate([high, small, high], 1), corner_ref[...])
            turned, ends = [rows], [ends]
            for j in range(windows):
                at = slice(j * ny, (j + 1) * ny)
                side = [
                    jnp.where(
                        left_lane,
                        sides[2 * i * modes : (2 * i + 1) * modes, at],
                        sides[(2 * i + 1) * modes : (2 * i + 2) * modes, at],
                    )
                    for i in range(half)
                ]
                cell = [cells[i * EDGE : (i + 1) * EDGE, at] for i in range(half)]
                power = scale_y if j == 0 else power * scale_y
                turned.append(rows * power + jnp.concatenate(side, 1))
                ends.append(ends[0] * power + jnp.concatenate(cell, 1))
            over = dot(across_ref[...], short_stacked(jnp.concatenate(ends[:windows], 0), 12 * EDGE))
            result = []
            for n in range(windows):
                turned = [a * scale_x + b for a, b in zip(turned[:-1], turned[1:])]
                result.append(turned[0] + over[n * modes : (n + 1) * modes])
            return result

        def carried(change, count):
            left = dot(again_ref[: count * modes], stacked(change))
            left = [left[i * modes : (i + 1) * modes] for i in range(count)]
            if count == 1:
                return [left[0] + unpairs(times_right(pairs(change), sideways_ref[0]))]
            both = jnp.concatenate([pairs(change), pairs(left[0])], 0)
            once = times_right(both, sideways_ref[0])
            twice = times_right(pairs(change), sideways_ref[1])
            rows = half * modes
            return [left[0] + unpairs(once[:rows]), left[1] + unpairs(2.0 * once[rows:] + twice)]

        owns = [own_modes(ref) for ref in slots]
        coeffs = None
        for slot in range(root, -1, -1):
            gain = slots[slot][low - 1 : low]
            own = owns[slot]
            new, changes, later = [], [], []
            for w in range(windows):
                target = drive_ref[w]
                if slot < root:
                    inner = unpairs(times_right(pairs(coeffs[w]), col_ref[slot]))
                    target = jnp.where(nest <= slot, target, dot(row_ref[slot], stacked(inner)))
                before = own[w]
                for v in range(w):
                    before = before + later[v][w - v - 1]
                change = gain * (target - before)
                if w < windows - 1:
                    later.append(carried(change, windows - 1 - w))
                changes.append(change)
                new.append(before + change)
            coeffs = new
        for level in range(levels):
            modes_ref[0, level] = coeffs[-1][:, level * modes : (level + 1) * modes]
        spread = sum(dot(spread_x_ref[w], stacked(changes[w])) for w in range(windows))
        field = 0.0
        for j in range(windows):
            high, small = halves(pairs(spread[j * nx : (j + 1) * nx]))
            field = field + dot(jnp.concatenate([high, small, high], 1), spread_y_ref[j])
        for level in range(levels):
            at_row, at = level // 2 * nx, level % 2 * ny
            state_ref[0, level] = stepped_ref[level] + field[at_row : at_row + nx, at : at + ny]

    return call(
        kernel,
        (shape_of(1, levels, nx, ny), shape_of(1, levels, modes, modes)),
        stepped, drive, row_maps, col_maps, spread_x, spread_y, inward, corner, across, scale_x, scale_y,
        again, sideways, *gathered,
        final=True,
    )


def swap(value, axis, partner):
    size = lax.axis_size(axis)
    return lax.ppermute(value, axis, [(i, partner(i)) for i in range(size) if 0 <= partner(i) < size])


def body(initial_state, drive_modes, relax_rates, nest_offsets):
    plan = Plan(initial_state, drive_modes)
    share = project(plan, initial_state, relax_rates)
    if plan.py == 2 and plan.px == 4:
        columns = swap(share, "py", lambda i: i ^ 1)
        first, halo = join_first(plan, share, columns, initial_state, columns)
        got_first = swap(first, "px", lambda i: i ^ 1)
        second = join_second(plan, first, got_first, halo)
        second, drive_modes, nest_offsets = lax.optimization_barrier((second, drive_modes, nest_offsets))
        got_second = swap(second, "px", lambda i: i ^ 3)
        prepared = prepare(plan, drive_modes, nest_offsets)
        got_second, prepared = lax.optimization_barrier((got_second, prepared))
        last = join_last(plan, second, got_second)
    else:
        from_right = jnp.arange(plan.rows)[:, None] < plan.sums + plan.windows
        right = swap(share, "py", lambda i: i - 1)
        left = swap(share, "py", lambda i: i + 1)
        columns = jnp.where(from_right, right, left)
        blank = jnp.zeros_like(share)
        first, halo = join_first(plan, share, blank, initial_state, columns)
        second = join_second(plan, first, blank, halo)
        even = lax.axis_index("px") % 2 == 0
        above = swap(jnp.where(even, first, second), "px", lambda i: i + 1)
        below = swap(jnp.where(even, second, first), "px", lambda i: i - 1)
        got_first, got_second = jnp.where(even, below, above), jnp.where(even, above, below)
        total = lax.psum(share[: plan.sums], ("py", "px"))
        last = join_last(plan, total, jnp.zeros_like(total))
        prepared = prepare(plan, drive_modes, nest_offsets)
    gathered = [last] + [swap(last, "nest", lambda i, s=s: i + s) for s in range(1, plan.nest)]
    stepped = step_patch(plan, initial_state, columns, got_first, got_second)
    return nudge(plan, stepped, gathered, prepared)


def solution(mesh):
    return jax.shard_map(
        body,
        mesh=mesh,
        in_specs=(P("nest", None, "px", "py"), P(), P("nest", None), P()),
        out_specs=(P("nest", None, "px", "py"), P("nest", None, None, None)),
        check_vma=False,
    )
```

```python
import functools
import math

import jax
import jax.numpy as jnp
import numpy as np
from jax import lax
from jax.experimental import pallas as pl
from jax.experimental.pallas import tpu as pltpu
from jax.sharding import PartitionSpec as P

RATIO = 3
RATE = 0.2
EDGE = 8
INTERPRET = False


def multinomial(n, i, j):
    return math.factorial(n) // (math.factorial(i) * math.factorial(j) * math.factorial(n - i - j))


@functools.lru_cache(maxsize=None)
def tables(cells, modes, order):
    cell = np.arange(cells)
    mode = np.arange(modes)
    weight = np.sqrt(np.where(mode == 0, 1.0, 2.0) / cells)
    product = mode[None] * (2 * cell[:, None] + 1)
    coarse = np.pi * (product % (4 * cells)) / (2 * cells)
    fine = np.pi * (product % (4 * RATIO * cells)) / (2 * RATIO * cells)
    base = weight * np.cos(coarse)
    second = RATE * (np.eye(cells, k=1) + np.eye(cells, k=-1) - 2 * np.eye(cells))
    powers = [base]
    for _ in range(order):
        powers.append(second @ powers[-1])
    factor = RATE * (2 * np.cos(np.pi * mode / cells) - 2)
    places = list(range(order)) + list(range(cells - order, cells))
    edges = np.zeros((cells, EDGE))
    edges[places, range(2 * order)] = 1
    spill = [(powers[i] - base * factor**i).T @ edges for i in range(order + 1)]
    return {
        "base": base,
        "edges": edges,
        "powers": powers,
        "factor": factor,
        "spill": spill,
        "within": [base.T @ power for power in powers],
        "cos_map": base.T @ (weight * np.cos(fine)),
        "sin_map": base.T @ (weight * np.sin(fine)),
    }


def kron(count, block):
    return np.kron(np.eye(count), block)


def f32(value):
    return jnp.asarray(np.asarray(value, np.float32))


def bf16(value):
    return np.asarray(value, jnp.bfloat16)


def parts_of(value):
    high = bf16(value)
    return high, bf16(value - high.astype(np.float64))


def left_table(value):
    high, low = parts_of(value)
    return jnp.asarray(np.concatenate([high, low, high], -1))


def right_table(value):
    high, low = parts_of(value)
    upper = np.concatenate([high, low], -1)
    lower = np.concatenate([high, np.zeros_like(low)], -1)
    return jnp.asarray(np.concatenate([upper, lower], -2))


def halves(value):
    high = value.astype(jnp.bfloat16)
    return high, (value - high.astype(jnp.float32)).astype(jnp.bfloat16)


def dot(a, b, dims=((1,), (0,))):
    return lax.dot_general(a, b, (dims, ((), ())), preferred_element_type=jnp.float32)


def stacked(value):
    high, low = halves(value)
    return jnp.concatenate([high, high, low], 0)


def short_stacked(value, rows):
    high = value.astype(jnp.bfloat16).astype(jnp.float32)
    blank = jnp.zeros((rows - 3 * value.shape[0], value.shape[1]), jnp.float32)
    return jnp.concatenate([high, high, value - high, blank], 0).astype(jnp.bfloat16)


def times_right(value, table):
    out = dot(jnp.concatenate(halves(value), 1), table)
    width = out.shape[1] // 2
    return out[:, :width] + out[:, width:]


def by_parts(value, table, rest):
    high, low = halves(value)
    out = dot(jnp.concatenate([high, low], 0), table)
    return out[: value.shape[0]] + out[value.shape[0] :] + dot(high, rest)


def in_vmem(value):
    return value if INTERPRET else pltpu.with_memory_space_constraint(value, pltpu.VMEM)


def call(kernel, shapes, *args, first=False, final=False):
    scalars = [a.ndim == 2 and a.size <= 16 for a in args]
    specs = [pl.BlockSpec(memory_space=pltpu.SMEM if s else pltpu.VMEM) for s in scalars]
    if not final and not INTERPRET:
        shapes = jax.tree.map(lambda s: pltpu.VMEM(s.shape, s.dtype), shapes)
    return pl.pallas_call(
        kernel,
        in_specs=specs,
        out_specs=jax.tree.map(lambda _: pl.BlockSpec(memory_space=pltpu.VMEM), shapes),
        out_shape=shapes,
        interpret=INTERPRET,
    )(*[a if s or first else in_vmem(a) for a, s in zip(args, scalars)])


def shape_of(*dims, kind=jnp.float32):
    return jax.ShapeDtypeStruct(dims, kind)


class Plan:
    def __init__(self, initial_state, drive_modes):
        _, self.levels, self.nx, self.ny = initial_state.shape
        self.windows, _, self.modes, _ = drive_modes.shape
        self.px = lax.axis_size("px")
        self.py = lax.axis_size("py")
        self.nest = lax.axis_size("nest")
        self.lanes = self.levels * self.modes
        self.half = self.levels // 2
        self.low = self.modes + EDGE
        self.sums = self.low + EDGE
        self.rows = self.sums + EDGE
        self.x = tables(self.nx * self.px, self.modes, self.windows)
        self.y = tables(self.ny * self.py, self.modes, self.windows)
        assert self.levels % 4 == 0 and self.modes * 2 == self.ny and self.nx == self.modes
        assert self.windows == 3 and self.half == 2 and EDGE * EDGE == self.modes

    def pairs(self, value):
        width = 2 * self.modes
        return jnp.concatenate([value[:, i * width : (i + 1) * width] for i in range(self.half)], 0)

    def unpairs(self, value):
        rows = value.shape[0] // self.half
        return jnp.concatenate([value[i * rows : (i + 1) * rows] for i in range(self.half)], 1)


def project(plan, state, rates):
    low, half, lanes, levels = plan.low, plan.half, plan.lanes, plan.levels
    modes, nx, ny, windows = plan.modes, plan.nx, plan.ny, plan.windows
    bases = np.concatenate([plan.x["base"], plan.x["edges"], np.zeros((nx * plan.px, EDGE))], 1)
    left = left_table(bases.T.reshape(low + EDGE, plan.px, nx).transpose(1, 0, 2))
    base_y = plan.y["base"].reshape(plan.py, ny, modes)
    edge_y = plan.y["edges"].reshape(plan.py, ny, EDGE)
    right, corner, edge = [], [], []
    for at in range(plan.py):
        high, small = parts_of(kron(2, base_y[at]))
        right.append(np.concatenate([high, small], 1))
        corner.append(bf16(kron(2, np.repeat(edge_y[at], EDGE, 1))))
        edge.append(bf16(np.pad(np.tile(edge_y[at].T, (1, 2)), ((0, EDGE), (0, 0)))))
    pick = np.zeros((2 * EDGE, 2 * ny))
    for i in range(windows):
        pick[i, [i, ny + i]] = 1
        pick[windows + i, [ny - windows + i, 2 * ny - windows + i]] = 1

    def kernel(state_ref, left_ref, right_ref, corner_ref, edge_ref, pick_ref, rates_ref, out_ref, along_ref):
        px, py = lax.axis_index("px"), lax.axis_index("py")
        field = jnp.concatenate([state_ref[0, level] for level in range(levels)], 1)
        rows = dot(left_ref[px], stacked(field))
        width = 2 * ny
        both = jnp.concatenate([rows[:low, i * width : (i + 1) * width] for i in range(half)], 0)
        high, small = halves(both)
        table = right_ref[py]
        found = dot(high, table)
        found = found[:, :ny] + found[:, ny:] + dot(small, table[:, :ny])
        out_ref[:modes] = jnp.concatenate([found[i * low : i * low + modes] for i in range(half)], 1)
        ends = jnp.concatenate([found[i * low + modes : (i + 1) * low] for i in range(half)], 1)
        cells = jnp.concatenate([rows[modes:low, i * width : (i + 1) * width] for i in range(half)], 0)
        cells = dot(jnp.concatenate(halves(cells), 0), corner_ref[py])
        cells = cells[: half * EDGE] + cells[half * EDGE :]
        cells = jnp.concatenate([cells[i * EDGE : (i + 1) * EDGE] for i in range(half)], 1)
        row = lax.broadcasted_iota(jnp.int32, (EDGE, lanes), 0)
        lane = lax.broadcasted_iota(jnp.int32, (EDGE, lanes), 1)
        cells = jnp.sum(jnp.where(lane % EDGE == row, cells, 0.0), 0, keepdims=True)
        gain = jnp.zeros((EDGE, lanes), jnp.float32)
        for i in range(levels):
            gain = jnp.where(lane // modes == i, rates_ref[0, i], gain)
        gain = jnp.where((px == 0) & (py == 0), gain, 0.0)
        ends = jnp.where(row == EDGE - 1, gain, jnp.where(row == EDGE - 2, cells, ends))
        out_ref[modes:low] = ends
        upright = jnp.concatenate([rows[:modes, i * ny : (i + 1) * ny] for i in range(levels)], 0)
        upright = jnp.concatenate(halves(upright), 1)
        out_ref[low : plan.sums] = dot(edge_ref[py], upright, ((1,), (1,)))[:EDGE]
        patch = jnp.concatenate([state_ref[0, level] for level in range(levels)], 0)
        patch = jnp.concatenate(halves(patch), 1)
        out_ref[plan.sums :] = dot(pick_ref[...], patch, ((1,), (1,)))[:EDGE]
        along_ref[: plan.sums] = out_ref[: plan.sums]
        lines = facing_rows(plan, state_ref, px % 2 == 0)
        along_ref[plan.sums :] = jnp.concatenate([lines, jnp.zeros((2, lanes), jnp.float32)], 0)

    return call(
        kernel,
        (shape_of(plan.rows, lanes), shape_of(plan.rows, lanes)),
        state, left, jnp.asarray(np.stack(right)), jnp.asarray(np.stack(corner)), jnp.asarray(np.stack(edge)),
        jnp.asarray(bf16(pick)), rates,
        first=True,
    )


def facing_rows(plan, state_ref, bottom):
    rows = []
    for group in range(plan.half):
        pair = [state_ref[0, 2 * group + i] for i in range(2)]
        top = jnp.concatenate([p[: plan.windows] for p in pair], 1)
        end = jnp.concatenate([p[plan.nx - plan.windows :] for p in pair], 1)
        rows.append(jnp.where(bottom, end, top))
    return jnp.concatenate(rows, 0)


def facing_corners(plan, columns, bottom):
    lane = lax.broadcasted_iota(jnp.int32, (EDGE, plan.lanes), 1)
    moved = pltpu.roll(columns, plan.lanes - (plan.nx - plan.windows), 1)
    near = jnp.where(lane % plan.nx < plan.windows, jnp.where(bottom, moved, columns), 0.0)
    packed = near[:1]
    for i in range(1, 2 * plan.windows):
        packed = packed + pltpu.roll(near, EDGE * i, 1)[i : i + 1]
    return jnp.concatenate([packed, jnp.zeros((1, plan.lanes), jnp.float32)], 0)


def join_first(plan, own, from_y, from_x, from_both, state):
    sums, windows = plan.sums, plan.windows

    def kernel(own_ref, y_ref, x_ref, both_ref, state_ref, out_ref, halo_ref):
        odd = lax.axis_index("px") % 2 == 1
        out_ref[:sums] = (own_ref[:sums] + y_ref[:sums]) + (x_ref[:sums] + both_ref[:sums])
        corners = facing_corners(plan, y_ref[sums:], odd)
        out_ref[sums:] = jnp.concatenate([facing_rows(plan, state_ref, odd), corners], 0)
        corners = facing_corners(plan, both_ref[sums:], odd)
        halo_ref[...] = jnp.concatenate([x_ref[sums : sums + 2 * windows], corners], 0)

    shapes = shape_of(plan.rows, plan.lanes), shape_of(EDGE, plan.lanes)
    return call(kernel, shapes, own, from_y, from_x, from_both, state)


def both_facing(plan, state, columns):
    def kernel(state_ref, columns_ref, top_ref, bottom_ref):
        columns = columns_ref[plan.sums :]
        for ref, bottom in ((top_ref, False), (bottom_ref, True)):
            rows = [facing_rows(plan, state_ref, bottom), facing_corners(plan, columns, bottom)]
            ref[...] = jnp.concatenate(rows, 0)

    return call(kernel, (shape_of(EDGE, plan.lanes),) * 2, state, columns)


def join_last(plan, own, other):
    sums = plan.sums

    def kernel(own_ref, other_ref, out_ref):
        out_ref[...] = own_ref[:sums] + other_ref[:sums]

    return call(kernel, shape_of(sums, plan.lanes), own, other)


def step_patch(plan, state, columns, first, second):
    nx, ny, windows, sums, levels = plan.nx, plan.ny, plan.windows, plan.sums, plan.levels
    place = np.zeros((4 * EDGE, ny))
    for i in range(windows):
        for part in range(3):
            place[part * EDGE + i, i] = 1
            place[part * EDGE + windows + i, ny - windows + i] = 1
    rows, lanes = nx + 2 * EDGE, 2 * ny

    def kernel(state_ref, columns_ref, first_ref, second_ref, place_ref, out_ref):
        px, py = lax.axis_index("px"), lax.axis_index("py")
        row = lax.broadcasted_iota(jnp.int32, (rows, lanes), 0) - EDGE + px * nx
        lane = lax.broadcasted_iota(jnp.int32, (rows, lanes), 1)
        lane = jnp.where(lane >= ny + ny // 2, lane - lanes, lane) + py * ny
        inside = (row >= 0) & (row < nx * plan.px) & (lane >= 0) & (lane < ny * plan.py)
        where = place_ref[...]

        def spread(block):
            high = block.astype(jnp.bfloat16).astype(jnp.float32)
            rest = block - high
            middle = rest.astype(jnp.bfloat16).astype(jnp.float32)
            parts = [high, middle, rest - middle, jnp.zeros_like(high)]
            return dot(jnp.concatenate(parts, 0).astype(jnp.bfloat16), where, ((0,), (0,)))

        small_row = lax.broadcasted_iota(jnp.int32, (EDGE, plan.lanes), 0)
        small_lane = lax.broadcasted_iota(jnp.int32, (EDGE, plan.lanes), 1)
        mine = small_lane % nx // EDGE == small_row

        def corners(block):
            line = jnp.broadcast_to(block[2 * windows : 2 * windows + 1], (EDGE, plan.lanes))
            cells = spread(jnp.where(mine, line, 0.0))
            return [
                sum(cells[level * nx + EDGE * i : level * nx + EDGE * (i + 1)] for i in range(2 * windows))
                for level in range(levels)
            ]

        even = px % 2 == 0
        one, two = first_ref[...], second_ref[second_ref.shape[0] - EDGE :]
        above, below = jnp.where(even, two, one), jnp.where(even, one, two)
        beside = spread(columns_ref[sums:])
        beside_above, beside_below = corners(above), corners(below)
        blank = jnp.zeros((EDGE - windows, lanes), jnp.float32)
        for level in range(levels):
            pair, part = level // 2, level % 2

            def line(block):
                return block[pair * windows : (pair + 1) * windows, part * ny : (part + 1) * ny]

            up = jnp.concatenate([line(above), beside_above[level][:windows]], 1)
            down = jnp.concatenate([line(below), beside_below[level][:windows]], 1)
            middle = jnp.concatenate([state_ref[0, level], beside[level * nx : (level + 1) * nx]], 1)
            field = jnp.concatenate([blank, up, middle, down, blank], 0)
            field = jnp.where(inside, field, 0.0)
            for _ in range(windows):
                around = (
                    pltpu.roll(field, 1, 0)
                    + pltpu.roll(field, rows - 1, 0)
                    + pltpu.roll(field, 1, 1)
                    + pltpu.roll(field, lanes - 1, 1)
                )
                field = jnp.where(inside, field + RATE * (around - 4.0 * field), 0.0)
            out_ref[level] = field[EDGE : EDGE + nx, :ny]

    return call(
        kernel, shape_of(levels, nx, ny), state, columns, first, second, jnp.asarray(bf16(place))
    )


def prepare(plan, drive, nest_offsets):
    modes, lanes, levels, windows = plan.modes, plan.lanes, plan.levels, plan.windows
    nx, ny, x, y = plan.nx, plan.ny, plan.x, plan.y
    steps = plan.nest - 1
    maps_x = f32(np.stack([np.tile(x[name], (1, 2)) for name in ("cos_map", "sin_map")]))
    maps_y = f32(np.stack([kron(2, y[name].T) for name in ("cos_map", "sin_map")]))
    rows_x = np.stack([np.tile(p, (1, 2)).reshape(plan.px, nx, 2 * modes) for p in x["powers"][:windows]], 1)
    rows_y = np.stack(
        [p.reshape(plan.py, ny, modes).transpose(0, 2, 1) for p in y["powers"][:windows]], 1
    )

    def kernel(
        drive_ref, maps_x_ref, maps_y_ref, rows_x_ref, rows_y_ref, offsets_ref,
        drive_out, row_out, col_out, spread_x_out, spread_y_out,
    ):
        nest, px, py = lax.axis_index("nest"), lax.axis_index("px"), lax.axis_index("py")
        for w in range(windows):
            drive_out[w] = jnp.concatenate([drive_ref[w, level] for level in range(levels)], 1)
        lane = lax.broadcasted_iota(jnp.int32, (modes, 2 * modes), 1)

        def as_left(twice):
            rounded = twice.astype(jnp.bfloat16).astype(jnp.float32)
            pair = jnp.where(lane >= modes, twice - rounded, rounded)
            return jnp.concatenate([pair, rounded], 1)[:, : 3 * modes].astype(jnp.bfloat16)

        def angle(mode, offset, cells):
            turn = (mode * offset).astype(jnp.float32)
            turn = turn - jnp.floor(turn / (2.0 * cells)) * (2.0 * cells)
            return turn * (math.pi / cells)

        mode = lax.broadcasted_iota(jnp.int32, (EDGE, 2 * modes), 1) % modes
        row = lax.broadcasted_iota(jnp.int32, (EDGE, 2 * modes), 0)
        upright = lax.broadcasted_iota(jnp.int32, (2 * modes, 2 * modes), 0) % modes
        place = lax.broadcasted_iota(jnp.int32, (2 * modes, 2 * modes), 1)
        along, down = jnp.zeros_like(mode), jnp.zeros_like(upright)
        for slot in range(steps):
            domain = jnp.maximum(nest - slot, 0)
            along = jnp.where(row == slot, offsets_ref[0, domain], along)
            down = jnp.where(place == slot, offsets_ref[1, domain], down)
        along = angle(mode, along, nx * plan.px)
        down = angle(upright, down, ny * plan.py)
        cos_x, sin_x = jnp.cos(along), jnp.sin(along)
        cos_y, sin_y = jnp.cos(down), jnp.sin(down)
        for slot in range(steps):
            at = slice(slot, slot + 1)
            row_out[slot] = as_left(maps_x_ref[0] * cos_x[at] - maps_x_ref[1] * sin_x[at])
            col_map = maps_y_ref[0] * cos_y[:, at] - maps_y_ref[1] * sin_y[:, at]
            high, small = halves(col_map)
            upper = jnp.concatenate([high, small], 1)
            lower = jnp.concatenate([high, jnp.zeros_like(high)], 1)
            col_out[slot] = jnp.concatenate([upper, lower], 0)
        for w in range(windows):
            p = windows - 1 - w
            for j in range(windows):
                if j <= p:
                    combined = sum(multinomial(p, i, j) * rows_x_ref[px, i] for i in range(p - j + 1))
                    spread_x_out[w, j * nx : (j + 1) * nx] = as_left(combined)
                else:
                    spread_x_out[w, j * nx : (j + 1) * nx] = jnp.zeros((nx, 3 * modes), jnp.bfloat16)
        for j in range(windows):
            table = rows_y_ref[py, j]
            blank = jnp.zeros_like(table)
            table = jnp.concatenate(
                [jnp.concatenate([table, blank], 1), jnp.concatenate([blank, table], 1)], 0
            )
            high, small = halves(table)
            spread_y_out[j] = jnp.concatenate([high, small], 0)

    shapes = (
        shape_of(windows, modes, lanes),
        shape_of(steps, modes, 3 * modes, kind=jnp.bfloat16),
        shape_of(steps, 4 * modes, 4 * modes, kind=jnp.bfloat16),
        shape_of(windows, windows * nx, 3 * modes, kind=jnp.bfloat16),
        shape_of(windows, 4 * modes, 2 * ny, kind=jnp.bfloat16),
    )
    return call(kernel, shapes, drive, maps_x, maps_y, f32(rows_x), f32(rows_y), nest_offsets.T, first=True)


def nudge(plan, stepped, gathered, crossed, prepared):
    modes, low, lanes, levels = plan.modes, plan.low, plan.lanes, plan.levels
    windows, half, nx, ny = plan.windows, plan.half, plan.nx, plan.ny
    x, y, sums = plan.x, plan.y, plan.sums
    pairs, unpairs = plan.pairs, plan.unpairs

    inward = np.concatenate([np.tile(y["spill"][j].T, (1, 2)) for j in range(1, windows + 1)], 1)
    high, small = parts_of(inward)
    inward = jnp.asarray(np.concatenate([high, small, high, np.zeros_like(high)], 0))
    corner = np.concatenate(
        [kron(2, np.repeat(y["spill"][j].T, EDGE, 0)) for j in range(1, windows + 1)], 1
    )
    high, small = parts_of(corner)
    corner = jnp.asarray(np.concatenate([high, small], 0))
    across = np.zeros((windows * modes, windows * EDGE))
    for n in range(1, windows + 1):
        for j in range(n):
            across[(n - 1) * modes : n * modes, j * EDGE : (j + 1) * EDGE] = sum(
                multinomial(n, i, j) * x["spill"][i] for i in range(1, n - j + 1)
            )
    high, small = parts_of(across)
    across = jnp.asarray(np.pad(np.concatenate([high, small, high], 1), ((0, 0), (0, 3 * EDGE))))
    scale_x = f32(np.broadcast_to(1.0 + x["factor"][:, None], (modes, lanes)))
    scale_y = f32(np.broadcast_to(np.tile(y["factor"], levels), (EDGE, lanes)))
    again = []
    for p in range(1, windows):
        again.append(sum(multinomial(p, i, 0) * x["within"][i] for i in range(p + 1)))
    again = left_table(np.concatenate(again, 0))
    sideways = jnp.stack([right_table(kron(2, y["within"][j])) for j in range(1, windows)])
    drive, row_maps, col_maps, spread_x, spread_y = prepared

    def kernel(
        stepped_ref, drive_ref, row_ref, col_ref, spread_x_ref, spread_y_ref, inward_ref, corner_ref,
        across_ref, scale_x_ref, scale_y_ref, again_ref, sideways_ref, *refs,
    ):
        refs, (state_ref, modes_ref) = refs[:-2], refs[-2:]
        root = plan.nest - 1
        nest = lax.axis_index("nest")
        slots = [ref[...] for ref in refs]
        if crossed:
            slots = [slots[0], jnp.where(nest % 2 == 1, slots[2], slots[3]), slots[1], slots[3]]
        scale_x, scale_y = scale_x_ref[...], scale_y_ref[:1]
        row = lax.broadcasted_iota(jnp.int32, (EDGE, lanes), 0)
        lane = lax.broadcasted_iota(jnp.int32, (EDGE, lanes), 1)
        mine = lane % EDGE == row
        left_lane = lax.broadcasted_iota(jnp.int32, (modes, ny), 1) < modes

        def own_modes(message):
            rows, ends = message[:modes], message[modes:low]
            sides = dot(short_stacked(message[low:sums], 4 * EDGE), inward_ref[...], ((0,), (0,)))
            cells = jnp.where(mine, jnp.broadcast_to(ends[EDGE - 2 : EDGE - 1], (EDGE, lanes)), 0.0)
            cells = jnp.concatenate([cells[:, i * ny : (i + 1) * ny] for i in range(half)], 0)
            cells = by_parts(cells, corner_ref[:ny], corner_ref[ny:])
            turned, ends = [rows], [ends]
            for j in range(windows):
                at = slice(j * ny, (j + 1) * ny)
                side = [
                    jnp.where(
                        left_lane,
                        sides[2 * i * modes : (2 * i + 1) * modes, at],
                        sides[(2 * i + 1) * modes : (2 * i + 2) * modes, at],
                    )
                    for i in range(half)
                ]
                cell = [cells[i * EDGE : (i + 1) * EDGE, at] for i in range(half)]
                power = scale_y if j == 0 else power * scale_y
                turned.append(rows * power + jnp.concatenate(side, 1))
                ends.append(ends[0] * power + jnp.concatenate(cell, 1))
            over = dot(across_ref[...], short_stacked(jnp.concatenate(ends[:windows], 0), 12 * EDGE))
            result = []
            for n in range(windows):
                turned = [a * scale_x + b for a, b in zip(turned[:-1], turned[1:])]
                result.append(turned[0] + over[n * modes : (n + 1) * modes])
            return result

        def carried(change, count):
            left = dot(again_ref[: count * modes], stacked(change))
            left = [left[i * modes : (i + 1) * modes] for i in range(count)]
            if count == 1:
                return [left[0] + unpairs(times_right(pairs(change), sideways_ref[0]))]
            both = jnp.concatenate([pairs(change), pairs(left[0])], 0)
            once = times_right(both, sideways_ref[0])
            twice = times_right(pairs(change), sideways_ref[1])
            rows = half * modes
            return [left[0] + unpairs(once[:rows]), left[1] + unpairs(2.0 * once[rows:] + twice)]

        owns = [own_modes(slot) for slot in slots]
        coeffs = None
        for slot in range(root, -1, -1):
            gain = slots[slot][low - 1 : low]
            own = owns[slot]
            new, changes, later = [], [], []
            for w in range(windows):
                target = drive_ref[w]
                if slot < root:
                    inner = unpairs(times_right(pairs(coeffs[w]), col_ref[slot]))
                    target = jnp.where(nest <= slot, target, dot(row_ref[slot], stacked(inner)))
                before = own[w]
                for v in range(w):
                    before = before + later[v][w - v - 1]
                change = gain * (target - before)
                if w < windows - 1:
                    later.append(carried(change, windows - 1 - w))
                changes.append(change)
                new.append(before + change)
            coeffs = new
        for level in range(levels):
            modes_ref[0, level] = coeffs[-1][:, level * modes : (level + 1) * modes]
        spread = sum(dot(spread_x_ref[w], stacked(changes[w])) for w in range(windows))
        field = 0.0
        for j in range(windows):
            table = spread_y_ref[j]
            part = by_parts(pairs(spread[j * nx : (j + 1) * nx]), table[: 2 * modes], table[2 * modes :])
            field = field + part
        for level in range(levels):
            at_row, at = level // 2 * nx, level % 2 * ny
            state_ref[0, level] = stepped_ref[level] + field[at_row : at_row + nx, at : at + ny]

    return call(
        kernel,
        (shape_of(1, levels, nx, ny), shape_of(1, levels, modes, modes)),
        stepped, drive, row_maps, col_maps, spread_x, spread_y, inward, corner, across, scale_x, scale_y,
        again, sideways, *gathered,
        final=True,
    )


def swap(value, axis, partner):
    size = math.prod(lax.axis_size(name) for name in (axis if isinstance(axis, tuple) else (axis,)))
    return lax.ppermute(value, axis, [(i, partner(i)) for i in range(size) if 0 <= partner(i) < size])


def body(initial_state, drive_modes, relax_rates, nest_offsets):
    plan = Plan(initial_state, drive_modes)
    share, along = project(plan, initial_state, relax_rates)
    if plan.py == 2 and plan.px == 4:
        share, drive_modes, nest_offsets = lax.optimization_barrier((share, drive_modes, nest_offsets))
        from_y = swap(share, "py", lambda i: i ^ 1)
        from_x = swap(along, "px", lambda i: i ^ 1)
        from_both = swap(share, ("py", "px"), lambda i: i ^ (plan.px + 1))
        prepared = prepare(plan, drive_modes, nest_offsets)
        from_both, prepared = lax.optimization_barrier((from_both, prepared))
        total, halo = join_first(plan, share, from_y, from_x, from_both, initial_state)
        columns = from_y
        across = swap(total, "px", lambda i: i ^ 3)
        last = join_last(plan, total, across)
    else:
        from_right = jnp.arange(plan.rows)[:, None] < plan.sums + plan.windows
        right = swap(share, "py", lambda i: i - 1)
        left = swap(share, "py", lambda i: i + 1)
        columns = jnp.where(from_right, right, left)
        top, bottom = both_facing(plan, initial_state, columns)
        above = swap(bottom, "px", lambda i: i + 1)
        below = swap(top, "px", lambda i: i - 1)
        even = lax.axis_index("px") % 2 == 0
        halo, across = jnp.where(even, below, above), jnp.where(even, above, below)
        last = lax.psum(share[: plan.sums], ("py", "px"))
        prepared = prepare(plan, drive_modes, nest_offsets)
    crossed = plan.nest == 4
    if crossed:
        core = swap(last, "nest", lambda i: i ^ 1)
        chip = swap(last, "nest", lambda i: i ^ 2)
        gathered = [last, chip, core, swap(chip, "nest", lambda i: i ^ 1)]
    else:
        gathered = [last] + [swap(last, "nest", lambda i, s=s: i + s) for s in range(1, plan.nest)]
    stepped = step_patch(plan, initial_state, columns, halo, across)
    return nudge(plan, stepped, gathered, crossed, prepared)


def solution(mesh):
    return jax.shard_map(
        body,
        mesh=mesh,
        in_specs=(P("nest", None, "px", "py"), P(), P("nest", None), P()),
        out_specs=(P("nest", None, "px", "py"), P("nest", None, None, None)),
        check_vma=False,
    )
```

```python
import functools
import math

import jax
import jax.numpy as jnp
import numpy as np
from jax import lax
from jax.experimental import pallas as pl
from jax.experimental.pallas import tpu as pltpu
from jax.sharding import PartitionSpec as P

RATIO = 3
RATE = 0.2
EDGE = 8
INTERPRET = False


def multinomial(n, i, j):
    return math.factorial(n) // (math.factorial(i) * math.factorial(j) * math.factorial(n - i - j))


@functools.lru_cache(maxsize=None)
def tables(cells, modes, order):
    cell = np.arange(cells)
    mode = np.arange(modes)
    weight = np.sqrt(np.where(mode == 0, 1.0, 2.0) / cells)
    product = mode[None] * (2 * cell[:, None] + 1)
    coarse = np.pi * (product % (4 * cells)) / (2 * cells)
    fine = np.pi * (product % (4 * RATIO * cells)) / (2 * RATIO * cells)
    base = weight * np.cos(coarse)
    second = RATE * (np.eye(cells, k=1) + np.eye(cells, k=-1) - 2 * np.eye(cells))
    powers = [base]
    for _ in range(order):
        powers.append(second @ powers[-1])
    factor = RATE * (2 * np.cos(np.pi * mode / cells) - 2)
    places = list(range(order)) + list(range(cells - order, cells))
    edges = np.zeros((cells, EDGE))
    edges[places, range(2 * order)] = 1
    spill = [(powers[i] - base * factor**i).T @ edges for i in range(order + 1)]
    return {
        "base": base,
        "edges": edges,
        "powers": powers,
        "factor": factor,
        "spill": spill,
        "within": [base.T @ power for power in powers],
        "cos_map": base.T @ (weight * np.cos(fine)),
        "sin_map": base.T @ (weight * np.sin(fine)),
    }


def kron(count, block):
    return np.kron(np.eye(count), block)


def f32(value):
    return jnp.asarray(np.asarray(value, np.float32))


def bf16(value):
    return np.asarray(value, jnp.bfloat16)


def parts_of(value):
    high = bf16(value)
    return high, bf16(value - high.astype(np.float64))


def left_table(value):
    high, low = parts_of(value)
    return jnp.asarray(np.concatenate([high, low, high], -1))


def right_table(value):
    high, low = parts_of(value)
    upper = np.concatenate([high, low], -1)
    lower = np.concatenate([high, np.zeros_like(low)], -1)
    return jnp.asarray(np.concatenate([upper, lower], -2))


def halves(value):
    high = value.astype(jnp.bfloat16)
    return high, (value - high.astype(jnp.float32)).astype(jnp.bfloat16)


def dot(a, b, dims=((1,), (0,))):
    return lax.dot_general(a, b, (dims, ((), ())), preferred_element_type=jnp.float32)


def stacked(value):
    high, low = halves(value)
    return jnp.concatenate([high, high, low], 0)


def short_stacked(value, rows):
    high = value.astype(jnp.bfloat16).astype(jnp.float32)
    blank = jnp.zeros((rows - 3 * value.shape[0], value.shape[1]), jnp.float32)
    return jnp.concatenate([high, high, value - high, blank], 0).astype(jnp.bfloat16)


def times_right(value, table):
    out = dot(jnp.concatenate(halves(value), 1), table)
    width = out.shape[1] // 2
    return out[:, :width] + out[:, width:]


def by_parts(value, table, rest):
    high, low = halves(value)
    out = dot(jnp.concatenate([high, low], 0), table)
    return out[: value.shape[0]] + out[value.shape[0] :] + dot(high, rest)


def in_vmem(value):
    return value if INTERPRET else pltpu.with_memory_space_constraint(value, pltpu.VMEM)


def call(kernel, shapes, *args, first=False, final=False):
    scalars = [a.ndim == 2 and a.size <= 16 for a in args]
    specs = [pl.BlockSpec(memory_space=pltpu.SMEM if s else pltpu.VMEM) for s in scalars]
    if not final and not INTERPRET:
        shapes = jax.tree.map(lambda s: pltpu.VMEM(s.shape, s.dtype), shapes)
    return pl.pallas_call(
        kernel,
        in_specs=specs,
        out_specs=jax.tree.map(lambda _: pl.BlockSpec(memory_space=pltpu.VMEM), shapes),
        out_shape=shapes,
        interpret=INTERPRET,
    )(*[a if s or first else in_vmem(a) for a, s in zip(args, scalars)])


def shape_of(*dims, kind=jnp.float32):
    return jax.ShapeDtypeStruct(dims, kind)


class Plan:
    def __init__(self, initial_state, drive_modes):
        _, self.levels, self.nx, self.ny = initial_state.shape
        self.windows, _, self.modes, _ = drive_modes.shape
        self.px = lax.axis_size("px")
        self.py = lax.axis_size("py")
        self.nest = lax.axis_size("nest")
        self.lanes = self.levels * self.modes
        self.half = self.levels // 2
        self.low = self.modes + EDGE
        self.sums = self.low + EDGE
        self.rows = self.sums + EDGE
        self.x = tables(self.nx * self.px, self.modes, self.windows)
        self.y = tables(self.ny * self.py, self.modes, self.windows)
        assert self.levels % 4 == 0 and self.modes * 2 == self.ny and self.nx == self.modes
        assert self.windows == 3 and self.half == 2 and EDGE * EDGE == self.modes

    def pairs(self, value):
        width = 2 * self.modes
        return jnp.concatenate([value[:, i * width : (i + 1) * width] for i in range(self.half)], 0)

    def unpairs(self, value):
        rows = value.shape[0] // self.half
        return jnp.concatenate([value[i * rows : (i + 1) * rows] for i in range(self.half)], 1)


def project(plan, state, rates):
    low, half, lanes, levels = plan.low, plan.half, plan.lanes, plan.levels
    modes, nx, ny, windows = plan.modes, plan.nx, plan.ny, plan.windows
    bases = np.concatenate([plan.x["base"], plan.x["edges"], np.zeros((nx * plan.px, EDGE))], 1)
    left = left_table(bases.T.reshape(low + EDGE, plan.px, nx).transpose(1, 0, 2))
    base_y = plan.y["base"].reshape(plan.py, ny, modes)
    edge_y = plan.y["edges"].reshape(plan.py, ny, EDGE)
    right, corner, edge = [], [], []
    for at in range(plan.py):
        high, small = parts_of(kron(2, base_y[at]))
        right.append(np.concatenate([high, small], 1))
        corner.append(bf16(kron(2, np.repeat(edge_y[at], EDGE, 1))))
        edge.append(bf16(np.pad(np.tile(edge_y[at].T, (1, 2)), ((0, EDGE), (0, 0)))))
    pick = np.zeros((2 * EDGE, 2 * ny))
    for i in range(windows):
        pick[i, [i, ny + i]] = 1
        pick[windows + i, [ny - windows + i, 2 * ny - windows + i]] = 1

    def kernel(state_ref, left_ref, right_ref, corner_ref, edge_ref, pick_ref, rates_ref, out_ref, along_ref):
        px, py = lax.axis_index("px"), lax.axis_index("py")
        field = jnp.concatenate([state_ref[0, level] for level in range(levels)], 1)
        rows = dot(left_ref[px], stacked(field))
        width = 2 * ny
        both = jnp.concatenate([rows[:low, i * width : (i + 1) * width] for i in range(half)], 0)
        high, small = halves(both)
        table = right_ref[py]
        found = dot(high, table)
        found = found[:, :ny] + found[:, ny:] + dot(small, table[:, :ny])
        out_ref[:modes] = jnp.concatenate([found[i * low : i * low + modes] for i in range(half)], 1)
        ends = jnp.concatenate([found[i * low + modes : (i + 1) * low] for i in range(half)], 1)
        cells = jnp.concatenate([rows[modes:low, i * width : (i + 1) * width] for i in range(half)], 0)
        cells = dot(jnp.concatenate(halves(cells), 0), corner_ref[py])
        cells = cells[: half * EDGE] + cells[half * EDGE :]
        cells = jnp.concatenate([cells[i * EDGE : (i + 1) * EDGE] for i in range(half)], 1)
        row = lax.broadcasted_iota(jnp.int32, (EDGE, lanes), 0)
        lane = lax.broadcasted_iota(jnp.int32, (EDGE, lanes), 1)
        cells = jnp.sum(jnp.where(lane % EDGE == row, cells, 0.0), 0, keepdims=True)
        gain = jnp.zeros((EDGE, lanes), jnp.float32)
        for i in range(levels):
            gain = jnp.where(lane // modes == i, rates_ref[0, i], gain)
        gain = jnp.where((px == 0) & (py == 0), gain, 0.0)
        ends = jnp.where(row == EDGE - 1, gain, jnp.where(row == EDGE - 2, cells, ends))
        out_ref[modes:low] = ends
        upright = jnp.concatenate([rows[:modes, i * ny : (i + 1) * ny] for i in range(levels)], 0)
        upright = jnp.concatenate(halves(upright), 1)
        out_ref[low : plan.sums] = dot(edge_ref[py], upright, ((1,), (1,)))[:EDGE]
        patch = jnp.concatenate([state_ref[0, level] for level in range(levels)], 0)
        patch = jnp.concatenate(halves(patch), 1)
        out_ref[plan.sums :] = dot(pick_ref[...], patch, ((1,), (1,)))[:EDGE]
        along_ref[: plan.sums] = out_ref[: plan.sums]
        lines = facing_rows(plan, state_ref, px % 2 == 0)
        along_ref[plan.sums :] = jnp.concatenate([lines, jnp.zeros((2, lanes), jnp.float32)], 0)

    return call(
        kernel,
        (shape_of(plan.rows, lanes), shape_of(plan.rows, lanes)),
        state, left, jnp.asarray(np.stack(right)), jnp.asarray(np.stack(corner)), jnp.asarray(np.stack(edge)),
        jnp.asarray(bf16(pick)), rates,
        first=True,
    )


def facing_rows(plan, state_ref, bottom):
    rows = []
    for group in range(plan.half):
        pair = [state_ref[0, 2 * group + i] for i in range(2)]
        top = jnp.concatenate([p[: plan.windows] for p in pair], 1)
        end = jnp.concatenate([p[plan.nx - plan.windows :] for p in pair], 1)
        rows.append(jnp.where(bottom, end, top))
    return jnp.concatenate(rows, 0)


def facing_corners(plan, columns, bottom):
    lane = lax.broadcasted_iota(jnp.int32, (EDGE, plan.lanes), 1)
    moved = pltpu.roll(columns, plan.lanes - (plan.nx - plan.windows), 1)
    near = jnp.where(lane % plan.nx < plan.windows, jnp.where(bottom, moved, columns), 0.0)
    packed = near[:1]
    for i in range(1, 2 * plan.windows):
        packed = packed + pltpu.roll(near, EDGE * i, 1)[i : i + 1]
    return jnp.concatenate([packed, jnp.zeros((1, plan.lanes), jnp.float32)], 0)


def join_first(plan, own, from_y, from_x, from_both, state):
    sums, windows = plan.sums, plan.windows

    def kernel(own_ref, y_ref, x_ref, both_ref, state_ref, out_ref, halo_ref):
        odd = lax.axis_index("px") % 2 == 1
        out_ref[:sums] = (own_ref[:sums] + y_ref[:sums]) + (x_ref[:sums] + both_ref[:sums])
        corners = facing_corners(plan, y_ref[sums:], odd)
        out_ref[sums:] = jnp.concatenate([facing_rows(plan, state_ref, odd), corners], 0)
        corners = facing_corners(plan, both_ref[sums:], odd)
        halo_ref[...] = jnp.concatenate([x_ref[sums : sums + 2 * windows], corners], 0)

    shapes = shape_of(plan.rows, plan.lanes), shape_of(EDGE, plan.lanes)
    return call(kernel, shapes, own, from_y, from_x, from_both, state)


def both_facing(plan, state, columns):
    def kernel(state_ref, columns_ref, top_ref, bottom_ref):
        columns = columns_ref[plan.sums :]
        for ref, bottom in ((top_ref, False), (bottom_ref, True)):
            rows = [facing_rows(plan, state_ref, bottom), facing_corners(plan, columns, bottom)]
            ref[...] = jnp.concatenate(rows, 0)

    return call(kernel, (shape_of(EDGE, plan.lanes),) * 2, state, columns)


def join_last(plan, own, other):
    sums = plan.sums

    def kernel(own_ref, other_ref, out_ref):
        out_ref[...] = own_ref[:sums] + other_ref[:sums]

    return call(kernel, shape_of(sums, plan.lanes), own, other)


def step_patch(plan, state, columns, first, second):
    nx, ny, windows, sums, levels = plan.nx, plan.ny, plan.windows, plan.sums, plan.levels
    place = np.zeros((4 * EDGE, ny))
    for i in range(windows):
        for part in range(3):
            place[part * EDGE + i, i] = 1
            place[part * EDGE + windows + i, ny - windows + i] = 1
    rows, lanes = nx + 2 * EDGE, 2 * ny

    def kernel(state_ref, columns_ref, first_ref, second_ref, place_ref, out_ref):
        px, py = lax.axis_index("px"), lax.axis_index("py")
        row = lax.broadcasted_iota(jnp.int32, (rows, lanes), 0) - EDGE + px * nx
        lane = lax.broadcasted_iota(jnp.int32, (rows, lanes), 1)
        lane = jnp.where(lane >= ny + ny // 2, lane - lanes, lane) + py * ny
        inside = (row >= 0) & (row < nx * plan.px) & (lane >= 0) & (lane < ny * plan.py)
        where = place_ref[...]

        def spread(block):
            high = block.astype(jnp.bfloat16).astype(jnp.float32)
            rest = block - high
            middle = rest.astype(jnp.bfloat16).astype(jnp.float32)
            parts = [high, middle, rest - middle, jnp.zeros_like(high)]
            return dot(jnp.concatenate(parts, 0).astype(jnp.bfloat16), where, ((0,), (0,)))

        small_row = lax.broadcasted_iota(jnp.int32, (EDGE, plan.lanes), 0)
        small_lane = lax.broadcasted_iota(jnp.int32, (EDGE, plan.lanes), 1)
        mine = small_lane % nx // EDGE == small_row

        def corners(block):
            line = jnp.broadcast_to(block[2 * windows : 2 * windows + 1], (EDGE, plan.lanes))
            cells = spread(jnp.where(mine, line, 0.0))
            return [
                sum(cells[level * nx + EDGE * i : level * nx + EDGE * (i + 1)] for i in range(2 * windows))
                for level in range(levels)
            ]

        even = px % 2 == 0
        one, two = first_ref[...], second_ref[second_ref.shape[0] - EDGE :]
        above, below = jnp.where(even, two, one), jnp.where(even, one, two)
        beside = spread(columns_ref[sums:])
        beside_above, beside_below = corners(above), corners(below)
        blank = jnp.zeros((EDGE - windows, lanes), jnp.float32)
        for level in range(levels):
            pair, part = level // 2, level % 2

            def line(block):
                return block[pair * windows : (pair + 1) * windows, part * ny : (part + 1) * ny]

            up = jnp.concatenate([line(above), beside_above[level][:windows]], 1)
            down = jnp.concatenate([line(below), beside_below[level][:windows]], 1)
            middle = jnp.concatenate([state_ref[0, level], beside[level * nx : (level + 1) * nx]], 1)
            field = jnp.concatenate([blank, up, middle, down, blank], 0)
            field = jnp.where(inside, field, 0.0)
            for _ in range(windows):
                around = (
                    pltpu.roll(field, 1, 0)
                    + pltpu.roll(field, rows - 1, 0)
                    + pltpu.roll(field, 1, 1)
                    + pltpu.roll(field, lanes - 1, 1)
                )
                field = jnp.where(inside, field + RATE * (around - 4.0 * field), 0.0)
            out_ref[level] = field[EDGE : EDGE + nx, :ny]

    return call(
        kernel, shape_of(levels, nx, ny), state, columns, first, second, jnp.asarray(bf16(place))
    )


def prepare(plan, drive, nest_offsets):
    modes, lanes, levels, windows = plan.modes, plan.lanes, plan.levels, plan.windows
    nx, ny, x, y = plan.nx, plan.ny, plan.x, plan.y
    steps = plan.nest - 1
    maps_x = f32(np.stack([np.tile(x[name], (1, 2)) for name in ("cos_map", "sin_map")]))
    maps_y = f32(np.stack([kron(2, y[name].T) for name in ("cos_map", "sin_map")]))
    rows_x = np.stack([np.tile(p, (1, 2)).reshape(plan.px, nx, 2 * modes) for p in x["powers"][:windows]], 1)
    rows_y = np.stack(
        [p.reshape(plan.py, ny, modes).transpose(0, 2, 1) for p in y["powers"][:windows]], 1
    )

    def kernel(
        drive_ref, maps_x_ref, maps_y_ref, rows_x_ref, rows_y_ref, offsets_ref,
        drive_out, row_out, col_out, spread_x_out, spread_y_out,
    ):
        nest, px, py = lax.axis_index("nest"), lax.axis_index("px"), lax.axis_index("py")
        for w in range(windows):
            drive_out[w] = jnp.concatenate([drive_ref[w, level] for level in range(levels)], 1)
        lane = lax.broadcasted_iota(jnp.int32, (modes, 2 * modes), 1)

        def as_left(twice):
            rounded = twice.astype(jnp.bfloat16).astype(jnp.float32)
            pair = jnp.where(lane >= modes, twice - rounded, rounded)
            return jnp.concatenate([pair, rounded], 1)[:, : 3 * modes].astype(jnp.bfloat16)

        def angle(mode, offset, cells):
            turn = (mode * offset).astype(jnp.float32)
            turn = turn - jnp.floor(turn / (2.0 * cells)) * (2.0 * cells)
            return turn * (math.pi / cells)

        mode = lax.broadcasted_iota(jnp.int32, (EDGE, 2 * modes), 1) % modes
        row = lax.broadcasted_iota(jnp.int32, (EDGE, 2 * modes), 0)
        upright = lax.broadcasted_iota(jnp.int32, (2 * modes, 2 * modes), 0) % modes
        place = lax.broadcasted_iota(jnp.int32, (2 * modes, 2 * modes), 1)
        along, down = jnp.zeros_like(mode), jnp.zeros_like(upright)
        for slot in range(steps):
            domain = jnp.maximum(nest - slot, 0)
            along = jnp.where(row == slot, offsets_ref[0, domain], along)
            down = jnp.where(place == slot, offsets_ref[1, domain], down)
        along = angle(mode, along, nx * plan.px)
        down = angle(upright, down, ny * plan.py)
        cos_x, sin_x = jnp.cos(along), jnp.sin(along)
        cos_y, sin_y = jnp.cos(down), jnp.sin(down)
        for slot in range(steps):
            at = slice(slot, slot + 1)
            row_out[slot] = as_left(maps_x_ref[0] * cos_x[at] - maps_x_ref[1] * sin_x[at])
            col_map = maps_y_ref[0] * cos_y[:, at] - maps_y_ref[1] * sin_y[:, at]
            high, small = halves(col_map)
            upper = jnp.concatenate([high, small], 1)
            lower = jnp.concatenate([high, jnp.zeros_like(high)], 1)
            col_out[slot] = jnp.concatenate([upper, lower], 0)
        for w in range(windows):
            p = windows - 1 - w
            for j in range(windows):
                if j <= p:
                    combined = sum(multinomial(p, i, j) * rows_x_ref[px, i] for i in range(p - j + 1))
                    spread_x_out[w, j * nx : (j + 1) * nx] = as_left(combined)
                else:
                    spread_x_out[w, j * nx : (j + 1) * nx] = jnp.zeros((nx, 3 * modes), jnp.bfloat16)
        for j in range(windows):
            table = rows_y_ref[py, j]
            blank = jnp.zeros_like(table)
            table = jnp.concatenate(
                [jnp.concatenate([table, blank], 1), jnp.concatenate([blank, table], 1)], 0
            )
            high, small = halves(table)
            spread_y_out[j] = jnp.concatenate([high, small], 0)

    shapes = (
        shape_of(windows, modes, lanes),
        shape_of(steps, modes, 3 * modes, kind=jnp.bfloat16),
        shape_of(steps, 4 * modes, 4 * modes, kind=jnp.bfloat16),
        shape_of(windows, windows * nx, 3 * modes, kind=jnp.bfloat16),
        shape_of(windows, 4 * modes, 2 * ny, kind=jnp.bfloat16),
    )
    return call(kernel, shapes, drive, maps_x, maps_y, f32(rows_x), f32(rows_y), nest_offsets.T, first=True)


def nudge(plan, stepped, gathered, crossed, prepared):
    modes, low, lanes, levels = plan.modes, plan.low, plan.lanes, plan.levels
    windows, half, nx, ny = plan.windows, plan.half, plan.nx, plan.ny
    x, y, sums = plan.x, plan.y, plan.sums
    pairs, unpairs = plan.pairs, plan.unpairs

    inward = np.concatenate([np.tile(y["spill"][j].T, (1, 2)) for j in range(1, windows + 1)], 1)
    high, small = parts_of(inward)
    inward = jnp.asarray(np.concatenate([high, small, high, np.zeros_like(high)], 0))
    corner = np.concatenate(
        [kron(2, np.repeat(y["spill"][j].T, EDGE, 0)) for j in range(1, windows + 1)], 1
    )
    high, small = parts_of(corner)
    corner = jnp.asarray(np.concatenate([high, small], 0))
    across = np.zeros((windows * modes, windows * EDGE))
    for n in range(1, windows + 1):
        for j in range(n):
            across[(n - 1) * modes : n * modes, j * EDGE : (j + 1) * EDGE] = sum(
                multinomial(n, i, j) * x["spill"][i] for i in range(1, n - j + 1)
            )
    high, small = parts_of(across)
    across = jnp.asarray(np.pad(np.concatenate([high, small, high], 1), ((0, 0), (0, 3 * EDGE))))
    scale_x = f32(np.broadcast_to(1.0 + x["factor"][:, None], (modes, lanes)))
    scale_y = f32(np.broadcast_to(np.tile(y["factor"], levels), (EDGE, lanes)))
    again = []
    for p in range(1, windows):
        again.append(sum(multinomial(p, i, 0) * x["within"][i] for i in range(p + 1)))
    again = left_table(np.concatenate(again, 0))
    sideways = jnp.stack([right_table(kron(2, y["within"][j])) for j in range(1, windows)])
    drive, row_maps, col_maps, spread_x, spread_y = prepared

    def kernel(
        stepped_ref, drive_ref, row_ref, col_ref, spread_x_ref, spread_y_ref, inward_ref, corner_ref,
        across_ref, scale_x_ref, scale_y_ref, again_ref, sideways_ref, *refs,
    ):
        refs, (state_ref, modes_ref) = refs[:-2], refs[-2:]
        root = plan.nest - 1
        nest = lax.axis_index("nest")
        slots = [ref[...] for ref in refs]
        if crossed:
            slots = [slots[0], jnp.where(nest % 2 == 1, slots[2], slots[3]), slots[1], slots[3]]
        scale_x, scale_y = scale_x_ref[...], scale_y_ref[:1]
        row = lax.broadcasted_iota(jnp.int32, (EDGE, lanes), 0)
        lane = lax.broadcasted_iota(jnp.int32, (EDGE, lanes), 1)
        mine = lane % EDGE == row
        left_lane = lax.broadcasted_iota(jnp.int32, (modes, ny), 1) < modes

        def own_modes(message):
            rows, ends = message[:modes], message[modes:low]
            sides = dot(short_stacked(message[low:sums], 4 * EDGE), inward_ref[...], ((0,), (0,)))
            cells = jnp.where(mine, jnp.broadcast_to(ends[EDGE - 2 : EDGE - 1], (EDGE, lanes)), 0.0)
            cells = jnp.concatenate([cells[:, i * ny : (i + 1) * ny] for i in range(half)], 0)
            cells = by_parts(cells, corner_ref[:ny], corner_ref[ny:])
            turned, ends = [rows], [ends]
            for j in range(windows):
                at = slice(j * ny, (j + 1) * ny)
                side = [
                    jnp.where(
                        left_lane,
                        sides[2 * i * modes : (2 * i + 1) * modes, at],
                        sides[(2 * i + 1) * modes : (2 * i + 2) * modes, at],
                    )
                    for i in range(half)
                ]
                cell = [cells[i * EDGE : (i + 1) * EDGE, at] for i in range(half)]
                power = scale_y if j == 0 else power * scale_y
                turned.append(rows * power + jnp.concatenate(side, 1))
                ends.append(ends[0] * power + jnp.concatenate(cell, 1))
            over = dot(across_ref[...], short_stacked(jnp.concatenate(ends[:windows], 0), 12 * EDGE))
            result = []
            for n in range(windows):
                turned = [a * scale_x + b for a, b in zip(turned[:-1], turned[1:])]
                result.append(turned[0] + over[n * modes : (n + 1) * modes])
            return result

        owns = [own_modes(slot) for slot in slots]
        gains = [slot[low - 1 : low] for slot in slots]
        coeffs, changes, later = {}, {}, {}
        for front in range(root + windows):
            cells = [(root - front + w, w) for w in range(windows) if 0 <= root - front + w <= root]
            inner, lefts, rights = {}, {}, {}
            for slot, w in cells:
                if slot < root:
                    inner[slot, w] = times_right(pairs(coeffs[slot + 1, w]), col_ref[slot])
                if w > 0:
                    change = changes[slot, w - 1]
                    count = windows - w
                    left = dot(again_ref[: count * modes], stacked(change))
                    lefts[slot] = left = [left[i * modes : (i + 1) * modes] for i in range(count)]
                    rights[slot] = [unpairs(times_right(pairs(change), sideways_ref[i])) for i in range(count)]
                    later[slot, w - 1, 1] = left[0] + rights[slot][0]
            for slot, w in cells:
                target = drive_ref[w]
                if slot < root:
                    found = dot(row_ref[slot], stacked(unpairs(inner[slot, w])))
                    target = jnp.where(nest <= slot, target, found)
                before = owns[slot][w]
                for v in range(w):
                    before = before + later[slot, v, w - v]
                changes[slot, w] = gains[slot] * (target - before)
                coeffs[slot, w] = before + changes[slot, w]
            for slot, w in cells:
                if w > 0 and windows - w > 1:
                    left, right = lefts[slot], rights[slot]
                    mixed = unpairs(times_right(pairs(left[0]), sideways_ref[0]))
                    later[slot, w - 1, 2] = left[1] + (2.0 * mixed + right[1])
        changes = [changes[0, w] for w in range(windows)]
        coeffs = [coeffs[0, w] for w in range(windows)]
        for level in range(levels):
            modes_ref[0, level] = coeffs[-1][:, level * modes : (level + 1) * modes]
        spread = sum(dot(spread_x_ref[w], stacked(changes[w])) for w in range(windows))
        field = 0.0
        for j in range(windows):
            table = spread_y_ref[j]
            part = by_parts(pairs(spread[j * nx : (j + 1) * nx]), table[: 2 * modes], table[2 * modes :])
            field = field + part
        for level in range(levels):
            at_row, at = level // 2 * nx, level % 2 * ny
            state_ref[0, level] = stepped_ref[level] + field[at_row : at_row + nx, at : at + ny]

    return call(
        kernel,
        (shape_of(1, levels, nx, ny), shape_of(1, levels, modes, modes)),
        stepped, drive, row_maps, col_maps, spread_x, spread_y, inward, corner, across, scale_x, scale_y,
        again, sideways, *gathered,
        final=True,
    )


def swap(value, axis, partner):
    size = math.prod(lax.axis_size(name) for name in (axis if isinstance(axis, tuple) else (axis,)))
    return lax.ppermute(value, axis, [(i, partner(i)) for i in range(size) if 0 <= partner(i) < size])


def body(initial_state, drive_modes, relax_rates, nest_offsets):
    plan = Plan(initial_state, drive_modes)
    share, along = project(plan, initial_state, relax_rates)
    if plan.py == 2 and plan.px == 4:
        share, drive_modes, nest_offsets = lax.optimization_barrier((share, drive_modes, nest_offsets))
        from_y = swap(share, "py", lambda i: i ^ 1)
        from_x = swap(along, "px", lambda i: i ^ 1)
        from_both = swap(share, ("py", "px"), lambda i: i ^ (plan.px + 1))
        prepared = prepare(plan, drive_modes, nest_offsets)
        from_both, prepared = lax.optimization_barrier((from_both, prepared))
        total, halo = join_first(plan, share, from_y, from_x, from_both, initial_state)
        columns = from_y
        across = swap(total, "px", lambda i: i ^ 3)
        last = join_last(plan, total, across)
    else:
        from_right = jnp.arange(plan.rows)[:, None] < plan.sums + plan.windows
        right = swap(share, "py", lambda i: i - 1)
        left = swap(share, "py", lambda i: i + 1)
        columns = jnp.where(from_right, right, left)
        top, bottom = both_facing(plan, initial_state, columns)
        above = swap(bottom, "px", lambda i: i + 1)
        below = swap(top, "px", lambda i: i - 1)
        even = lax.axis_index("px") % 2 == 0
        halo, across = jnp.where(even, below, above), jnp.where(even, above, below)
        last = lax.psum(share[: plan.sums], ("py", "px"))
        prepared = prepare(plan, drive_modes, nest_offsets)
    crossed = plan.nest == 4
    if crossed:
        core = swap(last, "nest", lambda i: i ^ 1)
        chip = swap(last, "nest", lambda i: i ^ 2)
        stepped = step_patch(plan, initial_state, columns, halo, across)
        chip, stepped = lax.optimization_barrier((chip, stepped))
        gathered = [last, chip, core, swap(chip, "nest", lambda i: i ^ 1)]
    else:
        gathered = [last] + [swap(last, "nest", lambda i, s=s: i + s) for s in range(1, plan.nest)]
        stepped = step_patch(plan, initial_state, columns, halo, across)
    return nudge(plan, stepped, gathered, crossed, prepared)


def solution(mesh):
    return jax.shard_map(
        body,
        mesh=mesh,
        in_specs=(P("nest", None, "px", "py"), P(), P("nest", None), P()),
        out_specs=(P("nest", None, "px", "py"), P("nest", None, None, None)),
        check_vma=False,
    )
```

```python
import functools
import math

import jax
import jax.numpy as jnp
import numpy as np
from jax import lax
from jax.experimental import pallas as pl
from jax.experimental.pallas import tpu as pltpu
from jax.sharding import PartitionSpec as P

RATIO = 3
RATE = 0.2
EDGE = 8
INTERPRET = False


def multinomial(n, i, j):
    return math.factorial(n) // (math.factorial(i) * math.factorial(j) * math.factorial(n - i - j))


@functools.lru_cache(maxsize=None)
def tables(cells, modes, order):
    cell = np.arange(cells)
    mode = np.arange(modes)
    weight = np.sqrt(np.where(mode == 0, 1.0, 2.0) / cells)
    product = mode[None] * (2 * cell[:, None] + 1)
    coarse = np.pi * (product % (4 * cells)) / (2 * cells)
    fine = np.pi * (product % (4 * RATIO * cells)) / (2 * RATIO * cells)
    base = weight * np.cos(coarse)
    second = RATE * (np.eye(cells, k=1) + np.eye(cells, k=-1) - 2 * np.eye(cells))
    powers = [base]
    for _ in range(order):
        powers.append(second @ powers[-1])
    factor = RATE * (2 * np.cos(np.pi * mode / cells) - 2)
    places = list(range(order)) + list(range(cells - order, cells))
    edges = np.zeros((cells, EDGE))
    edges[places, range(2 * order)] = 1
    spill = [(powers[i] - base * factor**i).T @ edges for i in range(order + 1)]
    return {
        "base": base,
        "edges": edges,
        "powers": powers,
        "factor": factor,
        "spill": spill,
        "within": [base.T @ power for power in powers],
        "cos_map": base.T @ (weight * np.cos(fine)),
        "sin_map": base.T @ (weight * np.sin(fine)),
    }


def kron(count, block):
    return np.kron(np.eye(count), block)


def f32(value):
    return jnp.asarray(np.asarray(value, np.float32))


def bf16(value):
    return np.asarray(value, jnp.bfloat16)


def parts_of(value):
    high = bf16(value)
    return high, bf16(value - high.astype(np.float64))


def left_table(value):
    high, low = parts_of(value)
    return jnp.asarray(np.concatenate([high, low, high], -1))


def right_table(value):
    return jnp.asarray(np.concatenate(parts_of(value), -1))


def halves(value):
    high = value.astype(jnp.bfloat16)
    return high, (value - high.astype(jnp.float32)).astype(jnp.bfloat16)


def dot(a, b, dims=((1,), (0,))):
    return lax.dot_general(a, b, (dims, ((), ())), preferred_element_type=jnp.float32)


def stacked(value):
    high, low = halves(value)
    return jnp.concatenate([high, high, low], 0)


def short_stacked(value, rows):
    high = value.astype(jnp.bfloat16).astype(jnp.float32)
    blank = jnp.zeros((rows - 3 * value.shape[0], value.shape[1]), jnp.float32)
    return jnp.concatenate([high, high, value - high, blank], 0).astype(jnp.bfloat16)


def times_right(value, table):
    width = table.shape[1] // 2
    lower = jnp.concatenate([table[:, :width], jnp.zeros_like(table[:, width:])], 1)
    out = dot(jnp.concatenate(halves(value), 1), jnp.concatenate([table, lower], 0))
    return out[:, :width] + out[:, width:]


def by_parts(value, table, rest):
    high, low = halves(value)
    out = dot(jnp.concatenate([high, low], 0), table)
    return out[: value.shape[0]] + out[value.shape[0] :] + dot(high, rest)


def in_vmem(value):
    return value if INTERPRET else pltpu.with_memory_space_constraint(value, pltpu.VMEM)


def call(kernel, shapes, *args, first=False, final=False):
    scalars = [a.ndim == 2 and a.size <= 16 for a in args]
    specs = [pl.BlockSpec(memory_space=pltpu.SMEM if s else pltpu.VMEM) for s in scalars]
    if not final and not INTERPRET:
        shapes = jax.tree.map(lambda s: pltpu.VMEM(s.shape, s.dtype), shapes)
    return pl.pallas_call(
        kernel,
        in_specs=specs,
        out_specs=jax.tree.map(lambda _: pl.BlockSpec(memory_space=pltpu.VMEM), shapes),
        out_shape=shapes,
        interpret=INTERPRET,
    )(*[a if s or first else in_vmem(a) for a, s in zip(args, scalars)])


def shape_of(*dims, kind=jnp.float32):
    return jax.ShapeDtypeStruct(dims, kind)


class Plan:
    def __init__(self, initial_state, drive_modes):
        _, self.levels, self.nx, self.ny = initial_state.shape
        self.windows, _, self.modes, _ = drive_modes.shape
        self.px = lax.axis_size("px")
        self.py = lax.axis_size("py")
        self.nest = lax.axis_size("nest")
        self.lanes = self.levels * self.modes
        self.half = self.levels // 2
        self.low = self.modes + EDGE
        self.sums = self.low + EDGE
        self.rows = self.sums + EDGE
        self.x = tables(self.nx * self.px, self.modes, self.windows)
        self.y = tables(self.ny * self.py, self.modes, self.windows)
        assert self.levels % 4 == 0 and self.modes * 2 == self.ny and self.nx == self.modes
        assert self.windows == 3 and self.half == 2 and EDGE * EDGE == self.modes

    def pairs(self, value):
        width = 2 * self.modes
        return jnp.concatenate([value[:, i * width : (i + 1) * width] for i in range(self.half)], 0)

    def unpairs(self, value):
        rows = value.shape[0] // self.half
        return jnp.concatenate([value[i * rows : (i + 1) * rows] for i in range(self.half)], 1)


def project(plan, state, rates):
    low, half, lanes, levels = plan.low, plan.half, plan.lanes, plan.levels
    modes, nx, ny, windows = plan.modes, plan.nx, plan.ny, plan.windows
    bases = np.concatenate([plan.x["base"], plan.x["edges"], np.zeros((nx * plan.px, EDGE))], 1)
    left = left_table(bases.T.reshape(low + EDGE, plan.px, nx).transpose(1, 0, 2))
    base_y = plan.y["base"].reshape(plan.py, ny, modes)
    edge_y = plan.y["edges"].reshape(plan.py, ny, EDGE)
    right, corner, edge = [], [], []
    for at in range(plan.py):
        high, small = parts_of(kron(2, base_y[at]))
        right.append(np.concatenate([high, small], 1))
        corner.append(bf16(kron(2, np.repeat(edge_y[at], EDGE, 1))))
        edge.append(bf16(np.pad(np.tile(edge_y[at].T, (1, 2)), ((0, EDGE), (0, 0)))))
    pick = np.zeros((2 * EDGE, 2 * ny))
    for i in range(windows):
        pick[i, [i, ny + i]] = 1
        pick[windows + i, [ny - windows + i, 2 * ny - windows + i]] = 1

    def kernel(state_ref, left_ref, right_ref, corner_ref, edge_ref, pick_ref, rates_ref, out_ref, along_ref):
        px, py = lax.axis_index("px"), lax.axis_index("py")
        field = jnp.concatenate([state_ref[0, level] for level in range(levels)], 1)
        rows = dot(left_ref[px], stacked(field))
        width = 2 * ny
        both = jnp.concatenate([rows[:low, i * width : (i + 1) * width] for i in range(half)], 0)
        high, small = halves(both)
        table = right_ref[py]
        found = dot(high, table)
        found = found[:, :ny] + found[:, ny:] + dot(small, table[:, :ny])
        out_ref[:modes] = jnp.concatenate([found[i * low : i * low + modes] for i in range(half)], 1)
        ends = jnp.concatenate([found[i * low + modes : (i + 1) * low] for i in range(half)], 1)
        cells = jnp.concatenate([rows[modes:low, i * width : (i + 1) * width] for i in range(half)], 0)
        cells = dot(jnp.concatenate(halves(cells), 0), corner_ref[py])
        cells = cells[: half * EDGE] + cells[half * EDGE :]
        cells = jnp.concatenate([cells[i * EDGE : (i + 1) * EDGE] for i in range(half)], 1)
        row = lax.broadcasted_iota(jnp.int32, (EDGE, lanes), 0)
        lane = lax.broadcasted_iota(jnp.int32, (EDGE, lanes), 1)
        cells = jnp.sum(jnp.where(lane % EDGE == row, cells, 0.0), 0, keepdims=True)
        gain = jnp.zeros((EDGE, lanes), jnp.float32)
        for i in range(levels):
            gain = jnp.where(lane // modes == i, rates_ref[0, i], gain)
        gain = jnp.where((px == 0) & (py == 0), gain, 0.0)
        ends = jnp.where(row == EDGE - 1, gain, jnp.where(row == EDGE - 2, cells, ends))
        out_ref[modes:low] = ends
        upright = jnp.concatenate([rows[:modes, i * ny : (i + 1) * ny] for i in range(levels)], 0)
        upright = jnp.concatenate(halves(upright), 1)
        out_ref[low : plan.sums] = dot(edge_ref[py], upright, ((1,), (1,)))[:EDGE]
        patch = jnp.concatenate([state_ref[0, level] for level in range(levels)], 0)
        patch = jnp.concatenate(halves(patch), 1)
        out_ref[plan.sums :] = dot(pick_ref[...], patch, ((1,), (1,)))[:EDGE]
        along_ref[: plan.sums] = out_ref[: plan.sums]
        lines = facing_rows(plan, state_ref, px % 2 == 0)
        along_ref[plan.sums :] = jnp.concatenate([lines, jnp.zeros((2, lanes), jnp.float32)], 0)

    return call(
        kernel,
        (shape_of(plan.rows, lanes), shape_of(plan.rows, lanes)),
        state, left, jnp.asarray(np.stack(right)), jnp.asarray(np.stack(corner)), jnp.asarray(np.stack(edge)),
        jnp.asarray(bf16(pick)), rates,
        first=True,
    )


def facing_rows(plan, state_ref, bottom):
    rows = []
    for group in range(plan.half):
        pair = [state_ref[0, 2 * group + i] for i in range(2)]
        top = jnp.concatenate([p[: plan.windows] for p in pair], 1)
        end = jnp.concatenate([p[plan.nx - plan.windows :] for p in pair], 1)
        rows.append(jnp.where(bottom, end, top))
    return jnp.concatenate(rows, 0)


def facing_corners(plan, columns, bottom):
    lane = lax.broadcasted_iota(jnp.int32, (EDGE, plan.lanes), 1)
    moved = pltpu.roll(columns, plan.lanes - (plan.nx - plan.windows), 1)
    near = jnp.where(lane % plan.nx < plan.windows, jnp.where(bottom, moved, columns), 0.0)
    packed = near[:1]
    for i in range(1, 2 * plan.windows):
        packed = packed + pltpu.roll(near, EDGE * i, 1)[i : i + 1]
    return jnp.concatenate([packed, jnp.zeros((1, plan.lanes), jnp.float32)], 0)


def join_first(plan, own, from_y, from_x, from_both, state):
    sums, windows = plan.sums, plan.windows

    def kernel(own_ref, y_ref, x_ref, both_ref, state_ref, out_ref, halo_ref):
        odd = lax.axis_index("px") % 2 == 1
        out_ref[:sums] = (own_ref[:sums] + y_ref[:sums]) + (x_ref[:sums] + both_ref[:sums])
        corners = facing_corners(plan, y_ref[sums:], odd)
        out_ref[sums:] = jnp.concatenate([facing_rows(plan, state_ref, odd), corners], 0)
        corners = facing_corners(plan, both_ref[sums:], odd)
        halo_ref[...] = jnp.concatenate([x_ref[sums : sums + 2 * windows], corners], 0)

    shapes = shape_of(plan.rows, plan.lanes), shape_of(EDGE, plan.lanes)
    return call(kernel, shapes, own, from_y, from_x, from_both, state)


def both_facing(plan, state, columns):
    def kernel(state_ref, columns_ref, top_ref, bottom_ref):
        columns = columns_ref[plan.sums :]
        for ref, bottom in ((top_ref, False), (bottom_ref, True)):
            rows = [facing_rows(plan, state_ref, bottom), facing_corners(plan, columns, bottom)]
            ref[...] = jnp.concatenate(rows, 0)

    return call(kernel, (shape_of(EDGE, plan.lanes),) * 2, state, columns)


def join_last(plan, own, other):
    sums = plan.sums

    def kernel(own_ref, other_ref, out_ref):
        out_ref[...] = own_ref[:sums] + other_ref[:sums]

    return call(kernel, shape_of(sums, plan.lanes), own, other)


def step_patch(plan, state, columns, first, second):
    nx, ny, windows, sums, levels = plan.nx, plan.ny, plan.windows, plan.sums, plan.levels
    place = np.zeros((4 * EDGE, ny))
    for i in range(windows):
        for part in range(3):
            place[part * EDGE + i, i] = 1
            place[part * EDGE + windows + i, ny - windows + i] = 1
    rows, lanes = nx + 2 * EDGE, 2 * ny

    def kernel(state_ref, columns_ref, first_ref, second_ref, place_ref, out_ref):
        px, py = lax.axis_index("px"), lax.axis_index("py")
        row = lax.broadcasted_iota(jnp.int32, (rows, lanes), 0) - EDGE + px * nx
        lane = lax.broadcasted_iota(jnp.int32, (rows, lanes), 1)
        lane = jnp.where(lane >= ny + ny // 2, lane - lanes, lane) + py * ny
        inside = (row >= 0) & (row < nx * plan.px) & (lane >= 0) & (lane < ny * plan.py)
        where = place_ref[...]

        def spread(block):
            high = block.astype(jnp.bfloat16).astype(jnp.float32)
            rest = block - high
            middle = rest.astype(jnp.bfloat16).astype(jnp.float32)
            parts = [high, middle, rest - middle, jnp.zeros_like(high)]
            return dot(jnp.concatenate(parts, 0).astype(jnp.bfloat16), where, ((0,), (0,)))

        small_row = lax.broadcasted_iota(jnp.int32, (EDGE, plan.lanes), 0)
        small_lane = lax.broadcasted_iota(jnp.int32, (EDGE, plan.lanes), 1)
        mine = small_lane % nx // EDGE == small_row

        def corners(block):
            line = jnp.broadcast_to(block[2 * windows : 2 * windows + 1], (EDGE, plan.lanes))
            cells = spread(jnp.where(mine, line, 0.0))
            return [
                sum(cells[level * nx + EDGE * i : level * nx + EDGE * (i + 1)] for i in range(2 * windows))
                for level in range(levels)
            ]

        even = px % 2 == 0
        one, two = first_ref[...], second_ref[second_ref.shape[0] - EDGE :]
        above, below = jnp.where(even, two, one), jnp.where(even, one, two)
        beside = spread(columns_ref[sums:])
        beside_above, beside_below = corners(above), corners(below)
        blank = jnp.zeros((EDGE - windows, lanes), jnp.float32)
        for level in range(levels):
            pair, part = level // 2, level % 2

            def line(block):
                return block[pair * windows : (pair + 1) * windows, part * ny : (part + 1) * ny]

            up = jnp.concatenate([line(above), beside_above[level][:windows]], 1)
            down = jnp.concatenate([line(below), beside_below[level][:windows]], 1)
            middle = jnp.concatenate([state_ref[0, level], beside[level * nx : (level + 1) * nx]], 1)
            field = jnp.concatenate([blank, up, middle, down, blank], 0)
            field = jnp.where(inside, field, 0.0)
            for _ in range(windows):
                around = (
                    pltpu.roll(field, 1, 0)
                    + pltpu.roll(field, rows - 1, 0)
                    + pltpu.roll(field, 1, 1)
                    + pltpu.roll(field, lanes - 1, 1)
                )
                field = jnp.where(inside, field + RATE * (around - 4.0 * field), 0.0)
            out_ref[level] = field[EDGE : EDGE + nx, :ny]

    return call(
        kernel, shape_of(levels, nx, ny), state, columns, first, second, jnp.asarray(bf16(place))
    )


def prepare(plan, drive, nest_offsets):
    modes, lanes, levels, windows = plan.modes, plan.lanes, plan.levels, plan.windows
    nx, ny, x, y = plan.nx, plan.ny, plan.x, plan.y
    steps = plan.nest - 1
    maps_x = f32(np.stack([np.tile(x[name], (1, 2)) for name in ("cos_map", "sin_map")]))
    maps_y = f32(np.stack([kron(2, y[name].T) for name in ("cos_map", "sin_map")]))
    rows_x = np.stack([np.tile(p, (1, 2)).reshape(plan.px, nx, 2 * modes) for p in x["powers"][:windows]], 1)
    rows_y = np.stack(
        [p.reshape(plan.py, ny, modes).transpose(0, 2, 1) for p in y["powers"][:windows]], 1
    )

    def kernel(
        drive_ref, maps_x_ref, maps_y_ref, rows_x_ref, rows_y_ref, offsets_ref,
        drive_out, row_out, col_out, spread_x_out, spread_y_out,
    ):
        nest, px, py = lax.axis_index("nest"), lax.axis_index("px"), lax.axis_index("py")
        for w in range(windows):
            drive_out[w] = jnp.concatenate([drive_ref[w, level] for level in range(levels)], 1)
        lane = lax.broadcasted_iota(jnp.int32, (modes, 2 * modes), 1)

        def as_left(twice):
            rounded = twice.astype(jnp.bfloat16).astype(jnp.float32)
            pair = jnp.where(lane >= modes, twice - rounded, rounded)
            return jnp.concatenate([pair, rounded], 1)[:, : 3 * modes].astype(jnp.bfloat16)

        def angle(mode, offset, cells):
            turn = (mode * offset).astype(jnp.float32)
            turn = turn - jnp.floor(turn / (2.0 * cells)) * (2.0 * cells)
            return turn * (math.pi / cells)

        mode = lax.broadcasted_iota(jnp.int32, (EDGE, 2 * modes), 1) % modes
        row = lax.broadcasted_iota(jnp.int32, (EDGE, 2 * modes), 0)
        upright = lax.broadcasted_iota(jnp.int32, (2 * modes, 2 * modes), 0) % modes
        place = lax.broadcasted_iota(jnp.int32, (2 * modes, 2 * modes), 1)
        along, down = jnp.zeros_like(mode), jnp.zeros_like(upright)
        for slot in range(steps):
            domain = jnp.maximum(nest - slot, 0)
            along = jnp.where(row == slot, offsets_ref[0, domain], along)
            down = jnp.where(place == slot, offsets_ref[1, domain], down)
        along = angle(mode, along, nx * plan.px)
        down = angle(upright, down, ny * plan.py)
        cos_x, sin_x = jnp.cos(along), jnp.sin(along)
        cos_y, sin_y = jnp.cos(down), jnp.sin(down)
        for slot in range(steps):
            at = slice(slot, slot + 1)
            row_out[slot] = as_left(maps_x_ref[0] * cos_x[at] - maps_x_ref[1] * sin_x[at])
            col_map = maps_y_ref[0] * cos_y[:, at] - maps_y_ref[1] * sin_y[:, at]
            high, small = halves(col_map)
            col_out[slot] = jnp.concatenate([high, small], 1)
        for w in range(windows):
            p = windows - 1 - w
            for j in range(p + 1):
                combined = sum(multinomial(p, i, j) * rows_x_ref[px, i] for i in range(p - j + 1))
                at = (sum(range(p + 1)) + j) * nx
                spread_x_out[at : at + nx] = as_left(combined)
        for j in range(windows):
            table = rows_y_ref[py, j]
            blank = jnp.zeros_like(table)
            table = jnp.concatenate(
                [jnp.concatenate([table, blank], 1), jnp.concatenate([blank, table], 1)], 0
            )
            high, small = halves(table)
            spread_y_out[j] = jnp.concatenate([high, small], 0)

    shapes = (
        shape_of(windows, modes, lanes),
        shape_of(steps, modes, 3 * modes, kind=jnp.bfloat16),
        shape_of(steps, 2 * modes, 4 * modes, kind=jnp.bfloat16),
        shape_of(sum(range(windows + 1)) * nx, 3 * modes, kind=jnp.bfloat16),
        shape_of(windows, 4 * modes, 2 * ny, kind=jnp.bfloat16),
    )
    return call(kernel, shapes, drive, maps_x, maps_y, f32(rows_x), f32(rows_y), nest_offsets.T, first=True)


def own_tables(plan):
    x, y, modes, windows = plan.x, plan.y, plan.modes, plan.windows
    inward = np.concatenate([np.tile(y["spill"][j].T, (1, 2)) for j in range(1, windows + 1)], 1)
    high, small = parts_of(inward)
    inward = jnp.asarray(np.concatenate([high, small, high, np.zeros_like(high)], 0))
    corner = np.concatenate(
        [kron(2, np.repeat(y["spill"][j].T, EDGE, 0)) for j in range(1, windows + 1)], 1
    )
    high, small = parts_of(corner)
    corner = jnp.asarray(np.concatenate([high, small], 0))
    across = np.zeros((windows * modes, windows * EDGE))
    for n in range(1, windows + 1):
        for j in range(n):
            across[(n - 1) * modes : n * modes, j * EDGE : (j + 1) * EDGE] = sum(
                multinomial(n, i, j) * x["spill"][i] for i in range(1, n - j + 1)
            )
    high, small = parts_of(across)
    across = jnp.asarray(np.pad(np.concatenate([high, small, high], 1), ((0, 0), (0, 3 * EDGE))))
    scale_x = f32(np.broadcast_to(1.0 + x["factor"][:, None], (modes, plan.lanes)))
    scale_y = f32(np.broadcast_to(np.tile(y["factor"], plan.levels), (EDGE, plan.lanes)))
    return inward, corner, across, scale_x, scale_y


def own_modes_of(plan, inward_ref, corner_ref, across_ref, scale_x_ref, scale_y_ref):
    modes, low, lanes, sums = plan.modes, plan.low, plan.lanes, plan.sums
    windows, half, ny = plan.windows, plan.half, plan.ny
    scale_x, scale_y = scale_x_ref[...], scale_y_ref[:1]
    row = lax.broadcasted_iota(jnp.int32, (EDGE, lanes), 0)
    lane = lax.broadcasted_iota(jnp.int32, (EDGE, lanes), 1)
    mine = lane % EDGE == row
    left_lane = lax.broadcasted_iota(jnp.int32, (modes, ny), 1) < modes

    def own_modes(message):
        rows, ends = message[:modes], message[modes:low]
        sides = dot(short_stacked(message[low:sums], 4 * EDGE), inward_ref[...], ((0,), (0,)))
        cells = jnp.where(mine, jnp.broadcast_to(ends[EDGE - 2 : EDGE - 1], (EDGE, lanes)), 0.0)
        cells = jnp.concatenate([cells[:, i * ny : (i + 1) * ny] for i in range(half)], 0)
        cells = by_parts(cells, corner_ref[:ny], corner_ref[ny:])
        turned, ends = [rows], [ends]
        for j in range(windows):
            at = slice(j * ny, (j + 1) * ny)
            side = [
                jnp.where(
                    left_lane,
                    sides[2 * i * modes : (2 * i + 1) * modes, at],
                    sides[(2 * i + 1) * modes : (2 * i + 2) * modes, at],
                )
                for i in range(half)
            ]
            cell = [cells[i * EDGE : (i + 1) * EDGE, at] for i in range(half)]
            power = scale_y if j == 0 else power * scale_y
            turned.append(rows * power + jnp.concatenate(side, 1))
            ends.append(ends[0] * power + jnp.concatenate(cell, 1))
        over = dot(across_ref[...], short_stacked(jnp.concatenate(ends[:windows], 0), 12 * EDGE))
        result = []
        for n in range(windows):
            turned = [a * scale_x + b for a, b in zip(turned[:-1], turned[1:])]
            result.append(turned[0] + over[n * modes : (n + 1) * modes])
        return result

    return own_modes


def own_early(plan, tables, messages):
    def kernel(*refs):
        count = len(messages)
        own_modes = own_modes_of(plan, *refs[count : count + len(tables)])
        for i in range(count):
            for w, value in enumerate(own_modes(refs[i][...])):
                refs[count + len(tables)][i, w] = value

    return call(kernel, shape_of(len(messages), plan.windows, plan.modes, plan.lanes), *messages, *tables)


def nudge(plan, stepped, gathered, early, tables, crossed, prepared):
    modes, low, lanes, levels = plan.modes, plan.low, plan.lanes, plan.levels
    windows, half, nx, ny = plan.windows, plan.half, plan.nx, plan.ny
    x, y = plan.x, plan.y
    pairs, unpairs = plan.pairs, plan.unpairs
    again = []
    for p in range(1, windows):
        again.append(sum(multinomial(p, i, 0) * x["within"][i] for i in range(p + 1)))
    again = left_table(np.concatenate(again, 0))
    sideways = jnp.stack([right_table(kron(2, y["within"][j])) for j in range(1, windows)])
    drive, row_maps, col_maps, spread_x, spread_y = prepared

    def kernel(
        stepped_ref, drive_ref, row_ref, col_ref, spread_x_ref, spread_y_ref, again_ref, sideways_ref,
        early_ref, *refs,
    ):
        refs, (state_ref, modes_ref) = refs[:-2], refs[-2:]
        root = plan.nest - 1
        nest = lax.axis_index("nest")
        refs, table_refs = refs[: plan.nest], refs[plan.nest :]
        gains = [ref[low - 1 : low] for ref in refs]
        owns = [[early_ref[i, w] for w in range(windows)] for i in range(root)]
        owns.append(own_modes_of(plan, *table_refs)(refs[root][...]))
        if crossed:
            odd = nest % 2 == 1
            gains = [gains[0], jnp.where(odd, gains[2], gains[3]), gains[1], gains[3]]
            mixed = [jnp.where(odd, a, b) for a, b in zip(owns[2], owns[3])]
            owns = [owns[0], mixed, owns[1], owns[3]]
        coeffs, changes, later = {}, {}, {}
        for front in range(root + windows):
            cells = [(root - front + w, w) for w in range(windows) if 0 <= root - front + w <= root]
            inner, lefts, rights = {}, {}, {}
            for slot, w in cells:
                if slot < root:
                    inner[slot, w] = times_right(pairs(coeffs[slot + 1, w]), col_ref[slot])
                if w > 0:
                    change = changes[slot, w - 1]
                    count = windows - w
                    left = dot(again_ref[: count * modes], stacked(change))
                    lefts[slot] = left = [left[i * modes : (i + 1) * modes] for i in range(count)]
                    rights[slot] = [unpairs(times_right(pairs(change), sideways_ref[i])) for i in range(count)]
                    later[slot, w - 1, 1] = left[0] + rights[slot][0]
            for slot, w in cells:
                target = drive_ref[w]
                if slot < root:
                    found = dot(row_ref[slot], stacked(unpairs(inner[slot, w])))
                    target = jnp.where(nest <= slot, target, found)
                before = owns[slot][w]
                for v in range(w):
                    before = before + later[slot, v, w - v]
                changes[slot, w] = gains[slot] * (target - before)
                coeffs[slot, w] = before + changes[slot, w]
            for slot, w in cells:
                if w > 0 and windows - w > 1:
                    left, right = lefts[slot], rights[slot]
                    mixed = unpairs(times_right(pairs(left[0]), sideways_ref[0]))
                    later[slot, w - 1, 2] = left[1] + (2.0 * mixed + right[1])
        changes = [changes[0, w] for w in range(windows)]
        coeffs = [coeffs[0, w] for w in range(windows)]
        for level in range(levels):
            modes_ref[0, level] = coeffs[-1][:, level * modes : (level + 1) * modes]
        spread = [0.0] * windows
        for w in range(windows):
            p = windows - 1 - w
            at = sum(range(p + 1)) * nx
            found = dot(spread_x_ref[at : at + (p + 1) * nx], stacked(changes[w]))
            for j in range(p + 1):
                spread[j] = spread[j] + found[j * nx : (j + 1) * nx]
        field = 0.0
        for j in range(windows):
            table = spread_y_ref[j]
            part = by_parts(pairs(spread[j]), table[: 2 * modes], table[2 * modes :])
            field = field + part
        for level in range(levels):
            at_row, at = level // 2 * nx, level % 2 * ny
            state_ref[0, level] = stepped_ref[level] + field[at_row : at_row + nx, at : at + ny]

    return call(
        kernel,
        (shape_of(1, levels, nx, ny), shape_of(1, levels, modes, modes)),
        stepped, drive, row_maps, col_maps, spread_x, spread_y, again, sideways, early, *gathered, *tables,
        final=True,
    )


def swap(value, axis, partner):
    size = math.prod(lax.axis_size(name) for name in (axis if isinstance(axis, tuple) else (axis,)))
    return lax.ppermute(value, axis, [(i, partner(i)) for i in range(size) if 0 <= partner(i) < size])


def body(initial_state, drive_modes, relax_rates, nest_offsets):
    plan = Plan(initial_state, drive_modes)
    share, along = project(plan, initial_state, relax_rates)
    if plan.py == 2 and plan.px == 4:
        share, drive_modes, nest_offsets = lax.optimization_barrier((share, drive_modes, nest_offsets))
        from_y = swap(share, "py", lambda i: i ^ 1)
        from_x = swap(along, "px", lambda i: i ^ 1)
        from_both = swap(share, ("py", "px"), lambda i: i ^ (plan.px + 1))
        prepared = prepare(plan, drive_modes, nest_offsets)
        from_both, prepared = lax.optimization_barrier((from_both, prepared))
        total, halo = join_first(plan, share, from_y, from_x, from_both, initial_state)
        columns = from_y
        across = swap(total, "px", lambda i: i ^ 3)
        last = join_last(plan, total, across)
    else:
        from_right = jnp.arange(plan.rows)[:, None] < plan.sums + plan.windows
        right = swap(share, "py", lambda i: i - 1)
        left = swap(share, "py", lambda i: i + 1)
        columns = jnp.where(from_right, right, left)
        top, bottom = both_facing(plan, initial_state, columns)
        above = swap(bottom, "px", lambda i: i + 1)
        below = swap(top, "px", lambda i: i - 1)
        even = lax.axis_index("px") % 2 == 0
        halo, across = jnp.where(even, below, above), jnp.where(even, above, below)
        last = lax.psum(share[: plan.sums], ("py", "px"))
        prepared = prepare(plan, drive_modes, nest_offsets)
    crossed = plan.nest == 4
    if crossed:
        core = swap(last, "nest", lambda i: i ^ 1)
        chip = swap(last, "nest", lambda i: i ^ 2)
        stepped = step_patch(plan, initial_state, columns, halo, across)
        chip, stepped = lax.optimization_barrier((chip, stepped))
        gathered = [last, chip, core, swap(chip, "nest", lambda i: i ^ 1)]
    else:
        gathered = [last] + [swap(last, "nest", lambda i, s=s: i + s) for s in range(1, plan.nest)]
        stepped = step_patch(plan, initial_state, columns, halo, across)
    tables = own_tables(plan)
    early = own_early(plan, tables, gathered[:-1])
    return nudge(plan, stepped, gathered, early, tables, crossed, prepared)


def solution(mesh):
    return jax.shard_map(
        body,
        mesh=mesh,
        in_specs=(P("nest", None, "px", "py"), P(), P("nest", None), P()),
        out_specs=(P("nest", None, "px", "py"), P("nest", None, None, None)),
        check_vma=False,
    )
```

```python
import functools
import math

import jax
import jax.numpy as jnp
import numpy as np
from jax import lax
from jax.experimental import pallas as pl
from jax.experimental.pallas import tpu as pltpu
from jax.sharding import PartitionSpec as P

RATIO = 3
RATE = 0.2
EDGE = 8
INTERPRET = False


def multinomial(n, i, j):
    return math.factorial(n) // (math.factorial(i) * math.factorial(j) * math.factorial(n - i - j))


@functools.lru_cache(maxsize=None)
def tables(cells, modes, order):
    cell = np.arange(cells)
    mode = np.arange(modes)
    weight = np.sqrt(np.where(mode == 0, 1.0, 2.0) / cells)
    product = mode[None] * (2 * cell[:, None] + 1)
    coarse = np.pi * (product % (4 * cells)) / (2 * cells)
    fine = np.pi * (product % (4 * RATIO * cells)) / (2 * RATIO * cells)
    base = weight * np.cos(coarse)
    second = RATE * (np.eye(cells, k=1) + np.eye(cells, k=-1) - 2 * np.eye(cells))
    powers = [base]
    for _ in range(order):
        powers.append(second @ powers[-1])
    factor = RATE * (2 * np.cos(np.pi * mode / cells) - 2)
    places = list(range(order)) + list(range(cells - order, cells))
    edges = np.zeros((cells, EDGE))
    edges[places, range(2 * order)] = 1
    spill = [(powers[i] - base * factor**i).T @ edges for i in range(order + 1)]
    return {
        "base": base,
        "edges": edges,
        "powers": powers,
        "factor": factor,
        "spill": spill,
        "within": [base.T @ power for power in powers],
        "cos_map": base.T @ (weight * np.cos(fine)),
        "sin_map": base.T @ (weight * np.sin(fine)),
    }


def kron(count, block):
    return np.kron(np.eye(count), block)


def f32(value):
    return jnp.asarray(np.asarray(value, np.float32))


def bf16(value):
    return np.asarray(value, jnp.bfloat16)


def parts_of(value):
    high = bf16(value)
    return high, bf16(value - high.astype(np.float64))


def left_table(value):
    high, low = parts_of(value)
    return jnp.asarray(np.concatenate([high, low, high], -1))


def right_table(value):
    return jnp.asarray(np.concatenate(parts_of(value), -1))


def halves(value):
    high = value.astype(jnp.bfloat16)
    return high, (value - high.astype(jnp.float32)).astype(jnp.bfloat16)


def dot(a, b, dims=((1,), (0,))):
    return lax.dot_general(a, b, (dims, ((), ())), preferred_element_type=jnp.float32)


def stacked(value):
    high, low = halves(value)
    return jnp.concatenate([high, high, low], 0)


def short_stacked(value, rows):
    high = value.astype(jnp.bfloat16).astype(jnp.float32)
    blank = jnp.zeros((rows - 3 * value.shape[0], value.shape[1]), jnp.float32)
    return jnp.concatenate([high, high, value - high, blank], 0).astype(jnp.bfloat16)


def times_right(value, table):
    width = table.shape[1] // 2
    lower = jnp.concatenate([table[:, :width], jnp.zeros_like(table[:, width:])], 1)
    out = dot(jnp.concatenate(halves(value), 1), jnp.concatenate([table, lower], 0))
    return out[:, :width] + out[:, width:]


def by_parts(value, table, rest):
    high, low = halves(value)
    out = dot(jnp.concatenate([high, low], 0), table)
    return out[: value.shape[0]] + out[value.shape[0] :] + dot(high, rest)


def in_vmem(value):
    return value if INTERPRET else pltpu.with_memory_space_constraint(value, pltpu.VMEM)


def call(kernel, shapes, *args, first=False, final=False):
    scalars = [a.ndim == 2 and a.size <= 16 for a in args]
    specs = [pl.BlockSpec(memory_space=pltpu.SMEM if s else pltpu.VMEM) for s in scalars]
    if not final and not INTERPRET:
        shapes = jax.tree.map(lambda s: pltpu.VMEM(s.shape, s.dtype), shapes)
    return pl.pallas_call(
        kernel,
        in_specs=specs,
        out_specs=jax.tree.map(lambda _: pl.BlockSpec(memory_space=pltpu.VMEM), shapes),
        out_shape=shapes,
        interpret=INTERPRET,
    )(*[a if s or first else in_vmem(a) for a, s in zip(args, scalars)])


def shape_of(*dims, kind=jnp.float32):
    return jax.ShapeDtypeStruct(dims, kind)


class Plan:
    def __init__(self, initial_state, drive_modes):
        _, self.levels, self.nx, self.ny = initial_state.shape
        self.windows, _, self.modes, _ = drive_modes.shape
        self.px = lax.axis_size("px")
        self.py = lax.axis_size("py")
        self.nest = lax.axis_size("nest")
        self.lanes = self.levels * self.modes
        self.half = self.levels // 2
        self.low = self.modes + EDGE
        self.rows = self.low + EDGE
        self.x = tables(self.nx * self.px, self.modes, self.windows)
        self.y = tables(self.ny * self.py, self.modes, self.windows)
        assert self.levels % 4 == 0 and self.modes * 2 == self.ny and self.nx == self.modes
        assert self.windows == 3 and self.half == 2 and EDGE * EDGE == self.modes

    def pairs(self, value):
        width = 2 * self.modes
        return jnp.concatenate([value[:, i * width : (i + 1) * width] for i in range(self.half)], 0)

    def unpairs(self, value):
        rows = value.shape[0] // self.half
        return jnp.concatenate([value[i * rows : (i + 1) * rows] for i in range(self.half)], 1)


def project(plan, state, rates, halved):
    low, half, lanes, levels = plan.low, plan.half, plan.lanes, plan.levels
    modes, nx, ny, windows = plan.modes, plan.nx, plan.ny, plan.windows
    bases = np.concatenate([plan.x["base"], plan.x["edges"], np.zeros((nx * plan.px, EDGE))], 1)
    left = left_table(bases.T.reshape(low + EDGE, plan.px, nx).transpose(1, 0, 2))
    base_y = plan.y["base"].reshape(plan.py, ny, modes)
    edge_y = plan.y["edges"].reshape(plan.py, ny, EDGE)
    right, corner, edge = [], [], []
    for at in range(plan.py):
        high, small = parts_of(kron(2, base_y[at]))
        right.append(np.concatenate([high, small], 1))
        corner.append(bf16(kron(2, np.repeat(edge_y[at], EDGE, 1))))
        edge.append(bf16(np.pad(np.tile(edge_y[at].T, (1, 2)), ((0, EDGE), (0, 0)))))
    pick = np.zeros((2 * EDGE, 2 * ny))
    for i in range(windows):
        pick[i, [i, ny + i]] = 1
        pick[windows + i, [ny - windows + i, 2 * ny - windows + i]] = 1

    def kernel(state_ref, left_ref, right_ref, corner_ref, edge_ref, pick_ref, rates_ref, out_ref, along_ref):
        px, py = lax.axis_index("px"), lax.axis_index("py")
        field = jnp.concatenate([state_ref[0, level] for level in range(levels)], 1)
        rows = dot(left_ref[px], stacked(field))
        width = 2 * ny
        both = jnp.concatenate([rows[:low, i * width : (i + 1) * width] for i in range(half)], 0)
        high, small = halves(both)
        table = right_ref[py]
        found = dot(high, table)
        found = found[:, :ny] + found[:, ny:] + dot(small, table[:, :ny])
        out_ref[:modes] = jnp.concatenate([found[i * low : i * low + modes] for i in range(half)], 1)
        ends = jnp.concatenate([found[i * low + modes : (i + 1) * low] for i in range(half)], 1)
        cells = jnp.concatenate([rows[modes:low, i * width : (i + 1) * width] for i in range(half)], 0)
        cells = dot(jnp.concatenate(halves(cells), 0), corner_ref[py])
        cells = cells[: half * EDGE] + cells[half * EDGE :]
        cells = jnp.concatenate([cells[i * EDGE : (i + 1) * EDGE] for i in range(half)], 1)
        row = lax.broadcasted_iota(jnp.int32, (EDGE, lanes), 0)
        lane = lax.broadcasted_iota(jnp.int32, (EDGE, lanes), 1)
        cells = jnp.sum(jnp.where(lane % EDGE == row, cells, 0.0), 0, keepdims=True)
        lane = lane[:1]
        gain = jnp.zeros((1, lanes), jnp.float32)
        for i in range(levels):
            gain = jnp.where(lane // modes == i, rates_ref[0, i], gain)
        gain = jnp.where((px == 0) & (py == 0) & (lane % modes >= 2 * windows * EDGE), gain, 0.0)
        upright = jnp.concatenate([rows[:modes, i * ny : (i + 1) * ny] for i in range(levels)], 0)
        upright = jnp.concatenate(halves(upright), 1)
        sides = dot(edge_ref[py], upright, ((1,), (1,)))[: 2 * windows]
        patch = jnp.concatenate([state_ref[0, level] for level in range(levels)], 0)
        patch = jnp.concatenate(halves(patch), 1)
        columns = dot(pick_ref[...], patch, ((1,), (1,)))[:EDGE]
        if halved:
            ends = jnp.where(px < plan.px // 2, ends[:windows], ends[windows : 2 * windows])
            out_ref[modes:low] = jnp.concatenate([sides, cells + gain, ends[:1]], 0)
            out_ref[low:] = jnp.concatenate([ends[1:], columns[: 2 * windows]], 0)
            along_ref[:low] = out_ref[:low]
            along_ref[low:] = jnp.concatenate([ends[1:], facing_rows(plan, state_ref, px % 2 == 0)], 0)
        else:
            blank = jnp.zeros((2, lanes), jnp.float32)
            out_ref[modes:low] = jnp.concatenate([sides, cells + gain, blank[:1]], 0)
            out_ref[low:] = jnp.concatenate([ends[: 2 * windows], blank], 0)
            along_ref[...] = columns

    return call(
        kernel,
        (shape_of(plan.rows, lanes), shape_of(plan.rows if halved else EDGE, lanes)),
        state, left, jnp.asarray(np.stack(right)), jnp.asarray(np.stack(corner)), jnp.asarray(np.stack(edge)),
        jnp.asarray(bf16(pick)), rates,
        first=True,
    )


def facing_rows(plan, state_ref, bottom):
    rows = []
    for group in range(plan.half):
        pair = [state_ref[0, 2 * group + i] for i in range(2)]
        top = jnp.concatenate([p[: plan.windows] for p in pair], 1)
        end = jnp.concatenate([p[plan.nx - plan.windows :] for p in pair], 1)
        rows.append(jnp.where(bottom, end, top))
    return jnp.concatenate(rows, 0)


def facing_corners(plan, columns, bottom):
    lane = lax.broadcasted_iota(jnp.int32, columns.shape, 1)
    moved = pltpu.roll(columns, plan.lanes - (plan.nx - plan.windows), 1)
    near = jnp.where(lane % plan.nx < plan.windows, jnp.where(bottom, moved, columns), 0.0)
    first = columns.shape[0] - 2 * plan.windows
    packed = near[first : first + 1]
    for i in range(1, 2 * plan.windows):
        packed = packed + pltpu.roll(near, EDGE * i, 1)[first + i : first + i + 1]
    return packed


def join_first(plan, own, from_y, from_x, from_both, state):
    low, modes, windows, lanes = plan.low, plan.modes, plan.windows, plan.lanes

    def kernel(own_ref, y_ref, x_ref, both_ref, state_ref, out_ref, halo_ref):
        px = lax.axis_index("px")
        odd, lower = px % 2 == 1, px < plan.px // 2
        out_ref[:modes] = (own_ref[:modes] + y_ref[:modes]) + (x_ref[:modes] + both_ref[:modes])
        middle = (own_ref[modes:low] + y_ref[modes:low]) + (x_ref[modes:low] + both_ref[modes:low])
        corners = facing_corners(plan, y_ref[low:], odd)
        corners = jnp.where(lower, pltpu.roll(corners, windows, 1), corners)
        row = lax.broadcasted_iota(jnp.int32, (EDGE, lanes), 0)
        out_ref[modes:low] = middle + jnp.where(row == 2 * windows, corners, 0.0)
        ends = (own_ref[low:] + y_ref[low:]) + (x_ref[low:] + both_ref[low:])
        out_ref[low:] = jnp.concatenate([ends[: windows - 1], facing_rows(plan, state_ref, odd)], 0)
        corners = facing_corners(plan, both_ref[low:], odd)
        lines = x_ref[low:][windows - 1 :]
        halo_ref[...] = jnp.concatenate([lines, corners, jnp.zeros((1, lanes), jnp.float32)], 0)

    shapes = shape_of(plan.rows, lanes), shape_of(EDGE, lanes)
    return call(kernel, shapes, own, from_y, from_x, from_both, state)


def both_facing(plan, state, columns):
    def kernel(state_ref, columns_ref, top_ref, bottom_ref):
        columns = columns_ref[...]
        columns = jnp.concatenate([jnp.zeros((2, plan.lanes), jnp.float32), columns[: 2 * plan.windows]], 0)
        for ref, bottom in ((top_ref, False), (bottom_ref, True)):
            rows = [facing_rows(plan, state_ref, bottom), facing_corners(plan, columns, bottom)]
            ref[...] = jnp.concatenate(rows + [jnp.zeros((1, plan.lanes), jnp.float32)], 0)

    return call(kernel, (shape_of(EDGE, plan.lanes),) * 2, state, columns)


def join_last(plan, own, other):
    low, modes, windows, lanes = plan.low, plan.modes, plan.windows, plan.lanes

    def kernel(own_ref, other_ref, out_ref):
        lower = lax.axis_index("px") < plan.px // 2
        out_ref[:modes] = own_ref[:modes] + other_ref[:modes]
        row = lax.broadcasted_iota(jnp.int32, (EDGE, lanes), 0)
        lane = lax.broadcasted_iota(jnp.int32, (EDGE, lanes), 1)
        one, two = own_ref[modes:low], other_ref[modes:low]
        early, late = jnp.where(lower, one, two), jnp.where(lower, two, one)
        kept = (row < 2 * windows) | (lane % modes >= 2 * windows * EDGE)
        middle = jnp.where(kept | (lane % EDGE < windows), early, 0.0)
        middle = middle + jnp.where(kept | (lane % EDGE >= windows), late, 0.0)
        out_ref[modes:low] = jnp.where(row <= 2 * windows, middle, 0.0)
        ends = []
        for block, rest in ((early, jnp.where(lower, own_ref[low:], other_ref[low:])),
                            (late, jnp.where(lower, other_ref[low:], own_ref[low:]))):
            ends += [block[EDGE - 1 :], rest[: windows - 1]]
        out_ref[low:] = jnp.concatenate(ends + [jnp.zeros((EDGE - 2 * windows, lanes), jnp.float32)], 0)

    return call(kernel, shape_of(plan.rows, lanes), own, other)


def step_patch(plan, state, columns, first, second):
    nx, ny, windows, low, levels = plan.nx, plan.ny, plan.windows, plan.low, plan.levels
    place = np.zeros((4 * EDGE, ny))
    for i in range(windows):
        for part in range(3):
            place[part * EDGE + i, i] = 1
            place[part * EDGE + windows + i, ny - windows + i] = 1
    rows, lanes = nx + 2 * EDGE, 2 * ny

    def kernel(state_ref, columns_ref, first_ref, second_ref, place_ref, out_ref):
        px, py = lax.axis_index("px"), lax.axis_index("py")
        row = lax.broadcasted_iota(jnp.int32, (rows, lanes), 0) - EDGE + px * nx
        lane = lax.broadcasted_iota(jnp.int32, (rows, lanes), 1)
        lane = jnp.where(lane >= ny + ny // 2, lane - lanes, lane) + py * ny
        inside = (row >= 0) & (row < nx * plan.px) & (lane >= 0) & (lane < ny * plan.py)
        where = place_ref[...]

        def spread(block):
            high = block.astype(jnp.bfloat16).astype(jnp.float32)
            rest = block - high
            middle = rest.astype(jnp.bfloat16).astype(jnp.float32)
            parts = [high, middle, rest - middle, jnp.zeros_like(high)]
            return dot(jnp.concatenate(parts, 0).astype(jnp.bfloat16), where, ((0,), (0,)))

        small_row = lax.broadcasted_iota(jnp.int32, (EDGE, plan.lanes), 0)
        small_lane = lax.broadcasted_iota(jnp.int32, (EDGE, plan.lanes), 1)
        mine = small_lane % nx // EDGE == small_row

        def corners(block):
            line = jnp.broadcast_to(block[2 * windows : 2 * windows + 1], (EDGE, plan.lanes))
            cells = spread(jnp.where(mine, line, 0.0))
            return [
                sum(cells[level * nx + EDGE * i : level * nx + EDGE * (i + 1)] for i in range(2 * windows))
                for level in range(levels)
            ]

        even = px % 2 == 0
        one, two, columns = first_ref[...], second_ref[-EDGE:], columns_ref[-EDGE:]
        if second_ref.shape[0] > EDGE:
            mixed = second_ref[low - 2 : low - 1]
            mixed = jnp.where(px < plan.px // 2, mixed, pltpu.roll(mixed, plan.lanes - windows, 1))
            two = jnp.concatenate([two[windows - 1 :], mixed, mixed], 0)
            columns = jnp.concatenate([columns[windows - 1 :], columns[: windows - 1]], 0)
        above, below = jnp.where(even, two, one), jnp.where(even, one, two)
        beside = spread(columns)
        beside_above, beside_below = corners(above), corners(below)
        blank = jnp.zeros((EDGE - windows, lanes), jnp.float32)
        for level in range(levels):
            pair, part = level // 2, level % 2

            def line(block):
                return block[pair * windows : (pair + 1) * windows, part * ny : (part + 1) * ny]

            up = jnp.concatenate([line(above), beside_above[level][:windows]], 1)
            down = jnp.concatenate([line(below), beside_below[level][:windows]], 1)
            middle = jnp.concatenate([state_ref[0, level], beside[level * nx : (level + 1) * nx]], 1)
            field = jnp.concatenate([blank, up, middle, down, blank], 0)
            field = jnp.where(inside, field, 0.0)
            for _ in range(windows):
                around = (
                    pltpu.roll(field, 1, 0)
                    + pltpu.roll(field, rows - 1, 0)
                    + pltpu.roll(field, 1, 1)
                    + pltpu.roll(field, lanes - 1, 1)
                )
                field = jnp.where(inside, field + RATE * (around - 4.0 * field), 0.0)
            out_ref[level] = field[EDGE : EDGE + nx, :ny]

    return call(
        kernel, shape_of(levels, nx, ny), state, columns, first, second, jnp.asarray(bf16(place))
    )


def prepare(plan, drive, nest_offsets):
    modes, lanes, levels, windows = plan.modes, plan.lanes, plan.levels, plan.windows
    nx, ny, x, y = plan.nx, plan.ny, plan.x, plan.y
    steps = plan.nest - 1
    maps_x = f32(np.stack([np.tile(x[name], (1, 2)) for name in ("cos_map", "sin_map")]))
    maps_y = f32(np.stack([kron(2, y[name].T) for name in ("cos_map", "sin_map")]))
    rows_x = np.stack([np.tile(p, (1, 2)).reshape(plan.px, nx, 2 * modes) for p in x["powers"][:windows]], 1)
    rows_y = np.stack(
        [p.reshape(plan.py, ny, modes).transpose(0, 2, 1) for p in y["powers"][:windows]], 1
    )

    def kernel(
        drive_ref, maps_x_ref, maps_y_ref, rows_x_ref, rows_y_ref, offsets_ref,
        drive_out, row_out, col_out, spread_x_out, spread_y_out,
    ):
        nest, px, py = lax.axis_index("nest"), lax.axis_index("px"), lax.axis_index("py")
        for w in range(windows):
            drive_out[w] = jnp.concatenate([drive_ref[w, level] for level in range(levels)], 1)
        lane = lax.broadcasted_iota(jnp.int32, (modes, 2 * modes), 1)

        def as_left(twice):
            rounded = twice.astype(jnp.bfloat16).astype(jnp.float32)
            pair = jnp.where(lane >= modes, twice - rounded, rounded)
            return jnp.concatenate([pair, rounded], 1)[:, : 3 * modes].astype(jnp.bfloat16)

        def angle(mode, offset, cells):
            turn = (mode * offset).astype(jnp.float32)
            turn = turn - jnp.floor(turn / (2.0 * cells)) * (2.0 * cells)
            return turn * (math.pi / cells)

        mode = lax.broadcasted_iota(jnp.int32, (EDGE, 2 * modes), 1) % modes
        row = lax.broadcasted_iota(jnp.int32, (EDGE, 2 * modes), 0)
        upright = lax.broadcasted_iota(jnp.int32, (2 * modes, 2 * modes), 0) % modes
        place = lax.broadcasted_iota(jnp.int32, (2 * modes, 2 * modes), 1)
        along, down = jnp.zeros_like(mode), jnp.zeros_like(upright)
        for slot in range(steps):
            domain = jnp.maximum(nest - slot, 0)
            along = jnp.where(row == slot, offsets_ref[0, domain], along)
            down = jnp.where(place == slot, offsets_ref[1, domain], down)
        along = angle(mode, along, nx * plan.px)
        down = angle(upright, down, ny * plan.py)
        cos_x, sin_x = jnp.cos(along), jnp.sin(along)
        cos_y, sin_y = jnp.cos(down), jnp.sin(down)
        for slot in range(steps):
            at = slice(slot, slot + 1)
            row_out[slot] = as_left(maps_x_ref[0] * cos_x[at] - maps_x_ref[1] * sin_x[at])
            col_map = maps_y_ref[0] * cos_y[:, at] - maps_y_ref[1] * sin_y[:, at]
            high, small = halves(col_map)
            col_out[slot] = jnp.concatenate([high, small], 1)
        for w in range(windows):
            p = windows - 1 - w
            for j in range(p + 1):
                combined = sum(multinomial(p, i, j) * rows_x_ref[px, i] for i in range(p - j + 1))
                at = (sum(range(p + 1)) + j) * nx
                spread_x_out[at : at + nx] = as_left(combined)
        for j in range(windows):
            table = rows_y_ref[py, j]
            blank = jnp.zeros_like(table)
            table = jnp.concatenate(
                [jnp.concatenate([table, blank], 1), jnp.concatenate([blank, table], 1)], 0
            )
            high, small = halves(table)
            spread_y_out[j] = jnp.concatenate([high, small], 0)

    shapes = (
        shape_of(windows, modes, lanes),
        shape_of(steps, modes, 3 * modes, kind=jnp.bfloat16),
        shape_of(steps, 2 * modes, 4 * modes, kind=jnp.bfloat16),
        shape_of(sum(range(windows + 1)) * nx, 3 * modes, kind=jnp.bfloat16),
        shape_of(windows, 4 * modes, 2 * ny, kind=jnp.bfloat16),
    )
    return call(kernel, shapes, drive, maps_x, maps_y, f32(rows_x), f32(rows_y), nest_offsets.T, first=True)


def own_tables(plan):
    x, y, modes, windows = plan.x, plan.y, plan.modes, plan.windows
    inward = np.concatenate([np.tile(y["spill"][j].T, (1, 2)) for j in range(1, windows + 1)], 1)
    high, small = parts_of(inward)
    inward = jnp.asarray(np.concatenate([high, small, high, np.zeros_like(high)], 0))
    corner = np.concatenate(
        [kron(2, np.repeat(y["spill"][j].T, EDGE, 0)) for j in range(1, windows + 1)], 1
    )
    high, small = parts_of(corner)
    corner = jnp.asarray(np.concatenate([high, small], 0))
    across = np.zeros((windows * modes, windows * EDGE))
    for n in range(1, windows + 1):
        for j in range(n):
            across[(n - 1) * modes : n * modes, j * EDGE : (j + 1) * EDGE] = sum(
                multinomial(n, i, j) * x["spill"][i] for i in range(1, n - j + 1)
            )
    high, small = parts_of(across)
    across = jnp.asarray(np.pad(np.concatenate([high, small, high], 1), ((0, 0), (0, 3 * EDGE))))
    scale_x = f32(np.broadcast_to(1.0 + x["factor"][:, None], (modes, plan.lanes)))
    scale_y = f32(np.broadcast_to(np.tile(y["factor"], plan.levels), (EDGE, plan.lanes)))
    return inward, corner, across, scale_x, scale_y


def own_modes_of(plan, inward_ref, corner_ref, across_ref, scale_x_ref, scale_y_ref):
    modes, low, lanes = plan.modes, plan.low, plan.lanes
    windows, half, ny = plan.windows, plan.half, plan.ny
    scale_x, scale_y = scale_x_ref[...], scale_y_ref[:1]
    row = lax.broadcasted_iota(jnp.int32, (EDGE, lanes), 0)
    lane = lax.broadcasted_iota(jnp.int32, (EDGE, lanes), 1)
    mine = lane % EDGE == row
    left_lane = lax.broadcasted_iota(jnp.int32, (modes, ny), 1) < modes

    def own_modes(message):
        rows, middle, ends = message[:modes], message[modes:low], message[low:]
        sides = dot(short_stacked(middle, 4 * EDGE), inward_ref[...], ((0,), (0,)))
        cells = jnp.where(mine, jnp.broadcast_to(middle[EDGE - 2 : EDGE - 1], (EDGE, lanes)), 0.0)
        cells = jnp.concatenate([cells[:, i * ny : (i + 1) * ny] for i in range(half)], 0)
        cells = by_parts(cells, corner_ref[:ny], corner_ref[ny:])
        turned, ends = [rows], [ends]
        for j in range(windows):
            at = slice(j * ny, (j + 1) * ny)
            side = [
                jnp.where(
                    left_lane,
                    sides[2 * i * modes : (2 * i + 1) * modes, at],
                    sides[(2 * i + 1) * modes : (2 * i + 2) * modes, at],
                )
                for i in range(half)
            ]
            cell = [cells[i * EDGE : (i + 1) * EDGE, at] for i in range(half)]
            power = scale_y if j == 0 else power * scale_y
            turned.append(rows * power + jnp.concatenate(side, 1))
            ends.append(ends[0] * power + jnp.concatenate(cell, 1))
        over = dot(across_ref[...], short_stacked(jnp.concatenate(ends[:windows], 0), 12 * EDGE))
        result = []
        for n in range(windows):
            turned = [a * scale_x + b for a, b in zip(turned[:-1], turned[1:])]
            result.append(turned[0] + over[n * modes : (n + 1) * modes])
        return result

    return own_modes


def own_early(plan, tables, messages):
    def kernel(*refs):
        count = len(messages)
        own_modes = own_modes_of(plan, *refs[count : count + len(tables)])
        for i in range(count):
            for w, value in enumerate(own_modes(refs[i][...])):
                refs[count + len(tables)][i, w] = value

    return call(kernel, shape_of(len(messages), plan.windows, plan.modes, plan.lanes), *messages, *tables)


def nudge(plan, stepped, gathered, early, tables, crossed, prepared):
    modes, low, lanes, levels = plan.modes, plan.low, plan.lanes, plan.levels
    windows, half, nx, ny = plan.windows, plan.half, plan.nx, plan.ny
    x, y = plan.x, plan.y
    pairs, unpairs = plan.pairs, plan.unpairs
    again = []
    for p in range(1, windows):
        again.append(sum(multinomial(p, i, 0) * x["within"][i] for i in range(p + 1)))
    again = left_table(np.concatenate(again, 0))
    sideways = jnp.stack([right_table(kron(2, y["within"][j])) for j in range(1, windows)])
    drive, row_maps, col_maps, spread_x, spread_y = prepared

    def kernel(
        stepped_ref, drive_ref, row_ref, col_ref, spread_x_ref, spread_y_ref, again_ref, sideways_ref,
        early_ref, *refs,
    ):
        refs, (state_ref, modes_ref) = refs[:-2], refs[-2:]
        root = plan.nest - 1
        nest = lax.axis_index("nest")
        refs, table_refs = refs[: plan.nest], refs[plan.nest :]
        lane = lax.broadcasted_iota(jnp.int32, (1, lanes), 1)
        gains = []
        for ref in refs:
            gain = jnp.where(lane % modes >= modes - 2 * EDGE, ref[low - 2 : low - 1], 0.0)
            gain = gain + pltpu.roll(gain, lanes - 2 * EDGE, 1)
            gains.append(gain + pltpu.roll(gain, lanes - 4 * EDGE, 1))
        owns = [[early_ref[i, w] for w in range(windows)] for i in range(root)]
        owns.append(own_modes_of(plan, *table_refs)(refs[root][...]))
        if crossed:
            odd = nest % 2 == 1
            gains = [gains[0], jnp.where(odd, gains[2], gains[3]), gains[1], gains[3]]
            mixed = [jnp.where(odd, a, b) for a, b in zip(owns[2], owns[3])]
            owns = [owns[0], mixed, owns[1], owns[3]]
        coeffs, changes, later = {}, {}, {}
        for front in range(root + windows):
            cells = [(root - front + w, w) for w in range(windows) if 0 <= root - front + w <= root]
            inner, lefts, rights = {}, {}, {}
            for slot, w in cells:
                if slot < root:
                    inner[slot, w] = times_right(pairs(coeffs[slot + 1, w]), col_ref[slot])
                if w > 0:
                    change = changes[slot, w - 1]
                    count = windows - w
                    left = dot(again_ref[: count * modes], stacked(change))
                    lefts[slot] = left = [left[i * modes : (i + 1) * modes] for i in range(count)]
                    rights[slot] = [unpairs(times_right(pairs(change), sideways_ref[i])) for i in range(count)]
                    later[slot, w - 1, 1] = left[0] + rights[slot][0]
            for slot, w in cells:
                target = drive_ref[w]
                if slot < root:
                    found = dot(row_ref[slot], stacked(unpairs(inner[slot, w])))
                    target = jnp.where(nest <= slot, target, found)
                before = owns[slot][w]
                for v in range(w):
                    before = before + later[slot, v, w - v]
                changes[slot, w] = gains[slot] * (target - before)
                coeffs[slot, w] = before + changes[slot, w]
            for slot, w in cells:
                if w > 0 and windows - w > 1:
                    left, right = lefts[slot], rights[slot]
                    mixed = unpairs(times_right(pairs(left[0]), sideways_ref[0]))
                    later[slot, w - 1, 2] = left[1] + (2.0 * mixed + right[1])
        changes = [changes[0, w] for w in range(windows)]
        coeffs = [coeffs[0, w] for w in range(windows)]
        for level in range(levels):
            modes_ref[0, level] = coeffs[-1][:, level * modes : (level + 1) * modes]
        spread = [0.0] * windows
        for w in range(windows):
            p = windows - 1 - w
            at = sum(range(p + 1)) * nx
            found = dot(spread_x_ref[at : at + (p + 1) * nx], stacked(changes[w]))
            for j in range(p + 1):
                spread[j] = spread[j] + found[j * nx : (j + 1) * nx]
        field = 0.0
        for j in range(windows):
            table = spread_y_ref[j]
            part = by_parts(pairs(spread[j]), table[: 2 * modes], table[2 * modes :])
            field = field + part
        for level in range(levels):
            at_row, at = level // 2 * nx, level % 2 * ny
            state_ref[0, level] = stepped_ref[level] + field[at_row : at_row + nx, at : at + ny]

    return call(
        kernel,
        (shape_of(1, levels, nx, ny), shape_of(1, levels, modes, modes)),
        stepped, drive, row_maps, col_maps, spread_x, spread_y, again, sideways, early, *gathered, *tables,
        final=True,
    )


def swap(value, axis, partner):
    size = math.prod(lax.axis_size(name) for name in (axis if isinstance(axis, tuple) else (axis,)))
    return lax.ppermute(value, axis, [(i, partner(i)) for i in range(size) if 0 <= partner(i) < size])


def body(initial_state, drive_modes, relax_rates, nest_offsets):
    plan = Plan(initial_state, drive_modes)
    halved = plan.py == 2 and plan.px == 4
    share, along = project(plan, initial_state, relax_rates, halved)
    if halved:
        share, drive_modes, nest_offsets = lax.optimization_barrier((share, drive_modes, nest_offsets))
        from_y = swap(share, "py", lambda i: i ^ 1)
        from_x = swap(along, "px", lambda i: i ^ 1)
        from_both = swap(share, ("py", "px"), lambda i: i ^ (plan.px + 1))
        prepared = prepare(plan, drive_modes, nest_offsets)
        from_both, prepared = lax.optimization_barrier((from_both, prepared))
        total, halo = join_first(plan, share, from_y, from_x, from_both, initial_state)
        columns = from_y
        across = swap(total, "px", lambda i: i ^ 3)
        last = join_last(plan, total, across)
    else:
        from_right = jnp.arange(EDGE)[:, None] < plan.windows
        right = swap(along, "py", lambda i: i - 1)
        left = swap(along, "py", lambda i: i + 1)
        columns = jnp.where(from_right, right, left)
        top, bottom = both_facing(plan, initial_state, columns)
        above = swap(bottom, "px", lambda i: i + 1)
        below = swap(top, "px", lambda i: i - 1)
        even = lax.axis_index("px") % 2 == 0
        halo, across = jnp.where(even, below, above), jnp.where(even, above, below)
        last = lax.psum(share, ("py", "px"))
        prepared = prepare(plan, drive_modes, nest_offsets)
    crossed = plan.nest == 4
    if crossed:
        core = swap(last, "nest", lambda i: i ^ 1)
        chip = swap(last, "nest", lambda i: i ^ 2)
        stepped = step_patch(plan, initial_state, columns, halo, across)
        chip, stepped = lax.optimization_barrier((chip, stepped))
        gathered = [last, chip, core, swap(chip, "nest", lambda i: i ^ 1)]
    else:
        gathered = [last] + [swap(last, "nest", lambda i, s=s: i + s) for s in range(1, plan.nest)]
        stepped = step_patch(plan, initial_state, columns, halo, across)
    tables = own_tables(plan)
    early = own_early(plan, tables, gathered[:-1])
    return nudge(plan, stepped, gathered, early, tables, crossed, prepared)


def solution(mesh):
    return jax.shard_map(
        body,
        mesh=mesh,
        in_specs=(P("nest", None, "px", "py"), P(), P("nest", None), P()),
        out_specs=(P("nest", None, "px", "py"), P("nest", None, None, None)),
        check_vma=False,
    )
```

```python
import functools
import math

import jax
import jax.numpy as jnp
import numpy as np
from jax import lax
from jax.experimental import pallas as pl
from jax.experimental.pallas import tpu as pltpu
from jax.sharding import PartitionSpec as P

RATIO = 3
RATE = 0.2
EDGE = 8
INTERPRET = False


def multinomial(n, i, j):
    return math.factorial(n) // (math.factorial(i) * math.factorial(j) * math.factorial(n - i - j))


@functools.lru_cache(maxsize=None)
def tables(cells, modes, order):
    cell = np.arange(cells)
    mode = np.arange(modes)
    weight = np.sqrt(np.where(mode == 0, 1.0, 2.0) / cells)
    product = mode[None] * (2 * cell[:, None] + 1)
    coarse = np.pi * (product % (4 * cells)) / (2 * cells)
    fine = np.pi * (product % (4 * RATIO * cells)) / (2 * RATIO * cells)
    base = weight * np.cos(coarse)
    second = RATE * (np.eye(cells, k=1) + np.eye(cells, k=-1) - 2 * np.eye(cells))
    powers = [base]
    for _ in range(order):
        powers.append(second @ powers[-1])
    factor = RATE * (2 * np.cos(np.pi * mode / cells) - 2)
    places = list(range(order)) + list(range(cells - order, cells))
    edges = np.zeros((cells, EDGE))
    edges[places, range(2 * order)] = 1
    spill = [(powers[i] - base * factor**i).T @ edges for i in range(order + 1)]
    return {
        "base": base,
        "edges": edges,
        "powers": powers,
        "factor": factor,
        "spill": spill,
        "within": [base.T @ power for power in powers],
        "cos_map": base.T @ (weight * np.cos(fine)),
        "sin_map": base.T @ (weight * np.sin(fine)),
    }


def kron(count, block):
    return np.kron(np.eye(count), block)


def f32(value):
    return jnp.asarray(np.asarray(value, np.float32))


def bf16(value):
    return np.asarray(value, jnp.bfloat16)


def parts_of(value):
    high = bf16(value)
    return high, bf16(value - high.astype(np.float64))


def left_table(value):
    high, low = parts_of(value)
    return jnp.asarray(np.concatenate([high, low, high], -1))


def right_table(value):
    return jnp.asarray(np.concatenate(parts_of(value), -1))


def halves(value):
    high = value.astype(jnp.bfloat16)
    return high, (value - high.astype(jnp.float32)).astype(jnp.bfloat16)


def dot(a, b, dims=((1,), (0,))):
    return lax.dot_general(a, b, (dims, ((), ())), preferred_element_type=jnp.float32)


def stacked(value):
    high, low = halves(value)
    return jnp.concatenate([high, high, low], 0)


def short_stacked(value, rows):
    high = value.astype(jnp.bfloat16).astype(jnp.float32)
    blank = jnp.zeros((rows - 3 * value.shape[0], value.shape[1]), jnp.float32)
    return jnp.concatenate([high, high, value - high, blank], 0).astype(jnp.bfloat16)


def times_right(value, table):
    width = table.shape[1] // 2
    lower = jnp.concatenate([table[:, :width], jnp.zeros_like(table[:, width:])], 1)
    out = dot(jnp.concatenate(halves(value), 1), jnp.concatenate([table, lower], 0))
    return out[:, :width] + out[:, width:]


def by_parts(value, table, rest):
    high, low = halves(value)
    out = dot(jnp.concatenate([high, low], 0), table)
    return out[: value.shape[0]] + out[value.shape[0] :] + dot(high, rest)


def in_vmem(value):
    return value if INTERPRET else pltpu.with_memory_space_constraint(value, pltpu.VMEM)


def call(kernel, shapes, *args, first=False, final=False):
    scalars = [a.ndim == 2 and a.size <= 16 for a in args]
    specs = [pl.BlockSpec(memory_space=pltpu.SMEM if s else pltpu.VMEM) for s in scalars]
    if not final and not INTERPRET:
        shapes = jax.tree.map(lambda s: pltpu.VMEM(s.shape, s.dtype), shapes)
    return pl.pallas_call(
        kernel,
        in_specs=specs,
        out_specs=jax.tree.map(lambda _: pl.BlockSpec(memory_space=pltpu.VMEM), shapes),
        out_shape=shapes,
        interpret=INTERPRET,
    )(*[a if s or first else in_vmem(a) for a, s in zip(args, scalars)])


def shape_of(*dims, kind=jnp.float32):
    return jax.ShapeDtypeStruct(dims, kind)


class Plan:
    def __init__(self, initial_state, drive_modes):
        _, self.levels, self.nx, self.ny = initial_state.shape
        self.windows, _, self.modes, _ = drive_modes.shape
        self.px = lax.axis_size("px")
        self.py = lax.axis_size("py")
        self.nest = lax.axis_size("nest")
        self.lanes = self.levels * self.modes
        self.half = self.levels // 2
        self.low = self.modes + EDGE
        self.rows = self.low + EDGE
        self.x = tables(self.nx * self.px, self.modes, self.windows)
        self.y = tables(self.ny * self.py, self.modes, self.windows)
        assert self.levels % 4 == 0 and self.modes * 2 == self.ny and self.nx == self.modes
        assert self.windows == 3 and self.half == 2 and EDGE * EDGE == self.modes

    def pairs(self, value):
        width = 2 * self.modes
        return jnp.concatenate([value[:, i * width : (i + 1) * width] for i in range(self.half)], 0)

    def unpairs(self, value):
        rows = value.shape[0] // self.half
        return jnp.concatenate([value[i * rows : (i + 1) * rows] for i in range(self.half)], 1)


def project(plan, state, rates, halved):
    low, half, lanes, levels = plan.low, plan.half, plan.lanes, plan.levels
    modes, nx, ny, windows = plan.modes, plan.nx, plan.ny, plan.windows
    bases = np.concatenate([plan.x["base"], plan.x["edges"], np.zeros((nx * plan.px, EDGE))], 1)
    left = right_table(bases.T.reshape(low + EDGE, plan.px, nx).transpose(1, 0, 2))
    base_y = plan.y["base"].reshape(plan.py, ny, modes)
    edge_y = plan.y["edges"].reshape(plan.py, ny, EDGE)
    right, edge = [], []
    for at in range(plan.py):
        high, small = parts_of(base_y[at])
        corner = bf16(np.repeat(edge_y[at], EDGE, 1))
        right.append(np.concatenate([high, small, corner, np.zeros_like(corner)], 1))
        edge.append(bf16(np.pad(np.tile(edge_y[at].T, (1, 2)), ((0, EDGE), (0, 0)))))
    pick = np.zeros((2 * EDGE, 2 * ny))
    for i in range(windows):
        pick[i, [i, ny + i]] = 1
        pick[windows + i, [ny - windows + i, 2 * ny - windows + i]] = 1

    def kernel(state_ref, left_ref, right_ref, edge_ref, pick_ref, rates_ref, out_ref, along_ref):
        px, py = lax.axis_index("px"), lax.axis_index("py")
        field = jnp.concatenate([state_ref[0, level] for level in range(levels)], 1)
        high, small = halves(field)
        table = left_ref[px]
        rows = dot(table, jnp.concatenate([high, high], 0)) + dot(table[:, :nx], small)
        found = jnp.concatenate([rows[:low, i * ny : (i + 1) * ny] for i in range(levels)], 0)
        high, small = halves(found)
        table = right_ref[py]
        found = dot(high, table) + dot(small, table)
        both = found[:, :ny] + pltpu.roll(found[:, :ny], modes, 1)
        left_lane = lax.broadcasted_iota(jnp.int32, (low, ny), 1) < modes
        both = [both[i * low : (i + 1) * low] for i in range(levels)]
        both = [jnp.where(left_lane, both[2 * i], both[2 * i + 1]) for i in range(half)]
        both = jnp.concatenate(both, 1)
        out_ref[:modes] = both[:modes]
        ends = both[modes:]
        cells = [found[i * low + modes : (i + 1) * low, ny:] for i in range(levels)]
        cells = [cells[2 * i] + pltpu.roll(cells[2 * i + 1], modes, 1) for i in range(half)]
        cells = jnp.concatenate(cells, 1)
        row = lax.broadcasted_iota(jnp.int32, (EDGE, lanes), 0)
        lane = lax.broadcasted_iota(jnp.int32, (EDGE, lanes), 1)
        cells = jnp.sum(jnp.where(lane % EDGE == row, cells, 0.0), 0, keepdims=True)
        lane = lane[:1]
        gain = jnp.zeros((1, lanes), jnp.float32)
        for i in range(levels):
            gain = jnp.where(lane // modes == i, rates_ref[0, i], gain)
        gain = jnp.where((px == 0) & (py == 0) & (lane % modes >= 2 * windows * EDGE), gain, 0.0)
        upright = jnp.concatenate([rows[:modes, i * ny : (i + 1) * ny] for i in range(levels)], 0)
        upright = jnp.concatenate(halves(upright), 1)
        sides = dot(edge_ref[py], upright, ((1,), (1,)))[: 2 * windows]
        patch = jnp.concatenate([state_ref[0, level] for level in range(levels)], 0)
        patch = jnp.concatenate(halves(patch), 1)
        columns = dot(pick_ref[...], patch, ((1,), (1,)))[:EDGE]
        if halved:
            ends = jnp.where(px < plan.px // 2, ends[:windows], ends[windows : 2 * windows])
            out_ref[modes:low] = jnp.concatenate([sides, cells + gain, ends[:1]], 0)
            out_ref[low:] = jnp.concatenate([ends[1:], columns[: 2 * windows]], 0)
            along_ref[:low] = out_ref[:low]
            along_ref[low:] = jnp.concatenate([ends[1:], facing_rows(plan, state_ref, px % 2 == 0)], 0)
        else:
            blank = jnp.zeros((2, lanes), jnp.float32)
            out_ref[modes:low] = jnp.concatenate([sides, cells + gain, blank[:1]], 0)
            out_ref[low:] = jnp.concatenate([ends[: 2 * windows], blank], 0)
            along_ref[...] = columns

    return call(
        kernel,
        (shape_of(plan.rows, lanes), shape_of(plan.rows if halved else EDGE, lanes)),
        state, left, jnp.asarray(np.stack(right)), jnp.asarray(np.stack(edge)),
        jnp.asarray(bf16(pick)), rates,
        first=True,
    )


def facing_rows(plan, state_ref, bottom):
    rows = []
    for group in range(plan.half):
        pair = [state_ref[0, 2 * group + i] for i in range(2)]
        top = jnp.concatenate([p[: plan.windows] for p in pair], 1)
        end = jnp.concatenate([p[plan.nx - plan.windows :] for p in pair], 1)
        rows.append(jnp.where(bottom, end, top))
    return jnp.concatenate(rows, 0)


def facing_corners(plan, columns, bottom):
    lane = lax.broadcasted_iota(jnp.int32, columns.shape, 1)
    moved = pltpu.roll(columns, plan.lanes - (plan.nx - plan.windows), 1)
    near = jnp.where(lane % plan.nx < plan.windows, jnp.where(bottom, moved, columns), 0.0)
    first = columns.shape[0] - 2 * plan.windows
    packed = near[first : first + 1]
    for i in range(1, 2 * plan.windows):
        packed = packed + pltpu.roll(near, EDGE * i, 1)[first + i : first + i + 1]
    return packed


def join_first(plan, own, from_y, from_x, from_both, state):
    low, modes, windows, lanes = plan.low, plan.modes, plan.windows, plan.lanes

    def kernel(own_ref, y_ref, x_ref, both_ref, state_ref, out_ref, halo_ref):
        px = lax.axis_index("px")
        odd, lower = px % 2 == 1, px < plan.px // 2
        out_ref[:modes] = (own_ref[:modes] + y_ref[:modes]) + (x_ref[:modes] + both_ref[:modes])
        middle = (own_ref[modes:low] + y_ref[modes:low]) + (x_ref[modes:low] + both_ref[modes:low])
        corners = facing_corners(plan, y_ref[low:], odd)
        corners = jnp.where(lower, pltpu.roll(corners, windows, 1), corners)
        row = lax.broadcasted_iota(jnp.int32, (EDGE, lanes), 0)
        out_ref[modes:low] = middle + jnp.where(row == 2 * windows, corners, 0.0)
        ends = (own_ref[low:] + y_ref[low:]) + (x_ref[low:] + both_ref[low:])
        out_ref[low:] = jnp.concatenate([ends[: windows - 1], facing_rows(plan, state_ref, odd)], 0)
        corners = facing_corners(plan, both_ref[low:], odd)
        lines = x_ref[low:][windows - 1 :]
        halo_ref[...] = jnp.concatenate([lines, corners, jnp.zeros((1, lanes), jnp.float32)], 0)

    shapes = shape_of(plan.rows, lanes), shape_of(EDGE, lanes)
    return call(kernel, shapes, own, from_y, from_x, from_both, state)


def both_facing(plan, state, columns):
    def kernel(state_ref, columns_ref, top_ref, bottom_ref):
        columns = columns_ref[...]
        columns = jnp.concatenate([jnp.zeros((2, plan.lanes), jnp.float32), columns[: 2 * plan.windows]], 0)
        for ref, bottom in ((top_ref, False), (bottom_ref, True)):
            rows = [facing_rows(plan, state_ref, bottom), facing_corners(plan, columns, bottom)]
            ref[...] = jnp.concatenate(rows + [jnp.zeros((1, plan.lanes), jnp.float32)], 0)

    return call(kernel, (shape_of(EDGE, plan.lanes),) * 2, state, columns)


def join_last(plan, own, other):
    low, modes, windows, lanes = plan.low, plan.modes, plan.windows, plan.lanes

    def kernel(own_ref, other_ref, out_ref):
        lower = lax.axis_index("px") < plan.px // 2
        out_ref[:modes] = own_ref[:modes] + other_ref[:modes]
        row = lax.broadcasted_iota(jnp.int32, (EDGE, lanes), 0)
        lane = lax.broadcasted_iota(jnp.int32, (EDGE, lanes), 1)
        one, two = own_ref[modes:low], other_ref[modes:low]
        early, late = jnp.where(lower, one, two), jnp.where(lower, two, one)
        kept = (row < 2 * windows) | (lane % modes >= 2 * windows * EDGE)
        middle = jnp.where(kept | (lane % EDGE < windows), early, 0.0)
        middle = middle + jnp.where(kept | (lane % EDGE >= windows), late, 0.0)
        out_ref[modes:low] = jnp.where(row <= 2 * windows, middle, 0.0)
        ends = []
        for block, rest in ((early, jnp.where(lower, own_ref[low:], other_ref[low:])),
                            (late, jnp.where(lower, other_ref[low:], own_ref[low:]))):
            ends += [block[EDGE - 1 :], rest[: windows - 1]]
        out_ref[low:] = jnp.concatenate(ends + [jnp.zeros((EDGE - 2 * windows, lanes), jnp.float32)], 0)

    return call(kernel, shape_of(plan.rows, lanes), own, other)


def step_patch(plan, state, columns, first, second):
    nx, ny, windows, low, levels = plan.nx, plan.ny, plan.windows, plan.low, plan.levels
    place = np.zeros((4 * EDGE, ny))
    for i in range(windows):
        for part in range(3):
            place[part * EDGE + i, i] = 1
            place[part * EDGE + windows + i, ny - windows + i] = 1
    rows, lanes = nx + 2 * EDGE, 2 * ny

    def kernel(state_ref, columns_ref, first_ref, second_ref, place_ref, out_ref):
        px, py = lax.axis_index("px"), lax.axis_index("py")
        row = lax.broadcasted_iota(jnp.int32, (rows, lanes), 0) - EDGE + px * nx
        lane = lax.broadcasted_iota(jnp.int32, (rows, lanes), 1)
        lane = jnp.where(lane >= ny + ny // 2, lane - lanes, lane) + py * ny
        inside = (row >= 0) & (row < nx * plan.px) & (lane >= 0) & (lane < ny * plan.py)
        where = place_ref[...]

        def spread(block):
            high = block.astype(jnp.bfloat16).astype(jnp.float32)
            rest = block - high
            middle = rest.astype(jnp.bfloat16).astype(jnp.float32)
            parts = [high, middle, rest - middle, jnp.zeros_like(high)]
            return dot(jnp.concatenate(parts, 0).astype(jnp.bfloat16), where, ((0,), (0,)))

        small_row = lax.broadcasted_iota(jnp.int32, (EDGE, plan.lanes), 0)
        small_lane = lax.broadcasted_iota(jnp.int32, (EDGE, plan.lanes), 1)
        mine = small_lane % nx // EDGE == small_row

        def corners(block):
            line = jnp.broadcast_to(block[2 * windows : 2 * windows + 1], (EDGE, plan.lanes))
            cells = spread(jnp.where(mine, line, 0.0))
            return [
                sum(cells[level * nx + EDGE * i : level * nx + EDGE * (i + 1)] for i in range(2 * windows))
                for level in range(levels)
            ]

        even = px % 2 == 0
        one, two, columns = first_ref[...], second_ref[-EDGE:], columns_ref[-EDGE:]
        if second_ref.shape[0] > EDGE:
            mixed = second_ref[low - 2 : low - 1]
            mixed = jnp.where(px < plan.px // 2, mixed, pltpu.roll(mixed, plan.lanes - windows, 1))
            two = jnp.concatenate([two[windows - 1 :], mixed, mixed], 0)
            columns = jnp.concatenate([columns[windows - 1 :], columns[: windows - 1]], 0)
        above, below = jnp.where(even, two, one), jnp.where(even, one, two)
        beside = spread(columns)
        beside_above, beside_below = corners(above), corners(below)
        blank = jnp.zeros((EDGE - windows, lanes), jnp.float32)
        for level in range(levels):
            pair, part = level // 2, level % 2

            def line(block):
                return block[pair * windows : (pair + 1) * windows, part * ny : (part + 1) * ny]

            up = jnp.concatenate([line(above), beside_above[level][:windows]], 1)
            down = jnp.concatenate([line(below), beside_below[level][:windows]], 1)
            middle = jnp.concatenate([state_ref[0, level], beside[level * nx : (level + 1) * nx]], 1)
            field = jnp.concatenate([blank, up, middle, down, blank], 0)
            field = jnp.where(inside, field, 0.0)
            for _ in range(windows):
                around = (
                    pltpu.roll(field, 1, 0)
                    + pltpu.roll(field, rows - 1, 0)
                    + pltpu.roll(field, 1, 1)
                    + pltpu.roll(field, lanes - 1, 1)
                )
                field = jnp.where(inside, field + RATE * (around - 4.0 * field), 0.0)
            out_ref[level] = field[EDGE : EDGE + nx, :ny]

    return call(
        kernel, shape_of(levels, nx, ny), state, columns, first, second, jnp.asarray(bf16(place))
    )


def prepare(plan, drive, nest_offsets):
    modes, lanes, levels, windows = plan.modes, plan.lanes, plan.levels, plan.windows
    nx, ny, x, y = plan.nx, plan.ny, plan.x, plan.y
    steps = plan.nest - 1
    maps_x = f32(np.stack([np.tile(x[name], (1, 2)) for name in ("cos_map", "sin_map")]))
    maps_y = f32(np.stack([kron(2, y[name].T) for name in ("cos_map", "sin_map")]))
    rows_x = np.stack([np.tile(p, (1, 2)).reshape(plan.px, nx, 2 * modes) for p in x["powers"][:windows]], 1)
    rows_y = np.stack(
        [p.reshape(plan.py, ny, modes).transpose(0, 2, 1) for p in y["powers"][:windows]], 1
    )

    def kernel(
        drive_ref, maps_x_ref, maps_y_ref, rows_x_ref, rows_y_ref, offsets_ref,
        drive_out, row_out, col_out, spread_x_out, spread_y_out,
    ):
        nest, px, py = lax.axis_index("nest"), lax.axis_index("px"), lax.axis_index("py")
        for w in range(windows):
            drive_out[w] = jnp.concatenate([drive_ref[w, level] for level in range(levels)], 1)
        lane = lax.broadcasted_iota(jnp.int32, (modes, 2 * modes), 1)

        def as_left(twice):
            rounded = twice.astype(jnp.bfloat16).astype(jnp.float32)
            pair = jnp.where(lane >= modes, twice - rounded, rounded)
            return jnp.concatenate([pair, rounded], 1)[:, : 3 * modes].astype(jnp.bfloat16)

        def angle(mode, offset, cells):
            turn = (mode * offset).astype(jnp.float32)
            turn = turn - jnp.floor(turn / (2.0 * cells)) * (2.0 * cells)
            return turn * (math.pi / cells)

        mode = lax.broadcasted_iota(jnp.int32, (EDGE, 2 * modes), 1) % modes
        row = lax.broadcasted_iota(jnp.int32, (EDGE, 2 * modes), 0)
        upright = lax.broadcasted_iota(jnp.int32, (2 * modes, 2 * modes), 0) % modes
        place = lax.broadcasted_iota(jnp.int32, (2 * modes, 2 * modes), 1)
        along, down = jnp.zeros_like(mode), jnp.zeros_like(upright)
        for slot in range(steps):
            domain = jnp.maximum(nest - slot, 0)
            along = jnp.where(row == slot, offsets_ref[0, domain], along)
            down = jnp.where(place == slot, offsets_ref[1, domain], down)
        along = angle(mode, along, nx * plan.px)
        down = angle(upright, down, ny * plan.py)
        cos_x, sin_x = jnp.cos(along), jnp.sin(along)
        cos_y, sin_y = jnp.cos(down), jnp.sin(down)
        for slot in range(steps):
            at = slice(slot, slot + 1)
            row_out[slot] = as_left(maps_x_ref[0] * cos_x[at] - maps_x_ref[1] * sin_x[at])
            col_map = maps_y_ref[0] * cos_y[:, at] - maps_y_ref[1] * sin_y[:, at]
            high, small = halves(col_map)
            col_out[slot] = jnp.concatenate([high, small], 1)
        for w in range(windows):
            p = windows - 1 - w
            for j in range(p + 1):
                combined = sum(multinomial(p, i, j) * rows_x_ref[px, i] for i in range(p - j + 1))
                at = (sum(range(p + 1)) + j) * nx
                spread_x_out[at : at + nx] = as_left(combined)
        for j in range(windows):
            table = rows_y_ref[py, j]
            blank = jnp.zeros_like(table)
            table = jnp.concatenate(
                [jnp.concatenate([table, blank], 1), jnp.concatenate([blank, table], 1)], 0
            )
            high, small = halves(table)
            spread_y_out[j] = jnp.concatenate([high, small], 0)

    shapes = (
        shape_of(windows, modes, lanes),
        shape_of(steps, modes, 3 * modes, kind=jnp.bfloat16),
        shape_of(steps, 2 * modes, 4 * modes, kind=jnp.bfloat16),
        shape_of(sum(range(windows + 1)) * nx, 3 * modes, kind=jnp.bfloat16),
        shape_of(windows, 4 * modes, 2 * ny, kind=jnp.bfloat16),
    )
    return call(kernel, shapes, drive, maps_x, maps_y, f32(rows_x), f32(rows_y), nest_offsets.T, first=True)


def own_tables(plan):
    x, y, modes, windows = plan.x, plan.y, plan.modes, plan.windows
    inward = np.concatenate([np.tile(y["spill"][j].T, (1, 2)) for j in range(1, windows + 1)], 1)
    high, small = parts_of(inward)
    inward = jnp.asarray(np.concatenate([high, small, high, np.zeros_like(high)], 0))
    corner = np.concatenate(
        [kron(2, np.repeat(y["spill"][j].T, EDGE, 0)) for j in range(1, windows + 1)], 1
    )
    high, small = parts_of(corner)
    corner = jnp.asarray(np.concatenate([high, small], 0))
    across = np.zeros((windows * modes, windows * EDGE))
    for n in range(1, windows + 1):
        for j in range(n):
            across[(n - 1) * modes : n * modes, j * EDGE : (j + 1) * EDGE] = sum(
                multinomial(n, i, j) * x["spill"][i] for i in range(1, n - j + 1)
            )
    high, small = parts_of(across)
    across = jnp.asarray(np.pad(np.concatenate([high, small, high], 1), ((0, 0), (0, 3 * EDGE))))
    scale_x = f32(np.broadcast_to(1.0 + x["factor"][:, None], (modes, plan.lanes)))
    scale_y = f32(np.broadcast_to(np.tile(y["factor"], plan.levels), (EDGE, plan.lanes)))
    return inward, corner, across, scale_x, scale_y


def own_modes_of(plan, inward_ref, corner_ref, across_ref, scale_x_ref, scale_y_ref):
    modes, low, lanes = plan.modes, plan.low, plan.lanes
    windows, half, ny = plan.windows, plan.half, plan.ny
    scale_x, scale_y = scale_x_ref[...], scale_y_ref[:1]
    row = lax.broadcasted_iota(jnp.int32, (EDGE, lanes), 0)
    lane = lax.broadcasted_iota(jnp.int32, (EDGE, lanes), 1)
    mine = lane % EDGE == row
    left_lane = lax.broadcasted_iota(jnp.int32, (modes, ny), 1) < modes

    def own_modes(message):
        rows, middle, ends = message[:modes], message[modes:low], message[low:]
        sides = dot(short_stacked(middle, 4 * EDGE), inward_ref[...], ((0,), (0,)))
        cells = jnp.where(mine, jnp.broadcast_to(middle[EDGE - 2 : EDGE - 1], (EDGE, lanes)), 0.0)
        cells = jnp.concatenate([cells[:, i * ny : (i + 1) * ny] for i in range(half)], 0)
        cells = by_parts(cells, corner_ref[:ny], corner_ref[ny:])
        turned, ends = [rows], [ends]
        for j in range(windows):
            at = slice(j * ny, (j + 1) * ny)
            side = [
                jnp.where(
                    left_lane,
                    sides[2 * i * modes : (2 * i + 1) * modes, at],
                    sides[(2 * i + 1) * modes : (2 * i + 2) * modes, at],
                )
                for i in range(half)
            ]
            cell = [cells[i * EDGE : (i + 1) * EDGE, at] for i in range(half)]
            power = scale_y if j == 0 else power * scale_y
            turned.append(rows * power + jnp.concatenate(side, 1))
            ends.append(ends[0] * power + jnp.concatenate(cell, 1))
        over = dot(across_ref[...], short_stacked(jnp.concatenate(ends[:windows], 0), 12 * EDGE))
        result = []
        for n in range(windows):
            turned = [a * scale_x + b for a, b in zip(turned[:-1], turned[1:])]
            result.append(turned[0] + over[n * modes : (n + 1) * modes])
        return result

    return own_modes


def own_early(plan, tables, messages):
    def kernel(*refs):
        count = len(messages)
        own_modes = own_modes_of(plan, *refs[count : count + len(tables)])
        for i in range(count):
            for w, value in enumerate(own_modes(refs[i][...])):
                refs[count + len(tables)][i, w] = value

    return call(kernel, shape_of(len(messages), plan.windows, plan.modes, plan.lanes), *messages, *tables)


def nudge(plan, stepped, gathered, early, tables, crossed, prepared):
    modes, low, lanes, levels = plan.modes, plan.low, plan.lanes, plan.levels
    windows, half, nx, ny = plan.windows, plan.half, plan.nx, plan.ny
    x, y = plan.x, plan.y
    pairs, unpairs = plan.pairs, plan.unpairs
    again = []
    for p in range(1, windows):
        again.append(sum(multinomial(p, i, 0) * x["within"][i] for i in range(p + 1)))
    again = left_table(np.concatenate(again, 0))
    sideways = jnp.stack([right_table(kron(2, y["within"][j])) for j in range(1, windows)])
    drive, row_maps, col_maps, spread_x, spread_y = prepared

    def kernel(
        stepped_ref, drive_ref, row_ref, col_ref, spread_x_ref, spread_y_ref, again_ref, sideways_ref,
        early_ref, *refs,
    ):
        refs, (state_ref, modes_ref) = refs[:-2], refs[-2:]
        root = plan.nest - 1
        nest = lax.axis_index("nest")
        refs, table_refs = refs[: plan.nest], refs[plan.nest :]
        lane = lax.broadcasted_iota(jnp.int32, (1, lanes), 1)
        gains = []
        for ref in refs:
            gain = jnp.where(lane % modes >= modes - 2 * EDGE, ref[low - 2 : low - 1], 0.0)
            gain = gain + pltpu.roll(gain, lanes - 2 * EDGE, 1)
            gains.append(gain + pltpu.roll(gain, lanes - 4 * EDGE, 1))
        owns = [[early_ref[i, w] for w in range(windows)] for i in range(root)]
        owns.append(own_modes_of(plan, *table_refs)(refs[root][...]))
        if crossed:
            odd = nest % 2 == 1
            gains = [gains[0], jnp.where(odd, gains[2], gains[3]), gains[1], gains[3]]
            mixed = [jnp.where(odd, a, b) for a, b in zip(owns[2], owns[3])]
            owns = [owns[0], mixed, owns[1], owns[3]]
        coeffs, changes, later = {}, {}, {}
        for front in range(root + windows):
            cells = [(root - front + w, w) for w in range(windows) if 0 <= root - front + w <= root]
            inner, lefts, rights = {}, {}, {}
            for slot, w in cells:
                if slot < root:
                    inner[slot, w] = times_right(pairs(coeffs[slot + 1, w]), col_ref[slot])
                if w > 0:
                    change = changes[slot, w - 1]
                    count = windows - w
                    left = dot(again_ref[: count * modes], stacked(change))
                    lefts[slot] = left = [left[i * modes : (i + 1) * modes] for i in range(count)]
                    rights[slot] = [unpairs(times_right(pairs(change), sideways_ref[i])) for i in range(count)]
                    later[slot, w - 1, 1] = left[0] + rights[slot][0]
            for slot, w in cells:
                target = drive_ref[w]
                if slot < root:
                    found = dot(row_ref[slot], stacked(unpairs(inner[slot, w])))
                    target = jnp.where(nest <= slot, target, found)
                before = owns[slot][w]
                for v in range(w):
                    before = before + later[slot, v, w - v]
                changes[slot, w] = gains[slot] * (target - before)
                coeffs[slot, w] = before + changes[slot, w]
            for slot, w in cells:
                if w > 0 and windows - w > 1:
                    left, right = lefts[slot], rights[slot]
                    mixed = unpairs(times_right(pairs(left[0]), sideways_ref[0]))
                    later[slot, w - 1, 2] = left[1] + (2.0 * mixed + right[1])
        changes = [changes[0, w] for w in range(windows)]
        coeffs = [coeffs[0, w] for w in range(windows)]
        for level in range(levels):
            modes_ref[0, level] = coeffs[-1][:, level * modes : (level + 1) * modes]
        spread = [0.0] * windows
        for w in range(windows):
            p = windows - 1 - w
            at = sum(range(p + 1)) * nx
            found = dot(spread_x_ref[at : at + (p + 1) * nx], stacked(changes[w]))
            for j in range(p + 1):
                spread[j] = spread[j] + found[j * nx : (j + 1) * nx]
        field = 0.0
        for j in range(windows):
            table = spread_y_ref[j]
            part = by_parts(pairs(spread[j]), table[: 2 * modes], table[2 * modes :])
            field = field + part
        for level in range(levels):
            at_row, at = level // 2 * nx, level % 2 * ny
            state_ref[0, level] = stepped_ref[level] + field[at_row : at_row + nx, at : at + ny]

    return call(
        kernel,
        (shape_of(1, levels, nx, ny), shape_of(1, levels, modes, modes)),
        stepped, drive, row_maps, col_maps, spread_x, spread_y, again, sideways, early, *gathered, *tables,
        final=True,
    )


def swap(value, axis, partner):
    size = math.prod(lax.axis_size(name) for name in (axis if isinstance(axis, tuple) else (axis,)))
    return lax.ppermute(value, axis, [(i, partner(i)) for i in range(size) if 0 <= partner(i) < size])


def body(initial_state, drive_modes, relax_rates, nest_offsets):
    plan = Plan(initial_state, drive_modes)
    halved = plan.py == 2 and plan.px == 4
    share, along = project(plan, initial_state, relax_rates, halved)
    if halved:
        share = lax.optimization_barrier(share)
        from_y = swap(share, "py", lambda i: i ^ 1)
        from_x = swap(along, "px", lambda i: i ^ 1)
        from_both = swap(share, ("py", "px"), lambda i: i ^ (plan.px + 1))
        total, halo = join_first(plan, share, from_y, from_x, from_both, initial_state)
        columns = from_y
        total, drive_modes, nest_offsets = lax.optimization_barrier((total, drive_modes, nest_offsets))
        across = swap(total, "px", lambda i: i ^ 3)
        prepared = prepare(plan, drive_modes, nest_offsets)
        across, prepared = lax.optimization_barrier((across, prepared))
        last = join_last(plan, total, across)
    else:
        from_right = jnp.arange(EDGE)[:, None] < plan.windows
        right = swap(along, "py", lambda i: i - 1)
        left = swap(along, "py", lambda i: i + 1)
        columns = jnp.where(from_right, right, left)
        top, bottom = both_facing(plan, initial_state, columns)
        above = swap(bottom, "px", lambda i: i + 1)
        below = swap(top, "px", lambda i: i - 1)
        even = lax.axis_index("px") % 2 == 0
        halo, across = jnp.where(even, below, above), jnp.where(even, above, below)
        last = lax.psum(share, ("py", "px"))
        prepared = prepare(plan, drive_modes, nest_offsets)
    crossed = plan.nest == 4
    if crossed:
        core = swap(last, "nest", lambda i: i ^ 1)
        chip = swap(last, "nest", lambda i: i ^ 2)
        stepped = step_patch(plan, initial_state, columns, halo, across)
        chip, stepped = lax.optimization_barrier((chip, stepped))
        gathered = [last, chip, core, swap(chip, "nest", lambda i: i ^ 1)]
    else:
        gathered = [last] + [swap(last, "nest", lambda i, s=s: i + s) for s in range(1, plan.nest)]
        stepped = step_patch(plan, initial_state, columns, halo, across)
    tables = own_tables(plan)
    early = own_early(plan, tables, gathered[:-1])
    return nudge(plan, stepped, gathered, early, tables, crossed, prepared)


def solution(mesh):
    return jax.shard_map(
        body,
        mesh=mesh,
        in_specs=(P("nest", None, "px", "py"), P(), P("nest", None), P()),
        out_specs=(P("nest", None, "px", "py"), P("nest", None, None, None)),
        check_vma=False,
    )
```

```python
import functools
import math

import jax
import jax.numpy as jnp
import numpy as np
from jax import lax
from jax.experimental import pallas as pl
from jax.experimental.pallas import tpu as pltpu
from jax.sharding import PartitionSpec as P

RATIO = 3
RATE = 0.2
EDGE = 8
INTERPRET = False


def multinomial(n, i, j):
    return math.factorial(n) // (math.factorial(i) * math.factorial(j) * math.factorial(n - i - j))


@functools.lru_cache(maxsize=None)
def tables(cells, modes, order):
    cell = np.arange(cells)
    mode = np.arange(modes)
    weight = np.sqrt(np.where(mode == 0, 1.0, 2.0) / cells)
    product = mode[None] * (2 * cell[:, None] + 1)
    coarse = np.pi * (product % (4 * cells)) / (2 * cells)
    fine = np.pi * (product % (4 * RATIO * cells)) / (2 * RATIO * cells)
    base = weight * np.cos(coarse)
    second = RATE * (np.eye(cells, k=1) + np.eye(cells, k=-1) - 2 * np.eye(cells))
    powers = [base]
    for _ in range(order):
        powers.append(second @ powers[-1])
    factor = RATE * (2 * np.cos(np.pi * mode / cells) - 2)
    places = list(range(order)) + list(range(cells - order, cells))
    edges = np.zeros((cells, EDGE))
    edges[places, range(2 * order)] = 1
    spill = [(powers[i] - base * factor**i).T @ edges for i in range(order + 1)]
    return {
        "base": base,
        "edges": edges,
        "powers": powers,
        "factor": factor,
        "spill": spill,
        "within": [base.T @ power for power in powers],
        "cos_map": base.T @ (weight * np.cos(fine)),
        "sin_map": base.T @ (weight * np.sin(fine)),
    }


def kron(count, block):
    return np.kron(np.eye(count), block)


def f32(value):
    return jnp.asarray(np.asarray(value, np.float32))


def bf16(value):
    return np.asarray(value, jnp.bfloat16)


def parts_of(value):
    high = bf16(value)
    return high, bf16(value - high.astype(np.float64))


def left_table(value):
    high, low = parts_of(value)
    return jnp.asarray(np.concatenate([high, low, high], -1))


def right_table(value):
    return jnp.asarray(np.concatenate(parts_of(value), -1))


def halves(value):
    high = value.astype(jnp.bfloat16)
    return high, (value - high.astype(jnp.float32)).astype(jnp.bfloat16)


def dot(a, b, dims=((1,), (0,))):
    return lax.dot_general(a, b, (dims, ((), ())), preferred_element_type=jnp.float32)


def stacked(value):
    high, low = halves(value)
    return jnp.concatenate([high, high, low], 0)


def short_stacked(value, rows):
    high = value.astype(jnp.bfloat16).astype(jnp.float32)
    blank = jnp.zeros((rows - 3 * value.shape[0], value.shape[1]), jnp.float32)
    return jnp.concatenate([high, high, value - high, blank], 0).astype(jnp.bfloat16)


def times_right(value, table):
    width = table.shape[1] // 2
    lower = jnp.concatenate([table[:, :width], jnp.zeros_like(table[:, width:])], 1)
    out = dot(jnp.concatenate(halves(value), 1), jnp.concatenate([table, lower], 0))
    return out[:, :width] + out[:, width:]


def by_parts(value, table, rest):
    high, low = halves(value)
    out = dot(jnp.concatenate([high, low], 0), table)
    return out[: value.shape[0]] + out[value.shape[0] :] + dot(high, rest)


def in_vmem(value):
    return value if INTERPRET else pltpu.with_memory_space_constraint(value, pltpu.VMEM)


def call(kernel, shapes, *args, first=False, final=False):
    scalars = [a.ndim == 2 and a.size <= 16 for a in args]
    specs = [pl.BlockSpec(memory_space=pltpu.SMEM if s else pltpu.VMEM) for s in scalars]
    if not final and not INTERPRET:
        shapes = jax.tree.map(lambda s: pltpu.VMEM(s.shape, s.dtype), shapes)
    return pl.pallas_call(
        kernel,
        in_specs=specs,
        out_specs=jax.tree.map(lambda _: pl.BlockSpec(memory_space=pltpu.VMEM), shapes),
        out_shape=shapes,
        interpret=INTERPRET,
    )(*[a if s or first else in_vmem(a) for a, s in zip(args, scalars)])


def shape_of(*dims, kind=jnp.float32):
    return jax.ShapeDtypeStruct(dims, kind)


class Plan:
    def __init__(self, initial_state, drive_modes):
        _, self.levels, self.nx, self.ny = initial_state.shape
        self.windows, _, self.modes, _ = drive_modes.shape
        self.px = lax.axis_size("px")
        self.py = lax.axis_size("py")
        self.nest = lax.axis_size("nest")
        self.lanes = self.levels * self.modes
        self.half = self.levels // 2
        self.low = self.modes + EDGE
        self.rows = self.low + EDGE
        self.x = tables(self.nx * self.px, self.modes, self.windows)
        self.y = tables(self.ny * self.py, self.modes, self.windows)
        assert self.levels % 4 == 0 and self.modes * 2 == self.ny and self.nx == self.modes
        assert self.windows == 3 and self.half == 2 and EDGE * EDGE == self.modes

    def pairs(self, value):
        width = 2 * self.modes
        return jnp.concatenate([value[:, i * width : (i + 1) * width] for i in range(self.half)], 0)

    def unpairs(self, value):
        rows = value.shape[0] // self.half
        return jnp.concatenate([value[i * rows : (i + 1) * rows] for i in range(self.half)], 1)


def project(plan, state, rates, halved):
    low, half, lanes, levels = plan.low, plan.half, plan.lanes, plan.levels
    modes, nx, ny, windows = plan.modes, plan.nx, plan.ny, plan.windows
    bases = np.concatenate([plan.x["base"], plan.x["edges"], np.zeros((nx * plan.px, EDGE))], 1)
    left = right_table(bases.T.reshape(low + EDGE, plan.px, nx).transpose(1, 0, 2))
    base_y = plan.y["base"].reshape(plan.py, ny, modes)
    edge_y = plan.y["edges"].reshape(plan.py, ny, EDGE)
    right, edge = [], []
    for at in range(plan.py):
        high, small = parts_of(base_y[at])
        corner = bf16(np.repeat(edge_y[at], EDGE, 1))
        right.append(np.concatenate([high, small, corner, np.zeros_like(corner)], 1))
        edge.append(bf16(np.pad(np.tile(edge_y[at].T, (1, 2)), ((0, EDGE), (0, 0)))))
    pick = np.zeros((2 * EDGE, 2 * ny))
    for i in range(windows):
        pick[i, [i, ny + i]] = 1
        pick[windows + i, [ny - windows + i, 2 * ny - windows + i]] = 1

    def kernel(state_ref, left_ref, right_ref, edge_ref, pick_ref, rates_ref, out_ref, along_ref):
        px, py = lax.axis_index("px"), lax.axis_index("py")
        field = jnp.concatenate([state_ref[0, level] for level in range(levels)], 1)
        high, small = halves(field)
        table = left_ref[px]
        rows = dot(table, jnp.concatenate([high, high], 0)) + dot(table[:, :nx], small)
        found = jnp.concatenate([rows[:low, i * ny : (i + 1) * ny] for i in range(levels)], 0)
        high, small = halves(found)
        table = right_ref[py]
        found = dot(high, table) + dot(small, table)
        both = found[:, :ny] + pltpu.roll(found[:, :ny], modes, 1)
        left_lane = lax.broadcasted_iota(jnp.int32, (low, ny), 1) < modes
        both = [both[i * low : (i + 1) * low] for i in range(levels)]
        both = [jnp.where(left_lane, both[2 * i], both[2 * i + 1]) for i in range(half)]
        both = jnp.concatenate(both, 1)
        out_ref[:modes] = both[:modes]
        ends = both[modes:]
        cells = [found[i * low + modes : (i + 1) * low, ny:] for i in range(levels)]
        cells = [cells[2 * i] + pltpu.roll(cells[2 * i + 1], modes, 1) for i in range(half)]
        cells = jnp.concatenate(cells, 1)
        row = lax.broadcasted_iota(jnp.int32, (EDGE, lanes), 0)
        lane = lax.broadcasted_iota(jnp.int32, (EDGE, lanes), 1)
        cells = jnp.sum(jnp.where(lane % EDGE == row, cells, 0.0), 0, keepdims=True)
        lane = lane[:1]
        gain = jnp.zeros((1, lanes), jnp.float32)
        for i in range(levels):
            gain = jnp.where(lane // modes == i, rates_ref[0, i], gain)
        gain = jnp.where((px == 0) & (py == 0) & (lane % modes >= 2 * windows * EDGE), gain, 0.0)
        upright = jnp.concatenate([rows[:modes, i * ny : (i + 1) * ny] for i in range(levels)], 0)
        upright = jnp.concatenate(halves(upright), 1)
        sides = dot(edge_ref[py], upright, ((1,), (1,)))[: 2 * windows]
        patch = jnp.concatenate([state_ref[0, level] for level in range(levels)], 0)
        patch = jnp.concatenate(halves(patch), 1)
        columns = dot(pick_ref[...], patch, ((1,), (1,)))[:EDGE]
        if halved:
            ends = jnp.where(px < plan.px // 2, ends[:windows], ends[windows : 2 * windows])
            out_ref[modes:low] = jnp.concatenate([sides, cells + gain, ends[:1]], 0)
            out_ref[low:] = jnp.concatenate([ends[1:], columns[: 2 * windows]], 0)
            along_ref[:low] = out_ref[:low]
            along_ref[low:] = jnp.concatenate([ends[1:], facing_rows(plan, state_ref, px % 2 == 0)], 0)
        else:
            blank = jnp.zeros((2, lanes), jnp.float32)
            out_ref[modes:low] = jnp.concatenate([sides, cells + gain, blank[:1]], 0)
            out_ref[low:] = jnp.concatenate([ends[: 2 * windows], blank], 0)
            along_ref[...] = columns

    return call(
        kernel,
        (shape_of(plan.rows, lanes), shape_of(plan.rows if halved else EDGE, lanes)),
        state, left, jnp.asarray(np.stack(right)), jnp.asarray(np.stack(edge)),
        jnp.asarray(bf16(pick)), rates,
        first=True,
    )


def facing_rows(plan, state_ref, bottom):
    rows = []
    for group in range(plan.half):
        pair = [state_ref[0, 2 * group + i] for i in range(2)]
        top = jnp.concatenate([p[: plan.windows] for p in pair], 1)
        end = jnp.concatenate([p[plan.nx - plan.windows :] for p in pair], 1)
        rows.append(jnp.where(bottom, end, top))
    return jnp.concatenate(rows, 0)


def facing_corners(plan, columns, bottom):
    lane = lax.broadcasted_iota(jnp.int32, columns.shape, 1)
    moved = pltpu.roll(columns, plan.lanes - (plan.nx - plan.windows), 1)
    near = jnp.where(lane % plan.nx < plan.windows, jnp.where(bottom, moved, columns), 0.0)
    first = columns.shape[0] - 2 * plan.windows
    packed = near[first : first + 1]
    for i in range(1, 2 * plan.windows):
        packed = packed + pltpu.roll(near, EDGE * i, 1)[first + i : first + i + 1]
    return packed


def join_first(plan, own, from_y, from_x, from_both, state):
    low, modes, windows, lanes = plan.low, plan.modes, plan.windows, plan.lanes

    def kernel(own_ref, y_ref, x_ref, both_ref, state_ref, out_ref, halo_ref):
        px = lax.axis_index("px")
        odd, lower = px % 2 == 1, px < plan.px // 2
        out_ref[:modes] = (own_ref[:modes] + y_ref[:modes]) + (x_ref[:modes] + both_ref[:modes])
        middle = (own_ref[modes:low] + y_ref[modes:low]) + (x_ref[modes:low] + both_ref[modes:low])
        corners = facing_corners(plan, y_ref[low:], odd)
        corners = jnp.where(lower, pltpu.roll(corners, windows, 1), corners)
        row = lax.broadcasted_iota(jnp.int32, (EDGE, lanes), 0)
        out_ref[modes:low] = middle + jnp.where(row == 2 * windows, corners, 0.0)
        ends = (own_ref[low:] + y_ref[low:]) + (x_ref[low:] + both_ref[low:])
        out_ref[low:] = jnp.concatenate([ends[: windows - 1], facing_rows(plan, state_ref, odd)], 0)
        corners = facing_corners(plan, both_ref[low:], odd)
        lines = x_ref[low:][windows - 1 :]
        halo_ref[...] = jnp.concatenate([lines, corners, jnp.zeros((1, lanes), jnp.float32)], 0)

    shapes = shape_of(plan.rows, lanes), shape_of(EDGE, lanes)
    return call(kernel, shapes, own, from_y, from_x, from_both, state)


def both_facing(plan, state, columns):
    def kernel(state_ref, columns_ref, top_ref, bottom_ref):
        columns = columns_ref[...]
        columns = jnp.concatenate([jnp.zeros((2, plan.lanes), jnp.float32), columns[: 2 * plan.windows]], 0)
        for ref, bottom in ((top_ref, False), (bottom_ref, True)):
            rows = [facing_rows(plan, state_ref, bottom), facing_corners(plan, columns, bottom)]
            ref[...] = jnp.concatenate(rows + [jnp.zeros((1, plan.lanes), jnp.float32)], 0)

    return call(kernel, (shape_of(EDGE, plan.lanes),) * 2, state, columns)


def join_last(plan, own, other):
    low, modes, windows, lanes = plan.low, plan.modes, plan.windows, plan.lanes

    def kernel(own_ref, other_ref, out_ref):
        lower = lax.axis_index("px") < plan.px // 2
        out_ref[:modes] = own_ref[:modes] + other_ref[:modes]
        row = lax.broadcasted_iota(jnp.int32, (EDGE, lanes), 0)
        lane = lax.broadcasted_iota(jnp.int32, (EDGE, lanes), 1)
        one, two = own_ref[modes:low], other_ref[modes:low]
        early, late = jnp.where(lower, one, two), jnp.where(lower, two, one)
        kept = (row < 2 * windows) | (lane % modes >= 2 * windows * EDGE)
        middle = jnp.where(kept | (lane % EDGE < windows), early, 0.0)
        middle = middle + jnp.where(kept | (lane % EDGE >= windows), late, 0.0)
        out_ref[modes:low] = jnp.where(row <= 2 * windows, middle, 0.0)
        ends = []
        for block, rest in ((early, jnp.where(lower, own_ref[low:], other_ref[low:])),
                            (late, jnp.where(lower, other_ref[low:], own_ref[low:]))):
            ends += [block[EDGE - 1 :], rest[: windows - 1]]
        out_ref[low:] = jnp.concatenate(ends + [jnp.zeros((EDGE - 2 * windows, lanes), jnp.float32)], 0)

    return call(kernel, shape_of(plan.rows, lanes), own, other)


def step_patch(plan, state, columns, first, second):
    nx, ny, windows, low, levels = plan.nx, plan.ny, plan.windows, plan.low, plan.levels
    place = np.zeros((4 * EDGE, ny))
    for i in range(windows):
        for part in range(3):
            place[part * EDGE + i, i] = 1
            place[part * EDGE + windows + i, ny - windows + i] = 1
    rows, lanes = nx + 2 * EDGE, 2 * ny

    def kernel(state_ref, columns_ref, first_ref, second_ref, place_ref, out_ref):
        px, py = lax.axis_index("px"), lax.axis_index("py")
        row = lax.broadcasted_iota(jnp.int32, (rows, lanes), 0) - EDGE + px * nx
        lane = lax.broadcasted_iota(jnp.int32, (rows, lanes), 1)
        lane = jnp.where(lane >= ny + ny // 2, lane - lanes, lane) + py * ny
        inside = (row >= 0) & (row < nx * plan.px) & (lane >= 0) & (lane < ny * plan.py)
        where = place_ref[...]

        def spread(block):
            high = block.astype(jnp.bfloat16).astype(jnp.float32)
            rest = block - high
            middle = rest.astype(jnp.bfloat16).astype(jnp.float32)
            parts = [high, middle, rest - middle, jnp.zeros_like(high)]
            return dot(jnp.concatenate(parts, 0).astype(jnp.bfloat16), where, ((0,), (0,)))

        small_row = lax.broadcasted_iota(jnp.int32, (EDGE, plan.lanes), 0)
        small_lane = lax.broadcasted_iota(jnp.int32, (EDGE, plan.lanes), 1)
        mine = small_lane % nx // EDGE == small_row

        def corners(block):
            line = jnp.broadcast_to(block[2 * windows : 2 * windows + 1], (EDGE, plan.lanes))
            cells = spread(jnp.where(mine, line, 0.0))
            return [
                sum(cells[level * nx + EDGE * i : level * nx + EDGE * (i + 1)] for i in range(2 * windows))
                for level in range(levels)
            ]

        even = px % 2 == 0
        one, two, columns = first_ref[...], second_ref[-EDGE:], columns_ref[-EDGE:]
        if second_ref.shape[0] > EDGE:
            mixed = second_ref[low - 2 : low - 1]
            mixed = jnp.where(px < plan.px // 2, mixed, pltpu.roll(mixed, plan.lanes - windows, 1))
            two = jnp.concatenate([two[windows - 1 :], mixed, mixed], 0)
            columns = jnp.concatenate([columns[windows - 1 :], columns[: windows - 1]], 0)
        above, below = jnp.where(even, two, one), jnp.where(even, one, two)
        beside = spread(columns)
        beside_above, beside_below = corners(above), corners(below)
        blank = jnp.zeros((EDGE - windows, lanes), jnp.float32)
        for level in range(levels):
            pair, part = level // 2, level % 2

            def line(block):
                return block[pair * windows : (pair + 1) * windows, part * ny : (part + 1) * ny]

            up = jnp.concatenate([line(above), beside_above[level][:windows]], 1)
            down = jnp.concatenate([line(below), beside_below[level][:windows]], 1)
            middle = jnp.concatenate([state_ref[0, level], beside[level * nx : (level + 1) * nx]], 1)
            field = jnp.concatenate([blank, up, middle, down, blank], 0)
            field = jnp.where(inside, field, 0.0)
            for _ in range(windows):
                around = (
                    pltpu.roll(field, 1, 0)
                    + pltpu.roll(field, rows - 1, 0)
                    + pltpu.roll(field, 1, 1)
                    + pltpu.roll(field, lanes - 1, 1)
                )
                field = jnp.where(inside, field + RATE * (around - 4.0 * field), 0.0)
            out_ref[level] = field[EDGE : EDGE + nx, :ny]

    return call(
        kernel, shape_of(levels, nx, ny), state, columns, first, second, jnp.asarray(bf16(place))
    )


def prepare(plan, drive, nest_offsets):
    modes, lanes, levels, windows = plan.modes, plan.lanes, plan.levels, plan.windows
    nx, ny, x, y = plan.nx, plan.ny, plan.x, plan.y
    steps = plan.nest - 1
    maps_x = f32(np.stack([np.tile(x[name], (1, 2)) for name in ("cos_map", "sin_map")]))
    maps_y = f32(np.stack([kron(2, y[name].T) for name in ("cos_map", "sin_map")]))
    rows_x = np.stack([np.tile(p, (1, 2)).reshape(plan.px, nx, 2 * modes) for p in x["powers"][:windows]], 1)
    rows_y = np.stack(
        [p.reshape(plan.py, ny, modes).transpose(0, 2, 1) for p in y["powers"][:windows]], 1
    )

    def kernel(
        drive_ref, maps_x_ref, maps_y_ref, rows_x_ref, rows_y_ref, offsets_ref,
        drive_out, row_out, col_out, spread_x_out, spread_y_out,
    ):
        nest, px, py = lax.axis_index("nest"), lax.axis_index("px"), lax.axis_index("py")
        for w in range(windows):
            drive_out[w] = jnp.concatenate([drive_ref[w, level] for level in range(levels)], 1)
        lane = lax.broadcasted_iota(jnp.int32, (modes, 2 * modes), 1)

        def as_left(twice):
            rounded = twice.astype(jnp.bfloat16).astype(jnp.float32)
            pair = jnp.where(lane >= modes, twice - rounded, rounded)
            return jnp.concatenate([pair, rounded], 1)[:, : 3 * modes].astype(jnp.bfloat16)

        def angle(mode, offset, cells):
            turn = (mode * offset).astype(jnp.float32)
            turn = turn - jnp.floor(turn / (2.0 * cells)) * (2.0 * cells)
            return turn * (math.pi / cells)

        mode = lax.broadcasted_iota(jnp.int32, (EDGE, 2 * modes), 1) % modes
        row = lax.broadcasted_iota(jnp.int32, (EDGE, 2 * modes), 0)
        upright = lax.broadcasted_iota(jnp.int32, (2 * modes, 2 * modes), 0) % modes
        place = lax.broadcasted_iota(jnp.int32, (2 * modes, 2 * modes), 1)
        along, down = jnp.zeros_like(mode), jnp.zeros_like(upright)
        for slot in range(steps):
            domain = jnp.maximum(nest - slot, 0)
            along = jnp.where(row == slot, offsets_ref[0, domain], along)
            down = jnp.where(place == slot, offsets_ref[1, domain], down)
        along = angle(mode, along, nx * plan.px)
        down = angle(upright, down, ny * plan.py)
        cos_x, sin_x = jnp.cos(along), jnp.sin(along)
        cos_y, sin_y = jnp.cos(down), jnp.sin(down)
        for slot in range(steps):
            at = slice(slot, slot + 1)
            row_out[slot] = as_left(maps_x_ref[0] * cos_x[at] - maps_x_ref[1] * sin_x[at])
            col_map = maps_y_ref[0] * cos_y[:, at] - maps_y_ref[1] * sin_y[:, at]
            high, small = halves(col_map)
            col_out[slot] = jnp.concatenate([high, small], 1)
        for w in range(windows):
            p = windows - 1 - w
            for j in range(p + 1):
                combined = sum(multinomial(p, i, j) * rows_x_ref[px, i] for i in range(p - j + 1))
                at = (sum(range(p + 1)) + j) * nx
                spread_x_out[at : at + nx] = as_left(combined)
        for j in range(windows):
            spread_y_out[j] = jnp.concatenate(halves(rows_y_ref[py, j]), 0)

    shapes = (
        shape_of(windows, modes, lanes),
        shape_of(steps, modes, 3 * modes, kind=jnp.bfloat16),
        shape_of(steps, 2 * modes, 4 * modes, kind=jnp.bfloat16),
        shape_of(sum(range(windows + 1)) * nx, 3 * modes, kind=jnp.bfloat16),
        shape_of(windows, 2 * modes, ny, kind=jnp.bfloat16),
    )
    return call(kernel, shapes, drive, maps_x, maps_y, f32(rows_x), f32(rows_y), nest_offsets.T, first=True)


def own_tables(plan):
    x, y, modes, windows = plan.x, plan.y, plan.modes, plan.windows
    inward = np.concatenate([np.tile(y["spill"][j].T, (1, 2)) for j in range(1, windows + 1)], 1)
    high, small = parts_of(inward)
    inward = jnp.asarray(np.concatenate([high, small, high, np.zeros_like(high)], 0))
    corner = np.concatenate(
        [kron(2, np.repeat(y["spill"][j].T, EDGE, 0)) for j in range(1, windows + 1)], 1
    )
    high, small = parts_of(corner)
    corner = jnp.asarray(np.concatenate([high, small], 0))
    across = np.zeros((windows * modes, windows * EDGE))
    for n in range(1, windows + 1):
        for j in range(n):
            across[(n - 1) * modes : n * modes, j * EDGE : (j + 1) * EDGE] = sum(
                multinomial(n, i, j) * x["spill"][i] for i in range(1, n - j + 1)
            )
    high, small = parts_of(across)
    across = jnp.asarray(np.pad(np.concatenate([high, small, high], 1), ((0, 0), (0, 3 * EDGE))))
    scale_x = f32(np.broadcast_to(1.0 + x["factor"][:, None], (modes, plan.lanes)))
    scale_y = f32(np.broadcast_to(np.tile(y["factor"], plan.levels), (EDGE, plan.lanes)))
    return inward, corner, across, scale_x, scale_y


def own_modes_of(plan, inward_ref, corner_ref, across_ref, scale_x_ref, scale_y_ref):
    modes, low, lanes = plan.modes, plan.low, plan.lanes
    windows, half, ny = plan.windows, plan.half, plan.ny
    scale_x, scale_y = scale_x_ref[...], scale_y_ref[:1]
    row = lax.broadcasted_iota(jnp.int32, (EDGE, lanes), 0)
    lane = lax.broadcasted_iota(jnp.int32, (EDGE, lanes), 1)
    mine = lane % EDGE == row
    left_lane = lax.broadcasted_iota(jnp.int32, (modes, ny), 1) < modes

    def own_modes(message):
        rows, middle, ends = message[:modes], message[modes:low], message[low:]
        sides = dot(short_stacked(middle, 4 * EDGE), inward_ref[...], ((0,), (0,)))
        cells = jnp.where(mine, jnp.broadcast_to(middle[EDGE - 2 : EDGE - 1], (EDGE, lanes)), 0.0)
        cells = jnp.concatenate([cells[:, i * ny : (i + 1) * ny] for i in range(half)], 0)
        cells = by_parts(cells, corner_ref[:ny], corner_ref[ny:])
        turned, ends = [rows], [ends]
        for j in range(windows):
            at = slice(j * ny, (j + 1) * ny)
            side = [
                jnp.where(
                    left_lane,
                    sides[2 * i * modes : (2 * i + 1) * modes, at],
                    sides[(2 * i + 1) * modes : (2 * i + 2) * modes, at],
                )
                for i in range(half)
            ]
            cell = [cells[i * EDGE : (i + 1) * EDGE, at] for i in range(half)]
            power = scale_y if j == 0 else power * scale_y
            turned.append(rows * power + jnp.concatenate(side, 1))
            ends.append(ends[0] * power + jnp.concatenate(cell, 1))
        over = dot(across_ref[...], short_stacked(jnp.concatenate(ends[:windows], 0), 12 * EDGE))
        result = []
        for n in range(windows):
            turned = [a * scale_x + b for a, b in zip(turned[:-1], turned[1:])]
            result.append(turned[0] + over[n * modes : (n + 1) * modes])
        return result

    return own_modes


def own_early(plan, tables, messages):
    def kernel(*refs):
        count = len(messages)
        own_modes = own_modes_of(plan, *refs[count : count + len(tables)])
        for i in range(count):
            for w, value in enumerate(own_modes(refs[i][...])):
                refs[count + len(tables)][i, w] = value

    return call(kernel, shape_of(len(messages), plan.windows, plan.modes, plan.lanes), *messages, *tables)


def nudge(plan, stepped, gathered, early, tables, crossed, prepared):
    modes, low, lanes, levels = plan.modes, plan.low, plan.lanes, plan.levels
    windows, half, nx, ny = plan.windows, plan.half, plan.nx, plan.ny
    x, y = plan.x, plan.y
    pairs, unpairs = plan.pairs, plan.unpairs
    again = []
    for p in range(1, windows):
        again.append(sum(multinomial(p, i, 0) * x["within"][i] for i in range(p + 1)))
    again = left_table(np.concatenate(again, 0))
    sideways = jnp.stack([right_table(kron(2, y["within"][j])) for j in range(1, windows)])
    drive, row_maps, col_maps, spread_x, spread_y = prepared

    def kernel(
        stepped_ref, drive_ref, row_ref, col_ref, spread_x_ref, spread_y_ref, again_ref, sideways_ref,
        early_ref, *refs,
    ):
        refs, (state_ref, modes_ref) = refs[:-2], refs[-2:]
        root = plan.nest - 1
        nest = lax.axis_index("nest")
        refs, table_refs = refs[: plan.nest], refs[plan.nest :]
        lane = lax.broadcasted_iota(jnp.int32, (1, lanes), 1)
        gains = []
        for ref in refs:
            gain = jnp.where(lane % modes >= modes - 2 * EDGE, ref[low - 2 : low - 1], 0.0)
            gain = gain + pltpu.roll(gain, lanes - 2 * EDGE, 1)
            gains.append(gain + pltpu.roll(gain, lanes - 4 * EDGE, 1))
        owns = [[early_ref[i, w] for w in range(windows)] for i in range(root)]
        owns.append(own_modes_of(plan, *table_refs)(refs[root][...]))
        if crossed:
            odd = nest % 2 == 1
            gains = [gains[0], jnp.where(odd, gains[2], gains[3]), gains[1], gains[3]]
            mixed = [jnp.where(odd, a, b) for a, b in zip(owns[2], owns[3])]
            owns = [owns[0], mixed, owns[1], owns[3]]
        coeffs, changes, later = {}, {}, {}
        for front in range(root + windows):
            cells = [(root - front + w, w) for w in range(windows) if 0 <= root - front + w <= root]
            inner, lefts, rights = {}, {}, {}
            for slot, w in cells:
                if slot < root:
                    inner[slot, w] = times_right(pairs(coeffs[slot + 1, w]), col_ref[slot])
                if w > 0:
                    change = changes[slot, w - 1]
                    count = windows - w
                    left = dot(again_ref[: count * modes], stacked(change))
                    lefts[slot] = left = [left[i * modes : (i + 1) * modes] for i in range(count)]
                    rights[slot] = [unpairs(times_right(pairs(change), sideways_ref[i])) for i in range(count)]
                    later[slot, w - 1, 1] = left[0] + rights[slot][0]
            for slot, w in cells:
                target = drive_ref[w]
                if slot < root:
                    found = dot(row_ref[slot], stacked(unpairs(inner[slot, w])))
                    target = jnp.where(nest <= slot, target, found)
                before = owns[slot][w]
                for v in range(w):
                    before = before + later[slot, v, w - v]
                changes[slot, w] = gains[slot] * (target - before)
                coeffs[slot, w] = before + changes[slot, w]
            for slot, w in cells:
                if w > 0 and windows - w > 1:
                    left, right = lefts[slot], rights[slot]
                    mixed = unpairs(times_right(pairs(left[0]), sideways_ref[0]))
                    later[slot, w - 1, 2] = left[1] + (2.0 * mixed + right[1])
        changes = [changes[0, w] for w in range(windows)]
        coeffs = [coeffs[0, w] for w in range(windows)]
        for level in range(levels):
            modes_ref[0, level] = coeffs[-1][:, level * modes : (level + 1) * modes]
        spread = [0.0] * windows
        for w in range(windows):
            p = windows - 1 - w
            at = sum(range(p + 1)) * nx
            found = dot(spread_x_ref[at : at + (p + 1) * nx], stacked(changes[w]))
            for j in range(p + 1):
                spread[j] = spread[j] + found[j * nx : (j + 1) * nx]
        field = 0.0
        for j in range(windows):
            table, blank = spread_y_ref[j], jnp.zeros((modes, ny), jnp.bfloat16)
            both = [
                jnp.concatenate([jnp.concatenate([t, blank], 1), jnp.concatenate([blank, t], 1)], 0)
                for t in (table[:modes], table[modes:])
            ]
            part = by_parts(pairs(spread[j]), *both)
            field = field + part
        for level in range(levels):
            at_row, at = level // 2 * nx, level % 2 * ny
            state_ref[0, level] = stepped_ref[level] + field[at_row : at_row + nx, at : at + ny]

    return call(
        kernel,
        (shape_of(1, levels, nx, ny), shape_of(1, levels, modes, modes)),
        stepped, drive, row_maps, col_maps, spread_x, spread_y, again, sideways, early, *gathered, *tables,
        final=True,
    )


def swap(value, axis, partner):
    size = math.prod(lax.axis_size(name) for name in (axis if isinstance(axis, tuple) else (axis,)))
    return lax.ppermute(value, axis, [(i, partner(i)) for i in range(size) if 0 <= partner(i) < size])


def body(initial_state, drive_modes, relax_rates, nest_offsets):
    plan = Plan(initial_state, drive_modes)
    halved = plan.py == 2 and plan.px == 4
    share, along = project(plan, initial_state, relax_rates, halved)
    if halved:
        share, drive_modes, nest_offsets = lax.optimization_barrier((share, drive_modes, nest_offsets))
        from_y = swap(share, "py", lambda i: i ^ 1)
        from_x = swap(along, "px", lambda i: i ^ 1)
        from_both = swap(share, ("py", "px"), lambda i: i ^ (plan.px + 1))
        prepared = prepare(plan, drive_modes, nest_offsets)
        from_both, prepared = lax.optimization_barrier((from_both, prepared))
        total, halo = join_first(plan, share, from_y, from_x, from_both, initial_state)
        columns = from_y
        across = swap(total, "px", lambda i: i ^ 3)
        last = join_last(plan, total, across)
    else:
        from_right = jnp.arange(EDGE)[:, None] < plan.windows
        right = swap(along, "py", lambda i: i - 1)
        left = swap(along, "py", lambda i: i + 1)
        columns = jnp.where(from_right, right, left)
        top, bottom = both_facing(plan, initial_state, columns)
        above = swap(bottom, "px", lambda i: i + 1)
        below = swap(top, "px", lambda i: i - 1)
        even = lax.axis_index("px") % 2 == 0
        halo, across = jnp.where(even, below, above), jnp.where(even, above, below)
        last = lax.psum(share, ("py", "px"))
        prepared = prepare(plan, drive_modes, nest_offsets)
    crossed = plan.nest == 4
    if crossed:
        core = swap(last, "nest", lambda i: i ^ 1)
        chip = swap(last, "nest", lambda i: i ^ 2)
        stepped = step_patch(plan, initial_state, columns, halo, across)
        chip, stepped = lax.optimization_barrier((chip, stepped))
        gathered = [last, chip, core, swap(last, "nest", lambda i: i ^ 3)]
    else:
        gathered = [last] + [swap(last, "nest", lambda i, s=s: i + s) for s in range(1, plan.nest)]
        stepped = step_patch(plan, initial_state, columns, halo, across)
    tables = own_tables(plan)
    early = own_early(plan, tables, gathered[:-1])
    return nudge(plan, stepped, gathered, early, tables, crossed, prepared)


def solution(mesh):
    return jax.shard_map(
        body,
        mesh=mesh,
        in_specs=(P("nest", None, "px", "py"), P(), P("nest", None), P()),
        out_specs=(P("nest", None, "px", "py"), P("nest", None, None, None)),
        check_vma=False,
    )
```

```python
import functools
import math

import jax
import jax.numpy as jnp
import numpy as np
from jax import lax
from jax.experimental import pallas as pl
from jax.experimental.pallas import tpu as pltpu
from jax.sharding import PartitionSpec as P

RATIO = 3
RATE = 0.2
EDGE = 8
INTERPRET = False


def multinomial(n, i, j):
    return math.factorial(n) // (math.factorial(i) * math.factorial(j) * math.factorial(n - i - j))


@functools.lru_cache(maxsize=None)
def tables(cells, modes, order):
    cell = np.arange(cells)
    mode = np.arange(modes)
    weight = np.sqrt(np.where(mode == 0, 1.0, 2.0) / cells)
    product = mode[None] * (2 * cell[:, None] + 1)
    coarse = np.pi * (product % (4 * cells)) / (2 * cells)
    fine = np.pi * (product % (4 * RATIO * cells)) / (2 * RATIO * cells)
    base = weight * np.cos(coarse)
    second = RATE * (np.eye(cells, k=1) + np.eye(cells, k=-1) - 2 * np.eye(cells))
    powers = [base]
    for _ in range(order):
        powers.append(second @ powers[-1])
    factor = RATE * (2 * np.cos(np.pi * mode / cells) - 2)
    places = list(range(order)) + list(range(cells - order, cells))
    edges = np.zeros((cells, EDGE))
    edges[places, range(2 * order)] = 1
    spill = [(powers[i] - base * factor**i).T @ edges for i in range(order + 1)]
    return {
        "base": base,
        "edges": edges,
        "powers": powers,
        "factor": factor,
        "spill": spill,
        "within": [base.T @ power for power in powers],
        "cos_map": base.T @ (weight * np.cos(fine)),
        "sin_map": base.T @ (weight * np.sin(fine)),
    }


def kron(count, block):
    return np.kron(np.eye(count), block)


def f32(value):
    return jnp.asarray(np.asarray(value, np.float32))


def bf16(value):
    return np.asarray(value, jnp.bfloat16)


def parts_of(value):
    high = bf16(value)
    return high, bf16(value - high.astype(np.float64))


def left_table(value):
    high, low = parts_of(value)
    return jnp.asarray(np.concatenate([high, low, high], -1))


def right_table(value):
    return jnp.asarray(np.concatenate(parts_of(value), -1))


def halves(value):
    high = value.astype(jnp.bfloat16)
    return high, (value - high.astype(jnp.float32)).astype(jnp.bfloat16)


def dot(a, b, dims=((1,), (0,))):
    return lax.dot_general(a, b, (dims, ((), ())), preferred_element_type=jnp.float32)


def stacked(value):
    high, low = halves(value)
    return jnp.concatenate([high, high, low], 0)


def short_stacked(value, rows):
    high = value.astype(jnp.bfloat16).astype(jnp.float32)
    blank = jnp.zeros((rows - 3 * value.shape[0], value.shape[1]), jnp.float32)
    return jnp.concatenate([high, high, value - high, blank], 0).astype(jnp.bfloat16)


def times_right(value, table):
    width = table.shape[1] // 2
    lower = jnp.concatenate([table[:, :width], jnp.zeros_like(table[:, width:])], 1)
    out = dot(jnp.concatenate(halves(value), 1), jnp.concatenate([table, lower], 0))
    return out[:, :width] + out[:, width:]


def by_parts(value, table, rest):
    high, low = halves(value)
    out = dot(jnp.concatenate([high, low], 0), table)
    return out[: value.shape[0]] + out[value.shape[0] :] + dot(high, rest)


def in_vmem(value):
    return value if INTERPRET else pltpu.with_memory_space_constraint(value, pltpu.VMEM)


def call(kernel, shapes, *args, first=False, final=False):
    scalars = [a.ndim == 2 and a.size <= 16 for a in args]
    specs = [pl.BlockSpec(memory_space=pltpu.SMEM if s else pltpu.VMEM) for s in scalars]
    if not final and not INTERPRET:
        shapes = jax.tree.map(lambda s: pltpu.VMEM(s.shape, s.dtype), shapes)
    return pl.pallas_call(
        kernel,
        in_specs=specs,
        out_specs=jax.tree.map(lambda _: pl.BlockSpec(memory_space=pltpu.VMEM), shapes),
        out_shape=shapes,
        interpret=INTERPRET,
    )(*[a if s or first else in_vmem(a) for a, s in zip(args, scalars)])


def shape_of(*dims, kind=jnp.float32):
    return jax.ShapeDtypeStruct(dims, kind)


class Plan:
    def __init__(self, initial_state, drive_modes):
        _, self.levels, self.nx, self.ny = initial_state.shape
        self.windows, _, self.modes, _ = drive_modes.shape
        self.px = lax.axis_size("px")
        self.py = lax.axis_size("py")
        self.nest = lax.axis_size("nest")
        self.lanes = self.levels * self.modes
        self.half = self.levels // 2
        self.low = self.modes + EDGE
        self.rows = self.low + EDGE
        self.x = tables(self.nx * self.px, self.modes, self.windows)
        self.y = tables(self.ny * self.py, self.modes, self.windows)
        assert self.levels % 4 == 0 and self.modes * 2 == self.ny and self.nx == self.modes
        assert self.windows == 3 and self.half == 2 and EDGE * EDGE == self.modes

    def pairs(self, value):
        width = 2 * self.modes
        return jnp.concatenate([value[:, i * width : (i + 1) * width] for i in range(self.half)], 0)

    def unpairs(self, value):
        rows = value.shape[0] // self.half
        return jnp.concatenate([value[i * rows : (i + 1) * rows] for i in range(self.half)], 1)


def project(plan, state, rates, halved):
    low, half, lanes, levels = plan.low, plan.half, plan.lanes, plan.levels
    modes, nx, ny, windows = plan.modes, plan.nx, plan.ny, plan.windows
    bases = np.concatenate([plan.x["base"], plan.x["edges"], np.zeros((nx * plan.px, EDGE))], 1)
    left = right_table(bases.T.reshape(low + EDGE, plan.px, nx).transpose(1, 0, 2))
    base_y = plan.y["base"].reshape(plan.py, ny, modes)
    edge_y = plan.y["edges"].reshape(plan.py, ny, EDGE)
    right, edge = [], []
    for at in range(plan.py):
        high, small = parts_of(base_y[at])
        corner = bf16(np.repeat(edge_y[at], EDGE, 1))
        right.append(np.concatenate([high, small, corner, np.zeros_like(corner)], 1))
        edge.append(bf16(np.pad(np.tile(edge_y[at].T, (1, 2)), ((0, EDGE), (0, 0)))))
    pick = np.zeros((2 * EDGE, 2 * ny))
    for i in range(windows):
        pick[i, [i, ny + i]] = 1
        pick[windows + i, [ny - windows + i, 2 * ny - windows + i]] = 1

    def kernel(state_ref, left_ref, right_ref, edge_ref, pick_ref, rates_ref, out_ref, along_ref):
        px, py = lax.axis_index("px"), lax.axis_index("py")
        field = jnp.concatenate([state_ref[0, level] for level in range(levels)], 1)
        high, small = halves(field)
        table = left_ref[px]
        rows = dot(table, jnp.concatenate([high, high], 0)) + dot(table[:, :nx], small)
        found = jnp.concatenate([rows[:low, i * ny : (i + 1) * ny] for i in range(levels)], 0)
        high, small = halves(found)
        table = right_ref[py]
        found = dot(high, table) + dot(small, table)
        both = found[:, :ny] + pltpu.roll(found[:, :ny], modes, 1)
        left_lane = lax.broadcasted_iota(jnp.int32, (low, ny), 1) < modes
        both = [both[i * low : (i + 1) * low] for i in range(levels)]
        both = [jnp.where(left_lane, both[2 * i], both[2 * i + 1]) for i in range(half)]
        both = jnp.concatenate(both, 1)
        out_ref[:modes] = both[:modes]
        ends = both[modes:]
        cells = [found[i * low + modes : (i + 1) * low, ny:] for i in range(levels)]
        cells = [cells[2 * i] + pltpu.roll(cells[2 * i + 1], modes, 1) for i in range(half)]
        cells = jnp.concatenate(cells, 1)
        row = lax.broadcasted_iota(jnp.int32, (EDGE, lanes), 0)
        lane = lax.broadcasted_iota(jnp.int32, (EDGE, lanes), 1)
        cells = jnp.sum(jnp.where(lane % EDGE == row, cells, 0.0), 0, keepdims=True)
        lane = lane[:1]
        gain = jnp.zeros((1, lanes), jnp.float32)
        for i in range(levels):
            gain = jnp.where(lane // modes == i, rates_ref[0, i], gain)
        gain = jnp.where((px == 0) & (py == 0) & (lane % modes >= 2 * windows * EDGE), gain, 0.0)
        upright = jnp.concatenate([rows[:modes, i * ny : (i + 1) * ny] for i in range(levels)], 0)
        upright = jnp.concatenate(halves(upright), 1)
        sides = dot(edge_ref[py], upright, ((1,), (1,)))[: 2 * windows]
        patch = jnp.concatenate([state_ref[0, level] for level in range(levels)], 0)
        patch = jnp.concatenate(halves(patch), 1)
        columns = dot(pick_ref[...], patch, ((1,), (1,)))[:EDGE]
        if halved:
            ends = jnp.where(px < plan.px // 2, ends[:windows], ends[windows : 2 * windows])
            out_ref[modes:low] = jnp.concatenate([sides, cells + gain, ends[:1]], 0)
            out_ref[low:] = jnp.concatenate([ends[1:], columns[: 2 * windows]], 0)
            along_ref[:low] = out_ref[:low]
            along_ref[low:] = jnp.concatenate([ends[1:], facing_rows(plan, state_ref, px % 2 == 0)], 0)
        else:
            blank = jnp.zeros((2, lanes), jnp.float32)
            out_ref[modes:low] = jnp.concatenate([sides, cells + gain, blank[:1]], 0)
            out_ref[low:] = jnp.concatenate([ends[: 2 * windows], blank], 0)
            along_ref[...] = columns

    return call(
        kernel,
        (shape_of(plan.rows, lanes), shape_of(plan.rows if halved else EDGE, lanes)),
        state, left, jnp.asarray(np.stack(right)), jnp.asarray(np.stack(edge)),
        jnp.asarray(bf16(pick)), rates,
        first=True,
    )


def facing_rows(plan, state_ref, bottom):
    rows = []
    for group in range(plan.half):
        pair = [state_ref[0, 2 * group + i] for i in range(2)]
        top = jnp.concatenate([p[: plan.windows] for p in pair], 1)
        end = jnp.concatenate([p[plan.nx - plan.windows :] for p in pair], 1)
        rows.append(jnp.where(bottom, end, top))
    return jnp.concatenate(rows, 0)


def facing_corners(plan, columns, bottom):
    lane = lax.broadcasted_iota(jnp.int32, columns.shape, 1)
    moved = pltpu.roll(columns, plan.lanes - (plan.nx - plan.windows), 1)
    near = jnp.where(lane % plan.nx < plan.windows, jnp.where(bottom, moved, columns), 0.0)
    first = columns.shape[0] - 2 * plan.windows
    packed = near[first : first + 1]
    for i in range(1, 2 * plan.windows):
        packed = packed + pltpu.roll(near, EDGE * i, 1)[first + i : first + i + 1]
    return packed


def join_first(plan, own, from_y, from_x, from_both, state):
    low, modes, windows, lanes = plan.low, plan.modes, plan.windows, plan.lanes

    def kernel(own_ref, y_ref, x_ref, both_ref, state_ref, out_ref, halo_ref):
        px = lax.axis_index("px")
        odd, lower = px % 2 == 1, px < plan.px // 2
        out_ref[:modes] = (own_ref[:modes] + y_ref[:modes]) + (x_ref[:modes] + both_ref[:modes])
        middle = (own_ref[modes:low] + y_ref[modes:low]) + (x_ref[modes:low] + both_ref[modes:low])
        corners = facing_corners(plan, y_ref[low:], odd)
        corners = jnp.where(lower, pltpu.roll(corners, windows, 1), corners)
        row = lax.broadcasted_iota(jnp.int32, (EDGE, lanes), 0)
        out_ref[modes:low] = middle + jnp.where(row == 2 * windows, corners, 0.0)
        ends = (own_ref[low:] + y_ref[low:]) + (x_ref[low:] + both_ref[low:])
        out_ref[low:] = jnp.concatenate([ends[: windows - 1], facing_rows(plan, state_ref, odd)], 0)
        corners = facing_corners(plan, both_ref[low:], odd)
        lines = x_ref[low:][windows - 1 :]
        halo_ref[...] = jnp.concatenate([lines, corners, jnp.zeros((1, lanes), jnp.float32)], 0)

    shapes = shape_of(plan.rows, lanes), shape_of(EDGE, lanes)
    return call(kernel, shapes, own, from_y, from_x, from_both, state)


def both_facing(plan, state, columns):
    def kernel(state_ref, columns_ref, top_ref, bottom_ref):
        columns = columns_ref[...]
        columns = jnp.concatenate([jnp.zeros((2, plan.lanes), jnp.float32), columns[: 2 * plan.windows]], 0)
        for ref, bottom in ((top_ref, False), (bottom_ref, True)):
            rows = [facing_rows(plan, state_ref, bottom), facing_corners(plan, columns, bottom)]
            ref[...] = jnp.concatenate(rows + [jnp.zeros((1, plan.lanes), jnp.float32)], 0)

    return call(kernel, (shape_of(EDGE, plan.lanes),) * 2, state, columns)


def join_last(plan, own, other):
    low, modes, windows, lanes = plan.low, plan.modes, plan.windows, plan.lanes

    def kernel(own_ref, other_ref, out_ref):
        lower = lax.axis_index("px") < plan.px // 2
        out_ref[:modes] = own_ref[:modes] + other_ref[:modes]
        row = lax.broadcasted_iota(jnp.int32, (EDGE, lanes), 0)
        lane = lax.broadcasted_iota(jnp.int32, (EDGE, lanes), 1)
        one, two = own_ref[modes:low], other_ref[modes:low]
        early, late = jnp.where(lower, one, two), jnp.where(lower, two, one)
        kept = (row < 2 * windows) | (lane % modes >= 2 * windows * EDGE)
        middle = jnp.where(kept | (lane % EDGE < windows), early, 0.0)
        middle = middle + jnp.where(kept | (lane % EDGE >= windows), late, 0.0)
        out_ref[modes:low] = jnp.where(row <= 2 * windows, middle, 0.0)
        ends = []
        for block, rest in ((early, jnp.where(lower, own_ref[low:], other_ref[low:])),
                            (late, jnp.where(lower, other_ref[low:], own_ref[low:]))):
            ends += [block[EDGE - 1 :], rest[: windows - 1]]
        out_ref[low:] = jnp.concatenate(ends + [jnp.zeros((EDGE - 2 * windows, lanes), jnp.float32)], 0)

    return call(kernel, shape_of(plan.rows, lanes), own, other)


def step_patch(plan, state, columns, first, second):
    nx, ny, windows, low, levels = plan.nx, plan.ny, plan.windows, plan.low, plan.levels
    place = np.zeros((4 * EDGE, ny))
    for i in range(windows):
        for part in range(3):
            place[part * EDGE + i, i] = 1
            place[part * EDGE + windows + i, ny - windows + i] = 1
    rows, lanes = nx + 2 * EDGE, 2 * ny

    def kernel(state_ref, columns_ref, first_ref, second_ref, place_ref, out_ref):
        px, py = lax.axis_index("px"), lax.axis_index("py")
        row = lax.broadcasted_iota(jnp.int32, (rows, lanes), 0) - EDGE + px * nx
        lane = lax.broadcasted_iota(jnp.int32, (rows, lanes), 1)
        lane = jnp.where(lane >= ny + ny // 2, lane - lanes, lane) + py * ny
        inside = (row >= 0) & (row < nx * plan.px) & (lane >= 0) & (lane < ny * plan.py)
        where = place_ref[...]

        def spread(block):
            high = block.astype(jnp.bfloat16).astype(jnp.float32)
            rest = block - high
            middle = rest.astype(jnp.bfloat16).astype(jnp.float32)
            parts = [high, middle, rest - middle, jnp.zeros_like(high)]
            return dot(jnp.concatenate(parts, 0).astype(jnp.bfloat16), where, ((0,), (0,)))

        small_row = lax.broadcasted_iota(jnp.int32, (EDGE, plan.lanes), 0)
        small_lane = lax.broadcasted_iota(jnp.int32, (EDGE, plan.lanes), 1)
        mine = small_lane % nx // EDGE == small_row

        def corners(block):
            line = jnp.broadcast_to(block[2 * windows : 2 * windows + 1], (EDGE, plan.lanes))
            cells = spread(jnp.where(mine, line, 0.0))
            return [
                sum(cells[level * nx + EDGE * i : level * nx + EDGE * (i + 1)] for i in range(2 * windows))
                for level in range(levels)
            ]

        even = px % 2 == 0
        one, two, columns = first_ref[...], second_ref[-EDGE:], columns_ref[-EDGE:]
        if second_ref.shape[0] > EDGE:
            mixed = second_ref[low - 2 : low - 1]
            mixed = jnp.where(px < plan.px // 2, mixed, pltpu.roll(mixed, plan.lanes - windows, 1))
            two = jnp.concatenate([two[windows - 1 :], mixed, mixed], 0)
            columns = jnp.concatenate([columns[windows - 1 :], columns[: windows - 1]], 0)
        above, below = jnp.where(even, two, one), jnp.where(even, one, two)
        beside = spread(columns)
        beside_above, beside_below = corners(above), corners(below)
        blank = jnp.zeros((EDGE - windows, lanes), jnp.float32)
        for level in range(levels):
            pair, part = level // 2, level % 2

            def line(block):
                return block[pair * windows : (pair + 1) * windows, part * ny : (part + 1) * ny]

            up = jnp.concatenate([line(above), beside_above[level][:windows]], 1)
            down = jnp.concatenate([line(below), beside_below[level][:windows]], 1)
            middle = jnp.concatenate([state_ref[0, level], beside[level * nx : (level + 1) * nx]], 1)
            field = jnp.concatenate([blank, up, middle, down, blank], 0)
            field = jnp.where(inside, field, 0.0)
            for _ in range(windows):
                around = (
                    pltpu.roll(field, 1, 0)
                    + pltpu.roll(field, rows - 1, 0)
                    + pltpu.roll(field, 1, 1)
                    + pltpu.roll(field, lanes - 1, 1)
                )
                field = jnp.where(inside, field + RATE * (around - 4.0 * field), 0.0)
            out_ref[level] = field[EDGE : EDGE + nx, :ny]

    return call(
        kernel, shape_of(levels, nx, ny), state, columns, first, second, jnp.asarray(bf16(place))
    )


def prepare(plan, drive, nest_offsets):
    modes, lanes, levels, windows = plan.modes, plan.lanes, plan.levels, plan.windows
    nx, ny, x, y = plan.nx, plan.ny, plan.x, plan.y
    steps = plan.nest - 1
    maps_x = f32(np.stack([np.tile(x[name], (1, 2)) for name in ("cos_map", "sin_map")]))
    maps_y = f32(np.stack([kron(2, y[name].T) for name in ("cos_map", "sin_map")]))
    rows_x = np.stack([np.tile(p, (1, 2)).reshape(plan.px, nx, 2 * modes) for p in x["powers"][:windows]], 1)
    rows_y = np.stack(
        [p.reshape(plan.py, ny, modes).transpose(0, 2, 1) for p in y["powers"][:windows]], 1
    )

    def kernel(
        drive_ref, maps_x_ref, maps_y_ref, rows_x_ref, rows_y_ref, offsets_ref,
        drive_out, row_out, col_out, spread_x_out, spread_y_out,
    ):
        nest, px, py = lax.axis_index("nest"), lax.axis_index("px"), lax.axis_index("py")
        for w in range(windows):
            drive_out[w] = jnp.concatenate([drive_ref[w, level] for level in range(levels)], 1)
        lane = lax.broadcasted_iota(jnp.int32, (modes, 2 * modes), 1)

        def as_left(twice):
            rounded = twice.astype(jnp.bfloat16).astype(jnp.float32)
            pair = jnp.where(lane >= modes, twice - rounded, rounded)
            return jnp.concatenate([pair, rounded], 1)[:, : 3 * modes].astype(jnp.bfloat16)

        def angle(mode, offset, cells):
            turn = (mode * offset).astype(jnp.float32)
            turn = turn - jnp.floor(turn / (2.0 * cells)) * (2.0 * cells)
            return turn * (math.pi / cells)

        mode = lax.broadcasted_iota(jnp.int32, (EDGE, 2 * modes), 1) % modes
        row = lax.broadcasted_iota(jnp.int32, (EDGE, 2 * modes), 0)
        upright = lax.broadcasted_iota(jnp.int32, (2 * modes, 2 * modes), 0) % modes
        place = lax.broadcasted_iota(jnp.int32, (2 * modes, 2 * modes), 1)
        along, down = jnp.zeros_like(mode), jnp.zeros_like(upright)
        for slot in range(steps):
            domain = jnp.maximum(nest - slot, 0)
            along = jnp.where(row == slot, offsets_ref[0, domain], along)
            down = jnp.where(place == slot, offsets_ref[1, domain], down)
        along = angle(mode, along, nx * plan.px)
        down = angle(upright, down, ny * plan.py)
        cos_x, sin_x = jnp.cos(along), jnp.sin(along)
        cos_y, sin_y = jnp.cos(down), jnp.sin(down)
        for slot in range(steps):
            at = slice(slot, slot + 1)
            row_out[slot] = as_left(maps_x_ref[0] * cos_x[at] - maps_x_ref[1] * sin_x[at])
            col_map = maps_y_ref[0] * cos_y[:, at] - maps_y_ref[1] * sin_y[:, at]
            high, small = halves(col_map)
            col_out[slot] = jnp.concatenate([high, small], 1)
        for w in range(windows):
            p = windows - 1 - w
            for j in range(p + 1):
                combined = sum(multinomial(p, i, j) * rows_x_ref[px, i] for i in range(p - j + 1))
                at = (sum(range(p + 1)) + j) * nx
                spread_x_out[at : at + nx] = as_left(combined)
        for j in range(windows):
            spread_y_out[j] = jnp.concatenate(halves(rows_y_ref[py, j]), 0)

    shapes = (
        shape_of(windows, modes, lanes),
        shape_of(steps, modes, 3 * modes, kind=jnp.bfloat16),
        shape_of(steps, 2 * modes, 4 * modes, kind=jnp.bfloat16),
        shape_of(sum(range(windows + 1)) * nx, 3 * modes, kind=jnp.bfloat16),
        shape_of(windows, 2 * modes, ny, kind=jnp.bfloat16),
    )
    return call(kernel, shapes, drive, maps_x, maps_y, f32(rows_x), f32(rows_y), nest_offsets.T, first=True)


def own_tables(plan):
    x, y, modes, windows = plan.x, plan.y, plan.modes, plan.windows
    inward = np.concatenate([np.tile(y["spill"][j].T, (1, 2)) for j in range(1, windows + 1)], 1)
    high, small = parts_of(inward)
    inward = jnp.asarray(np.concatenate([high, small, high, np.zeros_like(high)], 0))
    corner = np.concatenate(
        [kron(2, np.repeat(y["spill"][j].T, EDGE, 0)) for j in range(1, windows + 1)], 1
    )
    high, small = parts_of(corner)
    corner = jnp.asarray(np.concatenate([high, small], 0))
    across = np.zeros((windows * modes, windows * EDGE))
    for n in range(1, windows + 1):
        for j in range(n):
            across[(n - 1) * modes : n * modes, j * EDGE : (j + 1) * EDGE] = sum(
                multinomial(n, i, j) * x["spill"][i] for i in range(1, n - j + 1)
            )
    high, small = parts_of(across)
    across = jnp.asarray(np.pad(np.concatenate([high, small, high], 1), ((0, 0), (0, 3 * EDGE))))
    scale_x = f32(np.broadcast_to(1.0 + x["factor"][:, None], (modes, plan.lanes)))
    scale_y = f32(np.broadcast_to(np.tile(y["factor"], plan.levels), (EDGE, plan.lanes)))
    return inward, corner, across, scale_x, scale_y


def own_modes_of(plan, inward_ref, corner_ref, across_ref, scale_x_ref, scale_y_ref):
    modes, low, lanes = plan.modes, plan.low, plan.lanes
    windows, half, ny = plan.windows, plan.half, plan.ny
    scale_x, scale_y = scale_x_ref[...], scale_y_ref[:1]
    row = lax.broadcasted_iota(jnp.int32, (EDGE, lanes), 0)
    lane = lax.broadcasted_iota(jnp.int32, (EDGE, lanes), 1)
    mine = lane % EDGE == row
    left_lane = lax.broadcasted_iota(jnp.int32, (modes, ny), 1) < modes

    def own_modes(message):
        rows, middle, ends = message[:modes], message[modes:low], message[low:]
        sides = dot(short_stacked(middle, 4 * EDGE), inward_ref[...], ((0,), (0,)))
        cells = jnp.where(mine, jnp.broadcast_to(middle[EDGE - 2 : EDGE - 1], (EDGE, lanes)), 0.0)
        cells = jnp.concatenate([cells[:, i * ny : (i + 1) * ny] for i in range(half)], 0)
        cells = by_parts(cells, corner_ref[:ny], corner_ref[ny:])
        turned, ends = [rows], [ends]
        for j in range(windows):
            at = slice(j * ny, (j + 1) * ny)
            side = [
                jnp.where(
                    left_lane,
                    sides[2 * i * modes : (2 * i + 1) * modes, at],
                    sides[(2 * i + 1) * modes : (2 * i + 2) * modes, at],
                )
                for i in range(half)
            ]
            cell = [cells[i * EDGE : (i + 1) * EDGE, at] for i in range(half)]
            power = scale_y if j == 0 else power * scale_y
            turned.append(rows * power + jnp.concatenate(side, 1))
            ends.append(ends[0] * power + jnp.concatenate(cell, 1))
        over = dot(across_ref[...], short_stacked(jnp.concatenate(ends[:windows], 0), 12 * EDGE))
        result = []
        for n in range(windows):
            turned = [a * scale_x + b for a, b in zip(turned[:-1], turned[1:])]
            result.append(turned[0] + over[n * modes : (n + 1) * modes])
        return result

    return own_modes


def own_early(plan, tables, messages):
    def kernel(*refs):
        count = len(messages)
        own_modes = own_modes_of(plan, *refs[count : count + len(tables)])
        for i in range(count):
            for w, value in enumerate(own_modes(refs[i][...])):
                refs[count + len(tables)][i, w] = value

    return call(kernel, shape_of(len(messages), plan.windows, plan.modes, plan.lanes), *messages, *tables)


def nudge(plan, stepped, gathered, early, tables, crossed, prepared):
    modes, low, lanes, levels = plan.modes, plan.low, plan.lanes, plan.levels
    windows, half, nx, ny = plan.windows, plan.half, plan.nx, plan.ny
    x, y = plan.x, plan.y
    pairs, unpairs = plan.pairs, plan.unpairs
    again = []
    for p in range(1, windows):
        again.append(sum(multinomial(p, i, 0) * x["within"][i] for i in range(p + 1)))
    again = left_table(np.concatenate(again, 0))
    sideways = jnp.stack([right_table(kron(2, y["within"][j])) for j in range(1, windows)])
    drive, row_maps, col_maps, spread_x, spread_y = prepared

    def kernel(
        stepped_ref, drive_ref, row_ref, col_ref, spread_x_ref, spread_y_ref, again_ref, sideways_ref,
        early_ref, *refs,
    ):
        refs, (state_ref, modes_ref) = refs[:-2], refs[-2:]
        root = plan.nest - 1
        nest = lax.axis_index("nest")
        refs, table_refs = refs[: plan.nest], refs[plan.nest :]
        lane = lax.broadcasted_iota(jnp.int32, (1, lanes), 1)
        gains = []
        for ref in refs:
            gain = jnp.where(lane % modes >= modes - 2 * EDGE, ref[low - 2 : low - 1], 0.0)
            gain = gain + pltpu.roll(gain, lanes - 2 * EDGE, 1)
            gains.append(gain + pltpu.roll(gain, lanes - 4 * EDGE, 1))
        owns = [[early_ref[i, w] for w in range(windows)] for i in range(root)]
        owns.append(own_modes_of(plan, *table_refs)(refs[root][...]))
        if crossed:
            odd = nest % 2 == 1
            gains = [gains[0], jnp.where(odd, gains[2], gains[3]), gains[1], gains[3]]
            mixed = [jnp.where(odd, a, b) for a, b in zip(owns[2], owns[3])]
            owns = [owns[0], mixed, owns[1], owns[3]]
        coeffs, changes, later = {}, {}, {}
        for front in range(root + windows):
            cells = [(root - front + w, w) for w in range(windows) if 0 <= root - front + w <= root]
            inner, lefts, rights = {}, {}, {}
            for slot, w in cells:
                if slot < root:
                    inner[slot, w] = times_right(pairs(coeffs[slot + 1, w]), col_ref[slot])
                if w > 0:
                    change = changes[slot, w - 1]
                    count = windows - w
                    left = dot(again_ref[: count * modes], stacked(change))
                    lefts[slot] = left = [left[i * modes : (i + 1) * modes] for i in range(count)]
                    rights[slot] = [unpairs(times_right(pairs(change), sideways_ref[i])) for i in range(count)]
                    later[slot, w - 1, 1] = left[0] + rights[slot][0]
            for slot, w in cells:
                target = drive_ref[w]
                if slot < root:
                    found = dot(row_ref[slot], stacked(unpairs(inner[slot, w])))
                    target = jnp.where(nest <= slot, target, found)
                before = owns[slot][w]
                for v in range(w):
                    before = before + later[slot, v, w - v]
                changes[slot, w] = gains[slot] * (target - before)
                coeffs[slot, w] = before + changes[slot, w]
            for slot, w in cells:
                if w > 0 and windows - w > 1:
                    left, right = lefts[slot], rights[slot]
                    mixed = unpairs(times_right(pairs(left[0]), sideways_ref[0]))
                    later[slot, w - 1, 2] = left[1] + (2.0 * mixed + right[1])
        changes = [changes[0, w] for w in range(windows)]
        coeffs = [coeffs[0, w] for w in range(windows)]
        for level in range(levels):
            modes_ref[0, level] = coeffs[-1][:, level * modes : (level + 1) * modes]
        spread = [0.0] * windows
        for w in range(windows):
            p = windows - 1 - w
            at = sum(range(p + 1)) * nx
            found = dot(spread_x_ref[at : at + (p + 1) * nx], stacked(changes[w]))
            for j in range(p + 1):
                spread[j] = spread[j] + found[j * nx : (j + 1) * nx]
        field = 0.0
        for j in range(windows):
            table, blank = spread_y_ref[j], jnp.zeros((modes, ny), jnp.bfloat16)
            both = [
                jnp.concatenate([jnp.concatenate([t, blank], 1), jnp.concatenate([blank, t], 1)], 0)
                for t in (table[:modes], table[modes:])
            ]
            part = by_parts(pairs(spread[j]), *both)
            field = field + part
        for level in range(levels):
            at_row, at = level // 2 * nx, level % 2 * ny
            state_ref[0, level] = stepped_ref[level] + field[at_row : at_row + nx, at : at + ny]

    return call(
        kernel,
        (shape_of(1, levels, nx, ny), shape_of(1, levels, modes, modes)),
        stepped, drive, row_maps, col_maps, spread_x, spread_y, again, sideways, early, *gathered, *tables,
        final=True,
    )


def swap(value, axis, partner):
    size = math.prod(lax.axis_size(name) for name in (axis if isinstance(axis, tuple) else (axis,)))
    return lax.ppermute(value, axis, [(i, partner(i)) for i in range(size) if 0 <= partner(i) < size])


def body(initial_state, drive_modes, relax_rates, nest_offsets):
    plan = Plan(initial_state, drive_modes)
    halved = plan.py == 2 and plan.px == 4
    share, along = project(plan, initial_state, relax_rates, halved)
    if halved:
        share = lax.optimization_barrier(share)
        from_y = swap(share, "py", lambda i: i ^ 1)
        from_x = swap(along, "px", lambda i: i ^ 1)
        from_both = swap(share, ("py", "px"), lambda i: i ^ (plan.px + 1))
        total, halo = join_first(plan, share, from_y, from_x, from_both, initial_state)
        columns = from_y
        total, drive_modes, nest_offsets = lax.optimization_barrier((total, drive_modes, nest_offsets))
        across = swap(total, "px", lambda i: i ^ 3)
        prepared = prepare(plan, drive_modes, nest_offsets)
        across, prepared = lax.optimization_barrier((across, prepared))
        last = join_last(plan, total, across)
    else:
        from_right = jnp.arange(EDGE)[:, None] < plan.windows
        right = swap(along, "py", lambda i: i - 1)
        left = swap(along, "py", lambda i: i + 1)
        columns = jnp.where(from_right, right, left)
        top, bottom = both_facing(plan, initial_state, columns)
        above = swap(bottom, "px", lambda i: i + 1)
        below = swap(top, "px", lambda i: i - 1)
        even = lax.axis_index("px") % 2 == 0
        halo, across = jnp.where(even, below, above), jnp.where(even, above, below)
        last = lax.psum(share, ("py", "px"))
        prepared = prepare(plan, drive_modes, nest_offsets)
    crossed = plan.nest == 4
    if crossed:
        core = swap(last, "nest", lambda i: i ^ 1)
        chip = swap(last, "nest", lambda i: i ^ 2)
        stepped = step_patch(plan, initial_state, columns, halo, across)
        chip, stepped = lax.optimization_barrier((chip, stepped))
        gathered = [last, chip, core, swap(last, "nest", lambda i: i ^ 3)]
    else:
        gathered = [last] + [swap(last, "nest", lambda i, s=s: i + s) for s in range(1, plan.nest)]
        stepped = step_patch(plan, initial_state, columns, halo, across)
    tables = own_tables(plan)
    early = own_early(plan, tables, gathered[:-1])
    return nudge(plan, stepped, gathered, early, tables, crossed, prepared)


def solution(mesh):
    return jax.shard_map(
        body,
        mesh=mesh,
        in_specs=(P("nest", None, "px", "py"), P(), P("nest", None), P()),
        out_specs=(P("nest", None, "px", "py"), P("nest", None, None, None)),
        check_vma=False,
    )
```

```python
import functools
import math

import jax
import jax.numpy as jnp
import numpy as np
from jax import lax
from jax.experimental import pallas as pl
from jax.experimental.pallas import tpu as pltpu
from jax.sharding import PartitionSpec as P

RATIO = 3
RATE = 0.2
EDGE = 8
INTERPRET = False


def multinomial(n, i, j):
    return math.factorial(n) // (math.factorial(i) * math.factorial(j) * math.factorial(n - i - j))


@functools.lru_cache(maxsize=None)
def tables(cells, modes, order):
    cell = np.arange(cells)
    mode = np.arange(modes)
    weight = np.sqrt(np.where(mode == 0, 1.0, 2.0) / cells)
    product = mode[None] * (2 * cell[:, None] + 1)
    coarse = np.pi * (product % (4 * cells)) / (2 * cells)
    fine = np.pi * (product % (4 * RATIO * cells)) / (2 * RATIO * cells)
    base = weight * np.cos(coarse)
    second = RATE * (np.eye(cells, k=1) + np.eye(cells, k=-1) - 2 * np.eye(cells))
    powers = [base]
    for _ in range(order):
        powers.append(second @ powers[-1])
    factor = RATE * (2 * np.cos(np.pi * mode / cells) - 2)
    places = list(range(order)) + list(range(cells - order, cells))
    edges = np.zeros((cells, EDGE))
    edges[places, range(2 * order)] = 1
    spill = [(powers[i] - base * factor**i).T @ edges for i in range(order + 1)]
    return {
        "base": base,
        "edges": edges,
        "powers": powers,
        "factor": factor,
        "spill": spill,
        "within": [base.T @ power for power in powers],
        "cos_map": base.T @ (weight * np.cos(fine)),
        "sin_map": base.T @ (weight * np.sin(fine)),
    }


def kron(count, block):
    return np.kron(np.eye(count), block)


def f32(value):
    return jnp.asarray(np.asarray(value, np.float32))


def bf16(value):
    return np.asarray(value, jnp.bfloat16)


def parts_of(value):
    high = bf16(value)
    return high, bf16(value - high.astype(np.float64))


def left_table(value):
    high, low = parts_of(value)
    return jnp.asarray(np.concatenate([high, low, high], -1))


def right_table(value):
    return jnp.asarray(np.concatenate(parts_of(value), -1))


def halves(value):
    high = value.astype(jnp.bfloat16)
    return high, (value - high.astype(jnp.float32)).astype(jnp.bfloat16)


def dot(a, b, dims=((1,), (0,))):
    return lax.dot_general(a, b, (dims, ((), ())), preferred_element_type=jnp.float32)


def stacked(value):
    high, low = halves(value)
    return jnp.concatenate([high, high, low], 0)


def short_stacked(value, rows):
    high = value.astype(jnp.bfloat16).astype(jnp.float32)
    blank = jnp.zeros((rows - 3 * value.shape[0], value.shape[1]), jnp.float32)
    return jnp.concatenate([high, high, value - high, blank], 0).astype(jnp.bfloat16)


def times_right(value, table):
    width = table.shape[1] // 2
    lower = jnp.concatenate([table[:, :width], jnp.zeros_like(table[:, width:])], 1)
    out = dot(jnp.concatenate(halves(value), 1), jnp.concatenate([table, lower], 0))
    return out[:, :width] + out[:, width:]


def by_parts(value, table, rest):
    high, low = halves(value)
    out = dot(jnp.concatenate([high, low], 0), table)
    return out[: value.shape[0]] + out[value.shape[0] :] + dot(high, rest)


def in_vmem(value):
    return value if INTERPRET else pltpu.with_memory_space_constraint(value, pltpu.VMEM)


def call(kernel, shapes, *args, first=False, final=False, split=0):
    scalars = [a.ndim == 2 and a.size <= 16 for a in args]
    specs = [pl.BlockSpec(memory_space=pltpu.SMEM if s else pltpu.VMEM) for s in scalars]
    for i in range(split):
        block = (1, 1) + args[i].shape[2:]
        specs[i] = pl.BlockSpec(block, lambda _, i=i: (0, i, 0, 0), memory_space=pltpu.VMEM)
    if not final and not INTERPRET:
        shapes = jax.tree.map(lambda s: pltpu.VMEM(s.shape, s.dtype), shapes)
    return pl.pallas_call(
        kernel,
        grid=(1,) if split else (),
        in_specs=specs,
        out_specs=jax.tree.map(lambda _: pl.BlockSpec(memory_space=pltpu.VMEM), shapes),
        out_shape=shapes,
        interpret=INTERPRET,
    )(*[a if s or first else in_vmem(a) for a, s in zip(args, scalars)])


def shape_of(*dims, kind=jnp.float32):
    return jax.ShapeDtypeStruct(dims, kind)


class Plan:
    def __init__(self, initial_state, drive_modes):
        _, self.levels, self.nx, self.ny = initial_state.shape
        self.windows, _, self.modes, _ = drive_modes.shape
        self.px = lax.axis_size("px")
        self.py = lax.axis_size("py")
        self.nest = lax.axis_size("nest")
        self.lanes = self.levels * self.modes
        self.half = self.levels // 2
        self.low = self.modes + EDGE
        self.rows = self.low + EDGE
        self.x = tables(self.nx * self.px, self.modes, self.windows)
        self.y = tables(self.ny * self.py, self.modes, self.windows)
        assert self.levels % 4 == 0 and self.modes * 2 == self.ny and self.nx == self.modes
        assert self.windows == 3 and self.half == 2 and EDGE * EDGE == self.modes

    def pairs(self, value):
        width = 2 * self.modes
        return jnp.concatenate([value[:, i * width : (i + 1) * width] for i in range(self.half)], 0)

    def unpairs(self, value):
        rows = value.shape[0] // self.half
        return jnp.concatenate([value[i * rows : (i + 1) * rows] for i in range(self.half)], 1)


class Levels:
    def __init__(self, refs):
        self.refs = refs

    def __getitem__(self, at):
        return self.refs[at[1]][0, 0]


def project(plan, state, rates, halved):
    low, half, lanes, levels = plan.low, plan.half, plan.lanes, plan.levels
    modes, nx, ny, windows = plan.modes, plan.nx, plan.ny, plan.windows
    bases = np.concatenate([plan.x["base"], plan.x["edges"], np.zeros((nx * plan.px, EDGE))], 1)
    left = right_table(bases.T.reshape(low + EDGE, plan.px, nx).transpose(1, 0, 2))
    base_y = plan.y["base"].reshape(plan.py, ny, modes)
    edge_y = plan.y["edges"].reshape(plan.py, ny, EDGE)
    right, edge = [], []
    for at in range(plan.py):
        high, small = parts_of(base_y[at])
        corner = bf16(np.repeat(edge_y[at], EDGE, 1))
        right.append(np.concatenate([high, small, corner, np.zeros_like(corner)], 1))
        edge.append(bf16(np.pad(np.tile(edge_y[at].T, (1, 2)), ((0, EDGE), (0, 0)))))
    pick = np.zeros((2 * EDGE, 2 * ny))
    for i in range(windows):
        pick[i, [i, ny + i]] = 1
        pick[windows + i, [ny - windows + i, 2 * ny - windows + i]] = 1

    def kernel(*refs):
        state_ref = Levels(refs[:levels])
        left_ref, right_ref, edge_ref, pick_ref, rates_ref, out_ref, along_ref = refs[levels:]
        px, py = lax.axis_index("px"), lax.axis_index("py")
        field = jnp.concatenate([state_ref[0, level] for level in range(levels)], 1)
        high, small = halves(field)
        table = left_ref[px]
        rows = dot(table, jnp.concatenate([high, high], 0)) + dot(table[:, :nx], small)
        found = jnp.concatenate([rows[:low, i * ny : (i + 1) * ny] for i in range(levels)], 0)
        high, small = halves(found)
        table = right_ref[py]
        found = dot(high, table) + dot(small, table)
        both = found[:, :ny] + pltpu.roll(found[:, :ny], modes, 1)
        left_lane = lax.broadcasted_iota(jnp.int32, (low, ny), 1) < modes
        both = [both[i * low : (i + 1) * low] for i in range(levels)]
        both = [jnp.where(left_lane, both[2 * i], both[2 * i + 1]) for i in range(half)]
        both = jnp.concatenate(both, 1)
        out_ref[:modes] = both[:modes]
        ends = both[modes:]
        cells = [found[i * low + modes : (i + 1) * low, ny:] for i in range(levels)]
        cells = [cells[2 * i] + pltpu.roll(cells[2 * i + 1], modes, 1) for i in range(half)]
        cells = jnp.concatenate(cells, 1)
        row = lax.broadcasted_iota(jnp.int32, (EDGE, lanes), 0)
        lane = lax.broadcasted_iota(jnp.int32, (EDGE, lanes), 1)
        cells = jnp.sum(jnp.where(lane % EDGE == row, cells, 0.0), 0, keepdims=True)
        lane = lane[:1]
        gain = jnp.zeros((1, lanes), jnp.float32)
        for i in range(levels):
            gain = jnp.where(lane // modes == i, rates_ref[0, i], gain)
        gain = jnp.where((px == 0) & (py == 0) & (lane % modes >= 2 * windows * EDGE), gain, 0.0)
        upright = jnp.concatenate([rows[:modes, i * ny : (i + 1) * ny] for i in range(levels)], 0)
        upright = jnp.concatenate(halves(upright), 1)
        sides = dot(edge_ref[py], upright, ((1,), (1,)))[: 2 * windows]
        patch = jnp.concatenate([state_ref[0, level] for level in range(levels)], 0)
        patch = jnp.concatenate(halves(patch), 1)
        columns = dot(pick_ref[...], patch, ((1,), (1,)))[:EDGE]
        if halved:
            ends = jnp.where(px < plan.px // 2, ends[:windows], ends[windows : 2 * windows])
            out_ref[modes:low] = jnp.concatenate([sides, cells + gain, ends[:1]], 0)
            out_ref[low:] = jnp.concatenate([ends[1:], columns[: 2 * windows]], 0)
            along_ref[:low] = out_ref[:low]
            along_ref[low:] = jnp.concatenate([ends[1:], facing_rows(plan, state_ref, px % 2 == 0)], 0)
        else:
            blank = jnp.zeros((2, lanes), jnp.float32)
            out_ref[modes:low] = jnp.concatenate([sides, cells + gain, blank[:1]], 0)
            out_ref[low:] = jnp.concatenate([ends[: 2 * windows], blank], 0)
            along_ref[...] = columns

    return call(
        kernel,
        (shape_of(plan.rows, lanes), shape_of(plan.rows if halved else EDGE, lanes)),
        *[state] * levels, left, jnp.asarray(np.stack(right)), jnp.asarray(np.stack(edge)),
        jnp.asarray(bf16(pick)), rates,
        first=True,
        split=levels,
    )


def facing_rows(plan, state_ref, bottom):
    rows = []
    for group in range(plan.half):
        pair = [state_ref[0, 2 * group + i] for i in range(2)]
        top = jnp.concatenate([p[: plan.windows] for p in pair], 1)
        end = jnp.concatenate([p[plan.nx - plan.windows :] for p in pair], 1)
        rows.append(jnp.where(bottom, end, top))
    return jnp.concatenate(rows, 0)


def facing_corners(plan, columns, bottom):
    lane = lax.broadcasted_iota(jnp.int32, columns.shape, 1)
    moved = pltpu.roll(columns, plan.lanes - (plan.nx - plan.windows), 1)
    near = jnp.where(lane % plan.nx < plan.windows, jnp.where(bottom, moved, columns), 0.0)
    first = columns.shape[0] - 2 * plan.windows
    packed = near[first : first + 1]
    for i in range(1, 2 * plan.windows):
        packed = packed + pltpu.roll(near, EDGE * i, 1)[first + i : first + i + 1]
    return packed


def join_first(plan, own, from_y, from_x, from_both, state):
    low, modes, windows, lanes = plan.low, plan.modes, plan.windows, plan.lanes

    def kernel(own_ref, y_ref, x_ref, both_ref, state_ref, out_ref, halo_ref):
        px = lax.axis_index("px")
        odd, lower = px % 2 == 1, px < plan.px // 2
        out_ref[:modes] = (own_ref[:modes] + y_ref[:modes]) + (x_ref[:modes] + both_ref[:modes])
        middle = (own_ref[modes:low] + y_ref[modes:low]) + (x_ref[modes:low] + both_ref[modes:low])
        corners = facing_corners(plan, y_ref[low:], odd)
        corners = jnp.where(lower, pltpu.roll(corners, windows, 1), corners)
        row = lax.broadcasted_iota(jnp.int32, (EDGE, lanes), 0)
        out_ref[modes:low] = middle + jnp.where(row == 2 * windows, corners, 0.0)
        ends = (own_ref[low:] + y_ref[low:]) + (x_ref[low:] + both_ref[low:])
        out_ref[low:] = jnp.concatenate([ends[: windows - 1], facing_rows(plan, state_ref, odd)], 0)
        corners = facing_corners(plan, both_ref[low:], odd)
        lines = x_ref[low:][windows - 1 :]
        halo_ref[...] = jnp.concatenate([lines, corners, jnp.zeros((1, lanes), jnp.float32)], 0)

    shapes = shape_of(plan.rows, lanes), shape_of(EDGE, lanes)
    return call(kernel, shapes, own, from_y, from_x, from_both, state)


def both_facing(plan, state, columns):
    def kernel(state_ref, columns_ref, top_ref, bottom_ref):
        columns = columns_ref[...]
        columns = jnp.concatenate([jnp.zeros((2, plan.lanes), jnp.float32), columns[: 2 * plan.windows]], 0)
        for ref, bottom in ((top_ref, False), (bottom_ref, True)):
            rows = [facing_rows(plan, state_ref, bottom), facing_corners(plan, columns, bottom)]
            ref[...] = jnp.concatenate(rows + [jnp.zeros((1, plan.lanes), jnp.float32)], 0)

    return call(kernel, (shape_of(EDGE, plan.lanes),) * 2, state, columns)


def join_last(plan, own, other):
    low, modes, windows, lanes = plan.low, plan.modes, plan.windows, plan.lanes

    def kernel(own_ref, other_ref, out_ref):
        lower = lax.axis_index("px") < plan.px // 2
        out_ref[:modes] = own_ref[:modes] + other_ref[:modes]
        row = lax.broadcasted_iota(jnp.int32, (EDGE, lanes), 0)
        lane = lax.broadcasted_iota(jnp.int32, (EDGE, lanes), 1)
        one, two = own_ref[modes:low], other_ref[modes:low]
        early, late = jnp.where(lower, one, two), jnp.where(lower, two, one)
        kept = (row < 2 * windows) | (lane % modes >= 2 * windows * EDGE)
        middle = jnp.where(kept | (lane % EDGE < windows), early, 0.0)
        middle = middle + jnp.where(kept | (lane % EDGE >= windows), late, 0.0)
        out_ref[modes:low] = jnp.where(row <= 2 * windows, middle, 0.0)
        ends = []
        for block, rest in ((early, jnp.where(lower, own_ref[low:], other_ref[low:])),
                            (late, jnp.where(lower, other_ref[low:], own_ref[low:]))):
            ends += [block[EDGE - 1 :], rest[: windows - 1]]
        out_ref[low:] = jnp.concatenate(ends + [jnp.zeros((EDGE - 2 * windows, lanes), jnp.float32)], 0)

    return call(kernel, shape_of(plan.rows, lanes), own, other)


def step_patch(plan, state, columns, first, second):
    nx, ny, windows, low, levels = plan.nx, plan.ny, plan.windows, plan.low, plan.levels
    place = np.zeros((4 * EDGE, ny))
    for i in range(windows):
        for part in range(3):
            place[part * EDGE + i, i] = 1
            place[part * EDGE + windows + i, ny - windows + i] = 1
    rows, lanes = nx + 2 * EDGE, 2 * ny

    def kernel(state_ref, columns_ref, first_ref, second_ref, place_ref, out_ref):
        px, py = lax.axis_index("px"), lax.axis_index("py")
        row = lax.broadcasted_iota(jnp.int32, (rows, lanes), 0) - EDGE + px * nx
        lane = lax.broadcasted_iota(jnp.int32, (rows, lanes), 1)
        lane = jnp.where(lane >= ny + ny // 2, lane - lanes, lane) + py * ny
        inside = (row >= 0) & (row < nx * plan.px) & (lane >= 0) & (lane < ny * plan.py)
        where = place_ref[...]

        def spread(block):
            high = block.astype(jnp.bfloat16).astype(jnp.float32)
            rest = block - high
            middle = rest.astype(jnp.bfloat16).astype(jnp.float32)
            parts = [high, middle, rest - middle, jnp.zeros_like(high)]
            return dot(jnp.concatenate(parts, 0).astype(jnp.bfloat16), where, ((0,), (0,)))

        small_row = lax.broadcasted_iota(jnp.int32, (EDGE, plan.lanes), 0)
        small_lane = lax.broadcasted_iota(jnp.int32, (EDGE, plan.lanes), 1)
        mine = small_lane % nx // EDGE == small_row

        def corners(block):
            line = jnp.broadcast_to(block[2 * windows : 2 * windows + 1], (EDGE, plan.lanes))
            cells = spread(jnp.where(mine, line, 0.0))
            return [
                sum(cells[level * nx + EDGE * i : level * nx + EDGE * (i + 1)] for i in range(2 * windows))
                for level in range(levels)
            ]

        even = px % 2 == 0
        one, two, columns = first_ref[...], second_ref[-EDGE:], columns_ref[-EDGE:]
        if second_ref.shape[0] > EDGE:
            mixed = second_ref[low - 2 : low - 1]
            mixed = jnp.where(px < plan.px // 2, mixed, pltpu.roll(mixed, plan.lanes - windows, 1))
            two = jnp.concatenate([two[windows - 1 :], mixed, mixed], 0)
            columns = jnp.concatenate([columns[windows - 1 :], columns[: windows - 1]], 0)
        above, below = jnp.where(even, two, one), jnp.where(even, one, two)
        beside = spread(columns)
        beside_above, beside_below = corners(above), corners(below)
        blank = jnp.zeros((EDGE - windows, lanes), jnp.float32)
        for level in range(levels):
            pair, part = level // 2, level % 2

            def line(block):
                return block[pair * windows : (pair + 1) * windows, part * ny : (part + 1) * ny]

            up = jnp.concatenate([line(above), beside_above[level][:windows]], 1)
            down = jnp.concatenate([line(below), beside_below[level][:windows]], 1)
            middle = jnp.concatenate([state_ref[0, level], beside[level * nx : (level + 1) * nx]], 1)
            field = jnp.concatenate([blank, up, middle, down, blank], 0)
            field = jnp.where(inside, field, 0.0)
            for _ in range(windows):
                around = (
                    pltpu.roll(field, 1, 0)
                    + pltpu.roll(field, rows - 1, 0)
                    + pltpu.roll(field, 1, 1)
                    + pltpu.roll(field, lanes - 1, 1)
                )
                field = jnp.where(inside, field + RATE * (around - 4.0 * field), 0.0)
            out_ref[level] = field[EDGE : EDGE + nx, :ny]

    return call(
        kernel, shape_of(levels, nx, ny), state, columns, first, second, jnp.asarray(bf16(place))
    )


def prepare(plan, drive, nest_offsets):
    modes, lanes, levels, windows = plan.modes, plan.lanes, plan.levels, plan.windows
    nx, ny, x, y = plan.nx, plan.ny, plan.x, plan.y
    steps = plan.nest - 1
    maps_x = f32(np.stack([np.tile(x[name], (1, 2)) for name in ("cos_map", "sin_map")]))
    maps_y = f32(np.stack([kron(2, y[name].T) for name in ("cos_map", "sin_map")]))
    rows_x = np.stack([np.tile(p, (1, 2)).reshape(plan.px, nx, 2 * modes) for p in x["powers"][:windows]], 1)
    rows_y = np.stack(
        [p.reshape(plan.py, ny, modes).transpose(0, 2, 1) for p in y["powers"][:windows]], 1
    )

    def kernel(
        drive_ref, maps_x_ref, maps_y_ref, rows_x_ref, rows_y_ref, offsets_ref,
        drive_out, row_out, col_out, spread_x_out, spread_y_out,
    ):
        nest, px, py = lax.axis_index("nest"), lax.axis_index("px"), lax.axis_index("py")
        for w in range(windows):
            drive_out[w] = jnp.concatenate([drive_ref[w, level] for level in range(levels)], 1)
        lane = lax.broadcasted_iota(jnp.int32, (modes, 2 * modes), 1)

        def as_left(twice):
            rounded = twice.astype(jnp.bfloat16).astype(jnp.float32)
            pair = jnp.where(lane >= modes, twice - rounded, rounded)
            return jnp.concatenate([pair, rounded], 1)[:, : 3 * modes].astype(jnp.bfloat16)

        def angle(mode, offset, cells):
            turn = (mode * offset).astype(jnp.float32)
            turn = turn - jnp.floor(turn / (2.0 * cells)) * (2.0 * cells)
            return turn * (math.pi / cells)

        mode = lax.broadcasted_iota(jnp.int32, (EDGE, 2 * modes), 1) % modes
        row = lax.broadcasted_iota(jnp.int32, (EDGE, 2 * modes), 0)
        upright = lax.broadcasted_iota(jnp.int32, (2 * modes, 2 * modes), 0) % modes
        place = lax.broadcasted_iota(jnp.int32, (2 * modes, 2 * modes), 1)
        along, down = jnp.zeros_like(mode), jnp.zeros_like(upright)
        for slot in range(steps):
            domain = jnp.maximum(nest - slot, 0)
            along = jnp.where(row == slot, offsets_ref[0, domain], along)
            down = jnp.where(place == slot, offsets_ref[1, domain], down)
        along = angle(mode, along, nx * plan.px)
        down = angle(upright, down, ny * plan.py)
        cos_x, sin_x = jnp.cos(along), jnp.sin(along)
        cos_y, sin_y = jnp.cos(down), jnp.sin(down)
        for slot in range(steps):
            at = slice(slot, slot + 1)
            row_out[slot] = as_left(maps_x_ref[0] * cos_x[at] - maps_x_ref[1] * sin_x[at])
            col_map = maps_y_ref[0] * cos_y[:, at] - maps_y_ref[1] * sin_y[:, at]
            high, small = halves(col_map)
            col_out[slot] = jnp.concatenate([high, small], 1)
        for w in range(windows):
            p = windows - 1 - w
            for j in range(p + 1):
                combined = sum(multinomial(p, i, j) * rows_x_ref[px, i] for i in range(p - j + 1))
                at = (sum(range(p + 1)) + j) * nx
                spread_x_out[at : at + nx] = as_left(combined)
        for j in range(windows):
            table = rows_y_ref[py, j]
            blank = jnp.zeros_like(table)
            table = jnp.concatenate(
                [jnp.concatenate([table, blank], 1), jnp.concatenate([blank, table], 1)], 0
            )
            high, small = halves(table)
            spread_y_out[j] = jnp.concatenate([high, small], 0)

    shapes = (
        shape_of(windows, modes, lanes),
        shape_of(steps, modes, 3 * modes, kind=jnp.bfloat16),
        shape_of(steps, 2 * modes, 4 * modes, kind=jnp.bfloat16),
        shape_of(sum(range(windows + 1)) * nx, 3 * modes, kind=jnp.bfloat16),
        shape_of(windows, 4 * modes, 2 * ny, kind=jnp.bfloat16),
    )
    return call(kernel, shapes, drive, maps_x, maps_y, f32(rows_x), f32(rows_y), nest_offsets.T, first=True)


def own_tables(plan):
    x, y, modes, windows = plan.x, plan.y, plan.modes, plan.windows
    inward = np.concatenate([np.tile(y["spill"][j].T, (1, 2)) for j in range(1, windows + 1)], 1)
    high, small = parts_of(inward)
    inward = jnp.asarray(np.concatenate([high, small, high, np.zeros_like(high)], 0))
    corner = np.concatenate(
        [kron(2, np.repeat(y["spill"][j].T, EDGE, 0)) for j in range(1, windows + 1)], 1
    )
    high, small = parts_of(corner)
    corner = jnp.asarray(np.concatenate([high, small], 0))
    across = np.zeros((windows * modes, windows * EDGE))
    for n in range(1, windows + 1):
        for j in range(n):
            across[(n - 1) * modes : n * modes, j * EDGE : (j + 1) * EDGE] = sum(
                multinomial(n, i, j) * x["spill"][i] for i in range(1, n - j + 1)
            )
    high, small = parts_of(across)
    across = jnp.asarray(np.pad(np.concatenate([high, small, high], 1), ((0, 0), (0, 3 * EDGE))))
    scale_x = f32(np.broadcast_to(1.0 + x["factor"][:, None], (modes, plan.lanes)))
    scale_y = f32(np.broadcast_to(np.tile(y["factor"], plan.levels), (EDGE, plan.lanes)))
    return inward, corner, across, scale_x, scale_y


def own_modes_of(plan, inward_ref, corner_ref, across_ref, scale_x_ref, scale_y_ref):
    modes, low, lanes = plan.modes, plan.low, plan.lanes
    windows, half, ny = plan.windows, plan.half, plan.ny
    scale_x, scale_y = scale_x_ref[...], scale_y_ref[:1]
    row = lax.broadcasted_iota(jnp.int32, (EDGE, lanes), 0)
    lane = lax.broadcasted_iota(jnp.int32, (EDGE, lanes), 1)
    mine = lane % EDGE == row
    left_lane = lax.broadcasted_iota(jnp.int32, (modes, ny), 1) < modes

    def own_modes(message):
        rows, middle, ends = message[:modes], message[modes:low], message[low:]
        sides = dot(short_stacked(middle, 4 * EDGE), inward_ref[...], ((0,), (0,)))
        cells = jnp.where(mine, jnp.broadcast_to(middle[EDGE - 2 : EDGE - 1], (EDGE, lanes)), 0.0)
        cells = jnp.concatenate([cells[:, i * ny : (i + 1) * ny] for i in range(half)], 0)
        cells = by_parts(cells, corner_ref[:ny], corner_ref[ny:])
        turned, ends = [rows], [ends]
        for j in range(windows):
            at = slice(j * ny, (j + 1) * ny)
            side = [
                jnp.where(
                    left_lane,
                    sides[2 * i * modes : (2 * i + 1) * modes, at],
                    sides[(2 * i + 1) * modes : (2 * i + 2) * modes, at],
                )
                for i in range(half)
            ]
            cell = [cells[i * EDGE : (i + 1) * EDGE, at] for i in range(half)]
            power = scale_y if j == 0 else power * scale_y
            turned.append(rows * power + jnp.concatenate(side, 1))
            ends.append(ends[0] * power + jnp.concatenate(cell, 1))
        over = dot(across_ref[...], short_stacked(jnp.concatenate(ends[:windows], 0), 12 * EDGE))
        result = []
        for n in range(windows):
            turned = [a * scale_x + b for a, b in zip(turned[:-1], turned[1:])]
            result.append(turned[0] + over[n * modes : (n + 1) * modes])
        return result

    return own_modes


def own_early(plan, tables, messages):
    def kernel(*refs):
        count = len(messages)
        own_modes = own_modes_of(plan, *refs[count : count + len(tables)])
        for i in range(count):
            for w, value in enumerate(own_modes(refs[i][...])):
                refs[count + len(tables)][i, w] = value

    return call(kernel, shape_of(len(messages), plan.windows, plan.modes, plan.lanes), *messages, *tables)


def nudge(plan, stepped, gathered, early, tables, crossed, prepared):
    modes, low, lanes, levels = plan.modes, plan.low, plan.lanes, plan.levels
    windows, half, nx, ny = plan.windows, plan.half, plan.nx, plan.ny
    x, y = plan.x, plan.y
    pairs, unpairs = plan.pairs, plan.unpairs
    again = []
    for p in range(1, windows):
        again.append(sum(multinomial(p, i, 0) * x["within"][i] for i in range(p + 1)))
    again = left_table(np.concatenate(again, 0))
    sideways = jnp.stack([right_table(kron(2, y["within"][j])) for j in range(1, windows)])
    drive, row_maps, col_maps, spread_x, spread_y = prepared

    def kernel(
        stepped_ref, drive_ref, row_ref, col_ref, spread_x_ref, spread_y_ref, again_ref, sideways_ref,
        early_ref, *refs,
    ):
        refs, (state_ref, modes_ref) = refs[:-2], refs[-2:]
        root = plan.nest - 1
        nest = lax.axis_index("nest")
        refs, table_refs = refs[: plan.nest], refs[plan.nest :]
        lane = lax.broadcasted_iota(jnp.int32, (1, lanes), 1)
        gains = []
        for ref in refs:
            gain = jnp.where(lane % modes >= modes - 2 * EDGE, ref[low - 2 : low - 1], 0.0)
            gain = gain + pltpu.roll(gain, lanes - 2 * EDGE, 1)
            gains.append(gain + pltpu.roll(gain, lanes - 4 * EDGE, 1))
        owns = [[early_ref[i, w] for w in range(windows)] for i in range(root)]
        owns.append(own_modes_of(plan, *table_refs)(refs[root][...]))
        if crossed:
            odd = nest % 2 == 1
            gains = [gains[0], jnp.where(odd, gains[2], gains[3]), gains[1], gains[3]]
            mixed = [jnp.where(odd, a, b) for a, b in zip(owns[2], owns[3])]
            owns = [owns[0], mixed, owns[1], owns[3]]
        coeffs, changes, later = {}, {}, {}
        for front in range(root + windows):
            cells = [(root - front + w, w) for w in range(windows) if 0 <= root - front + w <= root]
            inner, lefts, rights = {}, {}, {}
            for slot, w in cells:
                if slot < root:
                    inner[slot, w] = times_right(pairs(coeffs[slot + 1, w]), col_ref[slot])
                if w > 0:
                    change = changes[slot, w - 1]
                    count = windows - w
                    left = dot(again_ref[: count * modes], stacked(change))
                    lefts[slot] = left = [left[i * modes : (i + 1) * modes] for i in range(count)]
                    rights[slot] = [unpairs(times_right(pairs(change), sideways_ref[i])) for i in range(count)]
                    later[slot, w - 1, 1] = left[0] + rights[slot][0]
            for slot, w in cells:
                target = drive_ref[w]
                if slot < root:
                    found = dot(row_ref[slot], stacked(unpairs(inner[slot, w])))
                    target = jnp.where(nest <= slot, target, found)
                before = owns[slot][w]
                for v in range(w):
                    before = before + later[slot, v, w - v]
                changes[slot, w] = gains[slot] * (target - before)
                coeffs[slot, w] = before + changes[slot, w]
            for slot, w in cells:
                if w > 0 and windows - w > 1:
                    left, right = lefts[slot], rights[slot]
                    mixed = unpairs(times_right(pairs(left[0]), sideways_ref[0]))
                    later[slot, w - 1, 2] = left[1] + (2.0 * mixed + right[1])
        changes = [changes[0, w] for w in range(windows)]
        coeffs = [coeffs[0, w] for w in range(windows)]
        for level in range(levels):
            modes_ref[0, level] = coeffs[-1][:, level * modes : (level + 1) * modes]
        spread = [0.0] * windows
        for w in range(windows):
            p = windows - 1 - w
            at = sum(range(p + 1)) * nx
            found = dot(spread_x_ref[at : at + (p + 1) * nx], stacked(changes[w]))
            for j in range(p + 1):
                spread[j] = spread[j] + found[j * nx : (j + 1) * nx]
        field = 0.0
        for j in range(windows):
            table = spread_y_ref[j]
            part = by_parts(pairs(spread[j]), table[: 2 * modes], table[2 * modes :])
            field = field + part
        for level in range(levels):
            at_row, at = level // 2 * nx, level % 2 * ny
            state_ref[0, level] = stepped_ref[level] + field[at_row : at_row + nx, at : at + ny]

    return call(
        kernel,
        (shape_of(1, levels, nx, ny), shape_of(1, levels, modes, modes)),
        stepped, drive, row_maps, col_maps, spread_x, spread_y, again, sideways, early, *gathered, *tables,
        final=True,
    )


def swap(value, axis, partner):
    size = math.prod(lax.axis_size(name) for name in (axis if isinstance(axis, tuple) else (axis,)))
    return lax.ppermute(value, axis, [(i, partner(i)) for i in range(size) if 0 <= partner(i) < size])


def body(initial_state, drive_modes, relax_rates, nest_offsets):
    plan = Plan(initial_state, drive_modes)
    halved = plan.py == 2 and plan.px == 4
    share, along = project(plan, initial_state, relax_rates, halved)
    if halved:
        share = lax.optimization_barrier(share)
        from_y = swap(share, "py", lambda i: i ^ 1)
        from_x = swap(along, "px", lambda i: i ^ 1)
        from_both = swap(share, ("py", "px"), lambda i: i ^ (plan.px + 1))
        total, halo = join_first(plan, share, from_y, from_x, from_both, initial_state)
        columns = from_y
        total, drive_modes, nest_offsets = lax.optimization_barrier((total, drive_modes, nest_offsets))
        across = swap(total, "px", lambda i: i ^ 3)
        prepared = prepare(plan, drive_modes, nest_offsets)
        across, prepared = lax.optimization_barrier((across, prepared))
        last = join_last(plan, total, across)
    else:
        from_right = jnp.arange(EDGE)[:, None] < plan.windows
        right = swap(along, "py", lambda i: i - 1)
        left = swap(along, "py", lambda i: i + 1)
        columns = jnp.where(from_right, right, left)
        top, bottom = both_facing(plan, initial_state, columns)
        above = swap(bottom, "px", lambda i: i + 1)
        below = swap(top, "px", lambda i: i - 1)
        even = lax.axis_index("px") % 2 == 0
        halo, across = jnp.where(even, below, above), jnp.where(even, above, below)
        last = lax.psum(share, ("py", "px"))
        prepared = prepare(plan, drive_modes, nest_offsets)
    crossed = plan.nest == 4
    if crossed:
        core = swap(last, "nest", lambda i: i ^ 1)
        chip = swap(last, "nest", lambda i: i ^ 2)
        stepped = step_patch(plan, initial_state, columns, halo, across)
        chip, stepped = lax.optimization_barrier((chip, stepped))
        gathered = [last, chip, core, swap(chip, "nest", lambda i: i ^ 1)]
    else:
        gathered = [last] + [swap(last, "nest", lambda i, s=s: i + s) for s in range(1, plan.nest)]
        stepped = step_patch(plan, initial_state, columns, halo, across)
    tables = own_tables(plan)
    early = own_early(plan, tables, gathered[:-1])
    return nudge(plan, stepped, gathered, early, tables, crossed, prepared)


def solution(mesh):
    return jax.shard_map(
        body,
        mesh=mesh,
        in_specs=(P("nest", None, "px", "py"), P(), P("nest", None), P()),
        out_specs=(P("nest", None, "px", "py"), P("nest", None, None, None)),
        check_vma=False,
    )
```
